32 devices in a mesh: row: 4 (over y, x), col: 4 (over z), depth: 2 (over core).
Axes of the slice: x: 2, y: 2, z: 4, core: 2. Of those that a mesh axis runs over, the one named last changes fastest.
Arguments:
- sequence_stack: bfloat16 [256, 96, 64], P('depth', ('row', 'col')), may hold values from -6 to 6
- present_sequence_flags: int32 [256], replicated, may hold values 0 or 1
- genuine_residue_flags: int32 [96], replicated, may hold values 0 or 1
- couple_state: bfloat16 [96, 96, 128], P('row', 'col'), may hold values from -6 to 6
- tensor_scale: float32 [64], replicated, may hold values from 0.1 to 1.9
- tensor_entry_matrix: bfloat16 [64, 64], replicated, may hold values from -0.75 to 0.75
- tensor_final_matrix: bfloat16 [1024, 128], replicated, may hold values from -1 to 1
- tensor_offset: float32 [128], replicated, may hold values from -3 to 3
- mean_sequence_scale: float32 [64], replicated, may hold values from 0.1 to 1.9
- mean_couple_scale: float32 [128], replicated, may hold values from 0.1 to 1.9
- mean_score_matrix: float32 [128, 8], replicated, may hold values from -64 to 64
- mean_content_matrix: bfloat16 [64, 256], replicated, may hold values from -0.75 to 0.75
- mean_sigmoid_matrix: bfloat16 [64, 256], replicated, may hold values from -0.75 to 0.75
- mean_final_matrix: bfloat16 [256, 64], replicated, may hold values from -0.375 to 0.375
- trimul_scale: float32 [128], replicated, may hold values from 0.1 to 1.9
- trimul_entry_matrix: bfloat16 [128, 640], replicated, may hold values from -0.5 to 0.5
- trimul_result_scale: float32 [128], replicated, may hold values from 0.1 to 1.9
- trimul_final_matrix: bfloat16 [128, 128], replicated, may hold values from -0.5 to 0.5
Outputs:
- revised_sequences: bfloat16 [256, 96, 64], P('depth', ('row', 'col'))
- pair_output: bfloat16 [96, 96, 128], P('row', 'col')
The draws below stay inside these ranges and needn't reach their ends.
All inputs are finite; a program needn't handle non-finite values.
Results may differ from the reference program's by a relative error of at most 0.012.
The reference program's roundings to bfloat16 on the way count: a program that leaves them out, or rounds other values in their place, can miss the bound.
Values may be sent and summed in bfloat16 or wider, within the bound.
No kernel may reach another device: no remote copies, remote signals or barrier semaphores. Data moves between devices by JAX's collectives and lax.ppermute only.
A program may use at most 128 MiB of HBM per device.

```python
import math
import jax
import jax.numpy as jnp
from jax import lax

SEQUENCE_WIDTH = 64
D_PAIR = 128
OPERAND_FEATURES = 32
MEAN_GROUPS = 8
GROUP_FEATURES = 32
COLUMN_TOKENS = 24
RESIDUE_COUNT = 96
SEQUENCE_COUNT = 256
N_COL = 4


def draw_mean_score_matrix(key, part):
    base = jnp.clip(jax.random.normal(key, (D_PAIR, MEAN_GROUPS), jnp.float32), -5.0, 5.0)
    spread = jnp.exp(jax.random.uniform(jax.random.fold_in(key, 7), (1, MEAN_GROUPS), jnp.float32, 0.0, 2.3))
    return base * spread * (1.0 / math.sqrt(D_PAIR))


def set_ends(result, rng, least, top_value):
    longest = result.shape.index(max(result.shape))
    spots = []
    for shift in (0, 1):
        where = [jax.random.randint(jax.random.fold_in(rng, axis), (), 0, length) for axis, length in enumerate(result.shape)]
        where[longest] = (where[longest] + shift) % result.shape[longest]
        spots.append(tuple(where))
    return result.at[spots[0]].set(least).at[spots[1]].set(top_value)


def level_of(rng, dims, shards, smallest, top_value):
    def one(position, parts):
        steps = jax.random.uniform(jax.random.fold_in(jax.random.fold_in(rng, 6), position), (parts,), jnp.float32, smallest / len(shards), top_value / len(shards))
        return jnp.repeat(jnp.exp(steps), dims[position] // parts).reshape((-1,) + (1,) * (len(dims) - position - 1))

    level = one(*shards[0])
    for cut in shards[1:]:
        level = level * one(*cut)
    return level


def scatter_about(key, dims, scale, reach, cuts=(), dtype=jnp.bfloat16):
    level = level_of(key, dims, cuts, -0.22, 0.18) if cuts else 1.0
    entries = jax.random.normal(key, dims, jnp.float32) * scale * level
    return jnp.minimum(jnp.maximum(entries, -reach), reach).astype(dtype)


def setup_inputs(seed: int = 0) -> dict:
    streams_of = jax.random.split(jax.random.key(seed), 19)
    sequence_stack = scatter_about(streams_of[0], (SEQUENCE_COUNT, RESIDUE_COUNT, SEQUENCE_WIDTH), 1.0, 6.0, ((0, 2), (1, 16)))
    present_sequence_flags = set_ends((jax.random.randint(streams_of[1], (SEQUENCE_COUNT,), 0, 4) < 3).astype(jnp.int32), jax.random.fold_in(streams_of[1], 1), 0, 1)
    genuine_residue_flags = set_ends((jax.random.randint(streams_of[2], (RESIDUE_COUNT,), 0, 8) < 7).astype(jnp.int32), jax.random.fold_in(streams_of[2], 1), 0, 1)
    couple_state = scatter_about(streams_of[3], (RESIDUE_COUNT, RESIDUE_COUNT, D_PAIR), 1.0, 6.0, ((0, 4), (1, 4)))
    tensor_scale = jnp.clip(1.0 + 0.18 * jax.random.normal(streams_of[4], (SEQUENCE_WIDTH,), jnp.float32), 0.1, 1.9)
    tensor_entry_matrix = scatter_about(streams_of[5], (SEQUENCE_WIDTH, 2 * OPERAND_FEATURES), SEQUENCE_WIDTH ** -0.5, 0.75)
    tensor_final_matrix = scatter_about(streams_of[6], (OPERAND_FEATURES * OPERAND_FEATURES, D_PAIR), OPERAND_FEATURES ** -0.5, 1.0)
    tensor_offset = scatter_about(streams_of[7], (D_PAIR,), 0.5, 3.0, (), jnp.float32)
    mean_sequence_scale = jnp.clip(1.0 + 0.18 * jax.random.normal(streams_of[8], (SEQUENCE_WIDTH,), jnp.float32), 0.1, 1.9)
    mean_couple_scale = jnp.clip(1.0 + 0.18 * jax.random.normal(streams_of[9], (D_PAIR,), jnp.float32), 0.1, 1.9)
    mean_score_matrix = draw_mean_score_matrix(jax.random.fold_in(streams_of[18], 71), 0)
    mean_content_matrix = scatter_about(streams_of[11], (SEQUENCE_WIDTH, MEAN_GROUPS * GROUP_FEATURES), SEQUENCE_WIDTH ** -0.5, 0.75)
    mean_sigmoid_matrix = scatter_about(streams_of[12], (SEQUENCE_WIDTH, MEAN_GROUPS * GROUP_FEATURES), SEQUENCE_WIDTH ** -0.5, 0.75)
    mean_final_matrix = scatter_about(streams_of[13], (MEAN_GROUPS * GROUP_FEATURES, SEQUENCE_WIDTH), (MEAN_GROUPS * GROUP_FEATURES) ** -0.5, 0.375)
    trimul_scale = jnp.clip(1.0 + 0.18 * jax.random.normal(streams_of[14], (D_PAIR,), jnp.float32), 0.1, 1.9)
    trimul_entry_matrix = scatter_about(streams_of[15], (D_PAIR, 5 * D_PAIR), D_PAIR ** -0.5, 0.5)
    trimul_result_scale = jnp.clip(1.0 + 0.18 * jax.random.normal(streams_of[16], (D_PAIR,), jnp.float32), 0.1, 1.9)
    trimul_final_matrix = scatter_about(streams_of[17], (D_PAIR, D_PAIR), D_PAIR ** -0.5, 0.5)
    return {"sequence_stack": sequence_stack, "present_sequence_flags": present_sequence_flags, "genuine_residue_flags": genuine_residue_flags, "couple_state": couple_state, "tensor_scale": tensor_scale, "tensor_entry_matrix": tensor_entry_matrix, "tensor_final_matrix": tensor_final_matrix, "tensor_offset": tensor_offset, "mean_sequence_scale": mean_sequence_scale, "mean_couple_scale": mean_couple_scale, "mean_score_matrix": mean_score_matrix, "mean_content_matrix": mean_content_matrix, "mean_sigmoid_matrix": mean_sigmoid_matrix, "mean_final_matrix": mean_final_matrix, "trimul_scale": trimul_scale, "trimul_entry_matrix": trimul_entry_matrix, "trimul_result_scale": trimul_result_scale, "trimul_final_matrix": trimul_final_matrix}


epsilon = 1e-05

def standardize_features(value_rows, scale):
    value_rows = value_rows.astype(jnp.float32)
    average = lax.optimization_barrier(jnp.mean(value_rows, -1, keepdims=True))
    centred = value_rows - average
    variance = lax.optimization_barrier(jnp.mean(centred * centred, -1, keepdims=True))
    return centred * lax.rsqrt(variance + epsilon) * scale

def reference(sequence_stack, present_sequence_flags, genuine_residue_flags, couple_state, tensor_scale, tensor_entry_matrix, tensor_final_matrix, tensor_offset, mean_sequence_scale, mean_couple_scale, mean_score_matrix, mean_content_matrix, mean_sigmoid_matrix, mean_final_matrix, trimul_scale, trimul_entry_matrix, trimul_result_scale, trimul_final_matrix):
    row_softmax_weight = present_sequence_flags.astype(jnp.float32)
    row_count = jnp.sum(row_softmax_weight)
    tensor_standardized = standardize_features(sequence_stack, tensor_scale).astype(jnp.bfloat16)
    factors = (jnp.dot(tensor_standardized, tensor_entry_matrix, preferred_element_type=jnp.float32) * row_softmax_weight[:, None, None]).astype(jnp.bfloat16)
    left_projection = factors[..., :OPERAND_FEATURES].astype(jnp.float32)
    right_proj = factors[..., OPERAND_FEATURES:].astype(jnp.float32)
    left_factor_blocks = jnp.transpose(left_projection.reshape(SEQUENCE_COUNT, N_COL, COLUMN_TOKENS, OPERAND_FEATURES), (1, 0, 2, 3))
    out_float = tensor_final_matrix.astype(jnp.float32)

    def outer_block(piece):
        outer_sum = jnp.einsum('sic,sjd->ijcd', piece, right_proj).reshape(COLUMN_TOKENS, RESIDUE_COUNT, OPERAND_FEATURES * OPERAND_FEATURES)
        return jnp.dot(outer_sum, out_float, precision=lax.Precision.HIGHEST)
    projected_outer = lax.map(outer_block, left_factor_blocks).reshape(RESIDUE_COUNT, RESIDUE_COUNT, D_PAIR)
    update = projected_outer / (row_count + 0.001) + tensor_offset
    pair_one = (couple_state.astype(jnp.float32) + update).astype(jnp.bfloat16)
    token_weight = genuine_residue_flags.astype(jnp.float32)
    logits = jnp.einsum('ijc,ch->ijh', standardize_features(pair_one, mean_couple_scale), mean_score_matrix, precision=lax.Precision.HIGHEST)
    logits = logits + 1000000000.0 * (token_weight - 1.0)[None, :, None]
    peak = lax.optimization_barrier(jnp.max(logits, axis=1, keepdims=True))
    expo = jnp.exp(logits - peak)
    weights = (expo / lax.optimization_barrier(jnp.sum(expo, axis=1, keepdims=True))).astype(jnp.bfloat16)
    mean_standardized = standardize_features(sequence_stack, mean_sequence_scale).astype(jnp.bfloat16)
    value_rows = jnp.dot(mean_standardized, mean_content_matrix, preferred_element_type=jnp.float32).astype(jnp.bfloat16)
    value_rows = value_rows.reshape(SEQUENCE_COUNT, RESIDUE_COUNT, MEAN_GROUPS, GROUP_FEATURES)
    gate_values = jax.nn.sigmoid(jnp.dot(mean_standardized, mean_sigmoid_matrix, preferred_element_type=jnp.float32))
    averaged_values = jnp.einsum('ijh,sjhe->sihe', weights.astype(jnp.float32), value_rows.astype(jnp.float32))
    gated_output = gate_values * averaged_values.reshape(SEQUENCE_COUNT, RESIDUE_COUNT, MEAN_GROUPS * GROUP_FEATURES)
    sequence_delta = jnp.dot(gated_output, mean_final_matrix.astype(jnp.float32), precision=lax.Precision.HIGHEST)
    revised_sequences = (sequence_stack.astype(jnp.float32) + sequence_delta).astype(jnp.bfloat16)
    tri_normed = standardize_features(pair_one, trimul_scale).astype(jnp.bfloat16)
    projected = jnp.dot(tri_normed, trimul_entry_matrix, preferred_element_type=jnp.float32)
    pair_mask = (token_weight[:, None] * token_weight[None, :])[..., None]
    width = D_PAIR
    tri_left = (jax.nn.sigmoid(projected[..., 0:width]) * projected[..., width:2 * width] * pair_mask).astype(jnp.bfloat16)
    tri_right = (jax.nn.sigmoid(projected[..., 2 * width:3 * width]) * projected[..., 3 * width:4 * width] * pair_mask).astype(jnp.bfloat16)
    out_gate = jax.nn.sigmoid(projected[..., 4 * width:5 * width])
    product = jnp.einsum('ikc,jkc->ijc', tri_left.astype(jnp.float32), tri_right.astype(jnp.float32))
    final = out_gate * jnp.dot(standardize_features(product, trimul_result_scale).astype(jnp.bfloat16), trimul_final_matrix, preferred_element_type=jnp.float32)
    pair_output = (pair_one.astype(jnp.float32) + final).astype(jnp.bfloat16)
    return (revised_sequences, pair_output)
```

```python
import jax
import jax.numpy as jnp
from jax import lax
from jax.sharding import PartitionSpec as P

epsilon = 1e-05
bf16 = jnp.bfloat16
f32 = jnp.float32


def from_root(array, axis, root):
    mine = lax.axis_index(axis) == root
    return lax.psum(jnp.where(mine, array, jnp.zeros_like(array)), axis)


def standardize_features(value_rows, scale):
    value_rows = value_rows.astype(jnp.float32)
    average = jnp.mean(value_rows, -1, keepdims=True)
    centred = value_rows - average
    variance = jnp.mean(centred * centred, -1, keepdims=True)
    return centred * lax.rsqrt(variance + epsilon) * scale


def on_device_generic(
    sequence_stack,
    present_sequence_flags,
    genuine_residue_flags,
    couple_state,
    tensor_scale,
    tensor_entry_matrix,
    tensor_final_matrix,
    tensor_offset,
    mean_sequence_scale,
    mean_couple_scale,
    mean_score_matrix,
    mean_content_matrix,
    mean_sigmoid_matrix,
    mean_final_matrix,
    trimul_scale,
    trimul_entry_matrix,
    trimul_result_scale,
    trimul_final_matrix,
):
    n_row = lax.axis_size("row")
    n_col = lax.axis_size("col")
    row_index = lax.axis_index("row")
    col_index = lax.axis_index("col")
    depth_position = lax.axis_index("depth")
    piece_rows, piece_columns, width = couple_state.shape
    sequence_count, shard_residues, ignored_quantity = sequence_stack.shape
    hidden = tensor_entry_matrix.shape[1] // 2
    head_split = mean_score_matrix.shape[1]
    head_channels = mean_content_matrix.shape[1] // head_split
    token_weight = genuine_residue_flags.astype(jnp.float32)
    mask_as_float = present_sequence_flags.astype(jnp.float32)
    row_softmax_weight = lax.dynamic_slice_in_dim(
        mask_as_float, depth_position * sequence_count, sequence_count
    )
    row_count = jnp.sum(mask_as_float)
    entire_sequences = lax.all_gather(sequence_stack, "col", axis=1, tiled=True)
    root_row = col_index * n_row // n_col
    offset = col_index * piece_columns - root_row * piece_rows
    column_piece = lax.dynamic_slice_in_dim(entire_sequences, offset, piece_columns, 1)
    whole_cols = from_root(column_piece, "row", root_row)
    opm_rows = standardize_features(entire_sequences, tensor_scale).astype(jnp.bfloat16)
    opm_cols = standardize_features(whole_cols, tensor_scale).astype(jnp.bfloat16)
    left_projection = (
        jnp.dot(opm_rows, tensor_entry_matrix[:, :hidden], preferred_element_type=jnp.float32)
        * row_softmax_weight[:, None, None]
    ).astype(jnp.bfloat16)
    right_proj = (
        jnp.dot(opm_cols, tensor_entry_matrix[:, hidden:], preferred_element_type=jnp.float32)
        * row_softmax_weight[:, None, None]
    ).astype(jnp.bfloat16)
    outer_sum = jnp.einsum(
        "sic,sjd->ijcd", left_projection, right_proj, preferred_element_type=jnp.float32
    )
    outer_sum = outer_sum.reshape(piece_rows, piece_columns, hidden * hidden)
    out_float = tensor_final_matrix.astype(jnp.float32)
    outer_share = lax.psum_scatter(outer_sum, "depth", scatter_dimension=0, tiled=True)
    share_rows = outer_share.shape[0]
    pair_share = lax.dynamic_slice_in_dim(couple_state, depth_position * share_rows, share_rows, 0)
    update = (
        jnp.dot(outer_share, out_float, precision=lax.Precision.HIGHEST) / (row_count + 0.001)
        + tensor_offset
    )
    new_share = (pair_share.astype(jnp.float32) + update).astype(jnp.bfloat16)
    pair_one = lax.all_gather(new_share, "depth", axis=0, tiled=True)
    row_tokens = lax.dynamic_slice_in_dim(token_weight, row_index * piece_rows, piece_rows)
    col_tokens = lax.dynamic_slice_in_dim(token_weight, col_index * piece_columns, piece_columns)
    logits = jnp.einsum(
        "ijc,ch->ijh",
        standardize_features(pair_one, mean_couple_scale),
        mean_score_matrix,
        precision=lax.Precision.HIGHEST,
    )
    logits = logits + 1000000000.0 * (col_tokens - 1.0)[None, :, None]
    peak = lax.pmax(jnp.max(logits, axis=1), "col")
    expo = jnp.exp(logits - peak[:, None, :])
    total = lax.psum(jnp.sum(expo, axis=1), "col")
    weights = (expo / total[:, None, :]).astype(jnp.bfloat16)
    col_normed = standardize_features(whole_cols, mean_sequence_scale).astype(jnp.bfloat16)
    value_rows = jnp.dot(
        col_normed, mean_content_matrix, preferred_element_type=jnp.float32
    ).astype(jnp.bfloat16)
    value_rows = value_rows.reshape(sequence_count, piece_columns, head_split, head_channels)
    averaged_values = jnp.einsum(
        "ijh,sjhe->sihe", weights, value_rows, preferred_element_type=jnp.float32
    )
    averaged_values = averaged_values.reshape(
        sequence_count, piece_rows, head_split * head_channels
    )
    output_weight = mean_final_matrix.astype(jnp.float32)
    local_portion = lax.psum_scatter(
        averaged_values.astype(jnp.bfloat16), "col", scatter_dimension=1, tiled=True
    ).astype(jnp.float32)
    shard_standardized = standardize_features(sequence_stack, mean_sequence_scale).astype(
        jnp.bfloat16
    )
    gate_values = jax.nn.sigmoid(
        jnp.dot(shard_standardized, mean_sigmoid_matrix, preferred_element_type=jnp.float32)
    )
    sequence_delta = jnp.dot(
        gate_values * local_portion, output_weight, precision=lax.Precision.HIGHEST
    )
    revised_sequences = (sequence_stack.astype(jnp.float32) + sequence_delta).astype(jnp.bfloat16)
    tri_normed = standardize_features(pair_one, trimul_scale).astype(jnp.bfloat16)
    projected = jnp.dot(tri_normed, trimul_entry_matrix, preferred_element_type=jnp.float32)
    pair_mask = (row_tokens[:, None] * col_tokens[None, :])[..., None]
    tri_left = (
        jax.nn.sigmoid(projected[..., 0:width]) * projected[..., width : 2 * width] * pair_mask
    ).astype(jnp.bfloat16)
    tri_right = (
        jax.nn.sigmoid(projected[..., 2 * width : 3 * width])
        * projected[..., 3 * width : 4 * width]
        * pair_mask
    ).astype(jnp.bfloat16)
    out_gate = jax.nn.sigmoid(projected[..., 4 * width : 5 * width])
    left_rows, right_rows = (
        lax.all_gather(tri_left, "col", axis=1, tiled=True),
        lax.all_gather(tri_right, "col", axis=1, tiled=True),
    )
    right_piece = lax.dynamic_slice_in_dim(right_rows, offset, piece_columns, 0)
    right_needed = from_root(right_piece, "row", root_row)
    product = jnp.einsum(
        "ikc,jkc->ijc", left_rows, right_needed, preferred_element_type=jnp.float32
    )
    final = out_gate * jnp.dot(
        standardize_features(product, trimul_result_scale).astype(jnp.bfloat16),
        trimul_final_matrix,
        preferred_element_type=jnp.float32,
    )
    pair_output = (pair_one.astype(jnp.float32) + final).astype(jnp.bfloat16)
    return (revised_sequences, pair_output)


def split_pieces(value, count):
    pieces = []
    for _ in range(count):
        piece = lax.reduce_precision(value, 8, 7)
        pieces.append(piece.astype(bf16))
        value = value - piece
    return pieces


def factor_stage(tokens, flags, scale, entry):
    value = tokens.astype(f32)
    average = jnp.mean(value, 1, keepdims=True)
    centred = value - average
    variance = jnp.mean(centred * centred, 1, keepdims=True)
    normed = (centred * lax.rsqrt(variance + epsilon) * scale[None, :, None]).astype(bf16)
    factors = jnp.einsum("tcs,cf->tfs", normed, entry, preferred_element_type=f32)
    return (factors * flags[None, None, :]).astype(bf16)


def outer_stage(left, right, final):
    n, t, hidden, s = left.shape
    outer = jnp.einsum(
        "ics,jds->ijcd",
        left.reshape(n * t, hidden, s),
        right.reshape(n * t, hidden, s),
        preferred_element_type=f32,
    ).reshape(n * t * n * t, hidden * hidden)
    high = outer.astype(bf16)
    low = (outer - high.astype(f32)).astype(bf16)
    update = jnp.dot(high, final, preferred_element_type=f32) + jnp.dot(
        low, final, preferred_element_type=f32
    )
    return update.reshape(n * t, n * t, -1)


def pair_stage(update, couple, inverse, offset, row_tokens, col_tokens, couple_scale, score, tri_scale, entry, half, parts):
    rows, cols, width = couple.shape
    pair_one = (couple.astype(f32) + update * inverse + offset).astype(bf16)
    value = pair_one.astype(f32)
    average = jnp.mean(value, -1, keepdims=True)
    centred = value - average
    variance = jnp.mean(centred * centred, -1, keepdims=True)
    unit = centred * lax.rsqrt(variance + epsilon)
    logits = jnp.einsum("ijc,ch->ihj", unit * couple_scale, score, precision=lax.Precision.HIGHEST)
    logits = logits + 1000000000.0 * (col_tokens - 1.0)[None, None, :]
    peak = jnp.max(logits, -1)
    expo = jnp.exp(logits - peak[..., None]).astype(bf16).reshape(rows, -1)
    normed = (unit * tri_scale).astype(bf16)
    mine = lax.dynamic_slice_in_dim(
        entry[:, : 4 * width].reshape(width, 4, 2, width // 2), half, 1, 2
    ).reshape(width, 2 * width)
    projected = jnp.einsum("ijz,zc->cij", normed, mine, preferred_element_type=f32)
    projected = projected.reshape(4, width // 2, rows, cols)
    mask = (row_tokens[:, None] * col_tokens[None, :])[None]
    left = (jax.nn.sigmoid(projected[0]) * projected[1] * mask).astype(bf16)
    right = (jax.nn.sigmoid(projected[2]) * projected[3] * mask).astype(bf16)

    def by_peer(operand):
        operand = operand.reshape(parts, -1, rows, cols)
        return operand.transpose(0, 2, 1, 3).reshape(parts, rows, -1)

    left, right = by_peer(left), by_peer(right)
    spare = 128 - left.shape[-1]

    def everyone(piece):
        return jnp.broadcast_to(piece[None], (parts,) + piece.shape)

    stats = jnp.concatenate(split_pieces(peak, 3), -1)
    lanes = stats.shape[-1]
    stats = stats.reshape(rows // 8, 8, lanes).transpose(1, 0, 2).reshape(8, -1)
    stats = jnp.pad(stats, ((0, 0), (0, 128 - stats.shape[-1])))
    block = jnp.concatenate(
        [
            jnp.concatenate([left, everyone(expo[:, 128 : 128 + spare])], -1),
            jnp.concatenate([right, everyone(expo[:, 128 + spare : 128 + 2 * spare])], -1),
            everyone(expo[:, :128]),
            everyone(stats),
        ],
        1,
    )
    return pair_one, block


def middle_stage(block, n, rows, cols, heads, seq_scale, content, sigmoid_matrix, final):
    parts = n * n
    ch = final.shape[1]
    feats = 128 // cols - (1 if (128 // cols) * cols > 96 else 0)
    left = block[:, :rows]
    right = block[:, rows : 2 * rows]
    expo = jnp.concatenate([block[:, 2 * rows : 3 * rows], left[..., feats * cols :], right[..., feats * cols :]], -1)
    stats = block[:, 3 * rows : 3 * rows + 8]
    slab = block[:, 3 * rows + 8 :]

    def whole(operand):
        operand = operand[..., : feats * cols].reshape(n, n, rows, feats, cols)
        return operand.transpose(3, 0, 2, 1, 4).reshape(feats, n * rows, n * cols)

    product = jnp.einsum("fik,fjk->fij", whole(left), whole(right), preferred_element_type=f32)
    product = product.astype(bf16).reshape(feats, n, rows, n, cols)
    product = product.transpose(1, 3, 2, 0, 4).reshape(parts, rows, feats * cols)
    product = jnp.pad(product, ((0, 0), (0, 0), (0, 128 - feats * cols)))
    stats = stats[..., : rows // 8 * 3 * heads].reshape(parts, 8, rows // 8, 3, heads)
    peak = stats.astype(f32).sum(3).transpose(0, 2, 1, 3).reshape(n, n, rows, heads)
    expo = expo.reshape(n, n, rows, heads, cols).astype(f32)
    top = jnp.max(peak, 1, keepdims=True)
    factor = jnp.exp(peak - top)
    total = jnp.sum(factor * jnp.sum(expo, -1), 1, keepdims=True)
    weights = (expo * (factor / total)[..., None]).astype(bf16)
    weights = weights.transpose(3, 0, 2, 1, 4).reshape(heads, n * rows, n * cols)
    groups = slab.shape[1] // 8
    tokens = slab.reshape(parts, groups, 8, 128 // ch, ch).transpose(2, 0, 1, 3, 4).reshape(8, n * rows, ch)
    normed = standardize_features(tokens, seq_scale).astype(bf16)
    values = jnp.dot(normed, content, preferred_element_type=f32).astype(bf16)
    gates = jax.nn.sigmoid(jnp.dot(normed, sigmoid_matrix, preferred_element_type=f32))
    values = values.reshape(8, n * rows, heads, -1)
    averaged = jnp.einsum("hij,sjhe->sihe", weights, values, preferred_element_type=f32)
    gated = gates * averaged.reshape(8, n * rows, -1)
    delta = jnp.dot(gated, final.astype(f32), precision=lax.Precision.HIGHEST)
    revised = (tokens.astype(f32) + delta).astype(bf16)
    revised = revised.reshape(8, parts, groups, 128 // ch, ch).transpose(1, 2, 0, 3, 4)
    revised = revised.reshape(parts, groups * 8, 128)
    return jnp.concatenate([product, revised], 1)


def final_stage(product, pair_one, tri_scale, entry, result_scale, final):
    rows, cols, width = pair_one.shape
    depth, parts = product.shape[:2]
    feats = width // (depth * parts)
    product = product[..., : feats * cols].reshape(depth, parts, rows, feats, cols)
    product = product.transpose(2, 4, 0, 1, 3).reshape(rows, cols, width)
    normed = standardize_features(pair_one, tri_scale).astype(bf16)
    gate = jax.nn.sigmoid(jnp.dot(normed, entry[:, 4 * width :], preferred_element_type=f32))
    final = gate * jnp.dot(
        standardize_features(product, result_scale).astype(bf16), final, preferred_element_type=f32
    )
    return (pair_one.astype(f32) + final).astype(bf16)


def on_device(
    sequence_stack,
    present_sequence_flags,
    genuine_residue_flags,
    couple_state,
    tensor_scale,
    tensor_entry_matrix,
    tensor_final_matrix,
    tensor_offset,
    mean_sequence_scale,
    mean_couple_scale,
    mean_score_matrix,
    mean_content_matrix,
    mean_sigmoid_matrix,
    mean_final_matrix,
    trimul_scale,
    trimul_entry_matrix,
    trimul_result_scale,
    trimul_final_matrix,
):
    n = lax.axis_size("row")
    parts = n * n
    row_index = lax.axis_index("row")
    col_index = lax.axis_index("col")
    half = lax.axis_index("depth")
    rows, cols, width = couple_state.shape
    count, t, ch = sequence_stack.shape
    hidden = tensor_entry_matrix.shape[1] // 2
    heads = mean_score_matrix.shape[1]
    token_weight = genuine_residue_flags.astype(f32)
    flags = present_sequence_flags.astype(f32)
    inverse = 1.0 / (jnp.sum(flags) + 0.001)
    my_flags = lax.dynamic_slice_in_dim(flags, half * count, count)
    tokens = sequence_stack.transpose(1, 2, 0)
    factors = factor_stage(tokens, my_flags, tensor_scale, tensor_entry_matrix)
    left, right = factors[:, :hidden], factors[:, hidden:]

    def move(array, where):
        pairs = [(r * n + c, where(r, c)[0] * n + where(r, c)[1]) for r in range(n) for c in range(n)]
        return lax.ppermute(array, ("row", "col"), pairs)

    lefts = [left] + [move(left, lambda r, c, k=k: (r, (c + k) % n)) for k in range(1, n)]
    rights = [move(right, lambda r, c, k=k: ((c + k) % n, r)) for k in range(n)]
    all_left = jnp.zeros((n,) + left.shape, bf16)
    all_right = jnp.zeros((n,) + left.shape, bf16)
    for k in range(n):
        all_left = lax.dynamic_update_index_in_dim(all_left, lefts[k], (col_index - k) % n, 0)
        all_right = lax.dynamic_update_index_in_dim(all_right, rights[k], (row_index - k) % n, 0)
    update = outer_stage(all_left, all_right, tensor_final_matrix)
    update = update + lax.ppermute(update, "depth", [(0, 1), (1, 0)])
    row_tokens = lax.dynamic_slice_in_dim(token_weight, row_index * rows, rows)
    col_tokens = lax.dynamic_slice_in_dim(token_weight, col_index * cols, cols)
    pair_one, block = pair_stage(
        update, couple_state, inverse, tensor_offset, row_tokens, col_tokens, mean_couple_scale,
        mean_score_matrix, trimul_scale, trimul_entry_matrix, half, parts,
    )
    slab = sequence_stack.reshape(parts, 8, t * ch // 128, 128).transpose(0, 2, 1, 3)
    slab = slab.reshape(parts, -1, 128)
    block = lax.all_to_all(jnp.concatenate([block, slab], 1), ("row", "col"), 0, 0, tiled=True)
    block = middle_stage(
        block, n, rows, cols, heads, mean_sequence_scale, mean_content_matrix, mean_sigmoid_matrix,
        mean_final_matrix,
    )
    block = lax.all_to_all(block, ("row", "col"), 0, 0, tiled=True)
    product = block[:, :rows]
    other = lax.ppermute(product, "depth", [(0, 1), (1, 0)])
    first = half == 0
    product = jnp.stack([jnp.where(first, product, other), jnp.where(first, other, product)])
    revised = block[:, rows:].reshape(parts, t * ch // 128, 8, 128).transpose(0, 2, 1, 3)
    revised = revised.reshape(count, t, ch)
    pair_output = final_stage(
        product, pair_one, trimul_scale, trimul_entry_matrix, trimul_result_scale, trimul_final_matrix
    )
    return (revised, pair_output)


def suits(mesh):
    return mesh.shape["row"] == mesh.shape["col"] and mesh.shape["depth"] == 2


def solution(mesh):
    placed = (P("depth", ("row", "col"), None), P(), P(), P("row", "col", None)) + (P(),) * 14
    return jax.shard_map(
        on_device if suits(mesh) else on_device_generic,
        mesh=mesh,
        in_specs=placed,
        out_specs=(P("depth", ("row", "col"), None), P("row", "col", None)),
        check_vma=False,
    )
```

```python
import jax
import jax.numpy as jnp
from jax import lax
from jax.experimental import pallas as pl
from jax.experimental.pallas import tpu as pltpu
from jax.sharding import PartitionSpec as P

epsilon = 1e-05
bf16 = jnp.bfloat16
f32 = jnp.float32


def from_root(array, axis, root):
    mine = lax.axis_index(axis) == root
    return lax.psum(jnp.where(mine, array, jnp.zeros_like(array)), axis)


def standardize_features(value_rows, scale):
    value_rows = value_rows.astype(jnp.float32)
    average = jnp.mean(value_rows, -1, keepdims=True)
    centred = value_rows - average
    variance = jnp.mean(centred * centred, -1, keepdims=True)
    return centred * lax.rsqrt(variance + epsilon) * scale


def on_device_generic(
    sequence_stack,
    present_sequence_flags,
    genuine_residue_flags,
    couple_state,
    tensor_scale,
    tensor_entry_matrix,
    tensor_final_matrix,
    tensor_offset,
    mean_sequence_scale,
    mean_couple_scale,
    mean_score_matrix,
    mean_content_matrix,
    mean_sigmoid_matrix,
    mean_final_matrix,
    trimul_scale,
    trimul_entry_matrix,
    trimul_result_scale,
    trimul_final_matrix,
):
    n_row = lax.axis_size("row")
    n_col = lax.axis_size("col")
    row_index = lax.axis_index("row")
    col_index = lax.axis_index("col")
    depth_position = lax.axis_index("depth")
    piece_rows, piece_columns, width = couple_state.shape
    sequence_count, shard_residues, ignored_quantity = sequence_stack.shape
    hidden = tensor_entry_matrix.shape[1] // 2
    head_split = mean_score_matrix.shape[1]
    head_channels = mean_content_matrix.shape[1] // head_split
    token_weight = genuine_residue_flags.astype(jnp.float32)
    mask_as_float = present_sequence_flags.astype(jnp.float32)
    row_softmax_weight = lax.dynamic_slice_in_dim(
        mask_as_float, depth_position * sequence_count, sequence_count
    )
    row_count = jnp.sum(mask_as_float)
    entire_sequences = lax.all_gather(sequence_stack, "col", axis=1, tiled=True)
    root_row = col_index * n_row // n_col
    offset = col_index * piece_columns - root_row * piece_rows
    column_piece = lax.dynamic_slice_in_dim(entire_sequences, offset, piece_columns, 1)
    whole_cols = from_root(column_piece, "row", root_row)
    opm_rows = standardize_features(entire_sequences, tensor_scale).astype(jnp.bfloat16)
    opm_cols = standardize_features(whole_cols, tensor_scale).astype(jnp.bfloat16)
    left_projection = (
        jnp.dot(opm_rows, tensor_entry_matrix[:, :hidden], preferred_element_type=jnp.float32)
        * row_softmax_weight[:, None, None]
    ).astype(jnp.bfloat16)
    right_proj = (
        jnp.dot(opm_cols, tensor_entry_matrix[:, hidden:], preferred_element_type=jnp.float32)
        * row_softmax_weight[:, None, None]
    ).astype(jnp.bfloat16)
    outer_sum = jnp.einsum(
        "sic,sjd->ijcd", left_projection, right_proj, preferred_element_type=jnp.float32
    )
    outer_sum = outer_sum.reshape(piece_rows, piece_columns, hidden * hidden)
    out_float = tensor_final_matrix.astype(jnp.float32)
    outer_share = lax.psum_scatter(outer_sum, "depth", scatter_dimension=0, tiled=True)
    share_rows = outer_share.shape[0]
    pair_share = lax.dynamic_slice_in_dim(couple_state, depth_position * share_rows, share_rows, 0)
    update = (
        jnp.dot(outer_share, out_float, precision=lax.Precision.HIGHEST) / (row_count + 0.001)
        + tensor_offset
    )
    new_share = (pair_share.astype(jnp.float32) + update).astype(jnp.bfloat16)
    pair_one = lax.all_gather(new_share, "depth", axis=0, tiled=True)
    row_tokens = lax.dynamic_slice_in_dim(token_weight, row_index * piece_rows, piece_rows)
    col_tokens = lax.dynamic_slice_in_dim(token_weight, col_index * piece_columns, piece_columns)
    logits = jnp.einsum(
        "ijc,ch->ijh",
        standardize_features(pair_one, mean_couple_scale),
        mean_score_matrix,
        precision=lax.Precision.HIGHEST,
    )
    logits = logits + 1000000000.0 * (col_tokens - 1.0)[None, :, None]
    peak = lax.pmax(jnp.max(logits, axis=1), "col")
    expo = jnp.exp(logits - peak[:, None, :])
    total = lax.psum(jnp.sum(expo, axis=1), "col")
    weights = (expo / total[:, None, :]).astype(jnp.bfloat16)
    col_normed = standardize_features(whole_cols, mean_sequence_scale).astype(jnp.bfloat16)
    value_rows = jnp.dot(
        col_normed, mean_content_matrix, preferred_element_type=jnp.float32
    ).astype(jnp.bfloat16)
    value_rows = value_rows.reshape(sequence_count, piece_columns, head_split, head_channels)
    averaged_values = jnp.einsum(
        "ijh,sjhe->sihe", weights, value_rows, preferred_element_type=jnp.float32
    )
    averaged_values = averaged_values.reshape(
        sequence_count, piece_rows, head_split * head_channels
    )
    output_weight = mean_final_matrix.astype(jnp.float32)
    local_portion = lax.psum_scatter(
        averaged_values.astype(jnp.bfloat16), "col", scatter_dimension=1, tiled=True
    ).astype(jnp.float32)
    shard_standardized = standardize_features(sequence_stack, mean_sequence_scale).astype(
        jnp.bfloat16
    )
    gate_values = jax.nn.sigmoid(
        jnp.dot(shard_standardized, mean_sigmoid_matrix, preferred_element_type=jnp.float32)
    )
    sequence_delta = jnp.dot(
        gate_values * local_portion, output_weight, precision=lax.Precision.HIGHEST
    )
    revised_sequences = (sequence_stack.astype(jnp.float32) + sequence_delta).astype(jnp.bfloat16)
    tri_normed = standardize_features(pair_one, trimul_scale).astype(jnp.bfloat16)
    projected = jnp.dot(tri_normed, trimul_entry_matrix, preferred_element_type=jnp.float32)
    pair_mask = (row_tokens[:, None] * col_tokens[None, :])[..., None]
    tri_left = (
        jax.nn.sigmoid(projected[..., 0:width]) * projected[..., width : 2 * width] * pair_mask
    ).astype(jnp.bfloat16)
    tri_right = (
        jax.nn.sigmoid(projected[..., 2 * width : 3 * width])
        * projected[..., 3 * width : 4 * width]
        * pair_mask
    ).astype(jnp.bfloat16)
    out_gate = jax.nn.sigmoid(projected[..., 4 * width : 5 * width])
    left_rows, right_rows = (
        lax.all_gather(tri_left, "col", axis=1, tiled=True),
        lax.all_gather(tri_right, "col", axis=1, tiled=True),
    )
    right_piece = lax.dynamic_slice_in_dim(right_rows, offset, piece_columns, 0)
    right_needed = from_root(right_piece, "row", root_row)
    product = jnp.einsum(
        "ikc,jkc->ijc", left_rows, right_needed, preferred_element_type=jnp.float32
    )
    final = out_gate * jnp.dot(
        standardize_features(product, trimul_result_scale).astype(jnp.bfloat16),
        trimul_final_matrix,
        preferred_element_type=jnp.float32,
    )
    pair_output = (pair_one.astype(jnp.float32) + final).astype(jnp.bfloat16)
    return (revised_sequences, pair_output)


def split_pieces(value, count):
    pieces = []
    for _ in range(count):
        piece = lax.reduce_precision(value, 8, 7)
        pieces.append(piece.astype(bf16))
        value = value - piece
    return pieces


def factor_stage(tokens, flags, scale, entry):
    value = tokens.astype(f32)
    average = jnp.mean(value, 1, keepdims=True)
    centred = value - average
    variance = jnp.mean(centred * centred, 1, keepdims=True)
    normed = (centred * lax.rsqrt(variance + epsilon) * scale[None, :, None]).astype(bf16)
    factors = jnp.einsum("tcs,cf->tfs", normed, entry, preferred_element_type=f32)
    return (factors * flags[None, None, :]).astype(bf16)


def outer_kernel(place, *refs):
    n, t, hidden = place.shape[0] // 2, refs[0].shape[0], refs[0].shape[1]
    s = refs[0].shape[2]
    lefts, rights = refs[:n], refs[n : 2 * n]
    final, out, left, pieces, right, plain, turned, outer, high, low = refs[2 * n :]
    tokens, ratio = n * t, 128 // hidden
    for k in range(n):
        left[place[k]] = lefts[k][...].reshape(t * hidden, s)
        pieces[place[n + k]] = rights[k][...].reshape(t * hidden, s).astype(f32)
    for k in range(n):
        for u in range(t):
            right[pl.ds(k * t + u, hidden, stride=tokens), :] = pieces[k, u * hidden : (u + 1) * hidden, :]
    plain[...] = final[...].astype(f32)
    for d in range(hidden):
        turned[d * hidden : (d + 1) * hidden, :] = plain[pl.ds(d, hidden, stride=hidden), :].astype(bf16)
    outer[...] = lax.dot_general(
        right[...].astype(bf16),
        left[...].reshape(tokens * hidden, s),
        (((1,), (1,)), ((), ())),
        preferred_element_type=f32,
    )
    lane = lax.broadcasted_iota(jnp.int32, (tokens, 128), 1)
    for g in range(tokens // ratio):
        for q in range(hidden // ratio):
            tiles = [
                outer[(q * ratio + d) * tokens : (q * ratio + d + 1) * tokens, g * 128 : (g + 1) * 128]
                for d in range(ratio)
            ]
            bit = 1
            while bit < ratio:
                upper = (lane // (hidden * bit)) % 2 == 1
                for x in range(ratio):
                    if x & bit:
                        continue
                    a, b = tiles[x], tiles[x | bit]
                    tiles[x] = jnp.where(upper, pltpu.roll(b, hidden * bit, 1), a)
                    tiles[x | bit] = jnp.where(upper, b, pltpu.roll(a, 128 - hidden * bit, 1))
                bit *= 2
            for x in range(ratio):
                i = g * ratio + x
                rounded = tiles[x].astype(bf16)
                high[i * tokens : (i + 1) * tokens, q * 128 : (q + 1) * 128] = rounded
                low[i * tokens : (i + 1) * tokens, q * 128 : (q + 1) * 128] = (
                    tiles[x] - rounded.astype(f32)
                ).astype(bf16)
    out[...] = jnp.dot(high[...], turned[...], preferred_element_type=f32) + jnp.dot(
        low[...], turned[...], preferred_element_type=f32
    )


def outer_stage(place, lefts, rights, final):
    n = len(lefts)
    t, hidden, s = lefts[0].shape
    tokens, width = n * t, final.shape[1]
    vmem = pl.BlockSpec(memory_space=pltpu.VMEM)
    return pl.pallas_call(
        outer_kernel,
        out_shape=jax.ShapeDtypeStruct((tokens * tokens, width), f32),
        in_specs=[pl.BlockSpec(memory_space=pltpu.SMEM)] + [vmem] * (2 * n + 1),
        out_specs=vmem,
        scratch_shapes=[
            pltpu.VMEM((n, t * hidden, s), bf16),
            pltpu.VMEM((n, t * hidden, s), f32),
            pltpu.VMEM((tokens * hidden, s), f32),
            pltpu.VMEM((hidden * hidden, width), f32),
            pltpu.VMEM((hidden * hidden, width), bf16),
            pltpu.VMEM((tokens * hidden, tokens * hidden), f32),
            pltpu.VMEM((tokens * tokens, hidden * hidden), bf16),
            pltpu.VMEM((tokens * tokens, hidden * hidden), bf16),
        ],
        name="outer_stage",
    )(place, *lefts, *rights, final)


def pair_stage(update, couple, inverse, offset, row_tokens, col_tokens, couple_scale, score, tri_scale, entry, half, parts):
    rows, cols, width = couple.shape
    pair_one = (couple.astype(f32) + update * inverse + offset).astype(bf16)
    value = pair_one.astype(f32)
    average = jnp.mean(value, -1, keepdims=True)
    centred = value - average
    variance = jnp.mean(centred * centred, -1, keepdims=True)
    unit = centred * lax.rsqrt(variance + epsilon)
    logits = jnp.einsum("ijc,ch->ihj", unit * couple_scale, score, precision=lax.Precision.HIGHEST)
    logits = logits + 1000000000.0 * (col_tokens - 1.0)[None, None, :]
    peak = jnp.max(logits, -1)
    expo = jnp.exp(logits - peak[..., None]).astype(bf16).reshape(rows, -1)
    normed = (unit * tri_scale).astype(bf16)
    mine = lax.dynamic_slice_in_dim(
        entry[:, : 4 * width].reshape(width, 4, 2, width // 2), half, 1, 2
    ).reshape(width, 2 * width)
    projected = jnp.einsum("ijz,zc->cij", normed, mine, preferred_element_type=f32)
    projected = projected.reshape(4, width // 2, rows, cols)
    mask = (row_tokens[:, None] * col_tokens[None, :])[None]
    left = (jax.nn.sigmoid(projected[0]) * projected[1] * mask).astype(bf16)
    right = (jax.nn.sigmoid(projected[2]) * projected[3] * mask).astype(bf16)

    def by_peer(operand):
        operand = operand.reshape(parts, -1, rows, cols)
        return operand.transpose(0, 2, 1, 3).reshape(parts, rows, -1)

    left, right = by_peer(left), by_peer(right)
    spare = 128 - left.shape[-1]

    def everyone(piece):
        return jnp.broadcast_to(piece[None], (parts,) + piece.shape)

    stats = jnp.concatenate(split_pieces(peak, 3), -1)
    lanes = stats.shape[-1]
    stats = stats.reshape(rows // 8, 8, lanes).transpose(1, 0, 2).reshape(8, -1)
    stats = jnp.pad(stats, ((0, 0), (0, 128 - stats.shape[-1])))
    block = jnp.concatenate(
        [
            jnp.concatenate([left, everyone(expo[:, 128 : 128 + spare])], -1),
            jnp.concatenate([right, everyone(expo[:, 128 + spare : 128 + 2 * spare])], -1),
            everyone(expo[:, :128]),
            everyone(stats),
        ],
        1,
    )
    return pair_one, block


def middle_stage(block, n, rows, cols, heads, seq_scale, content, sigmoid_matrix, final):
    parts = n * n
    ch = final.shape[1]
    feats = 128 // cols - (1 if (128 // cols) * cols > 96 else 0)
    left = block[:, :rows]
    right = block[:, rows : 2 * rows]
    expo = jnp.concatenate([block[:, 2 * rows : 3 * rows], left[..., feats * cols :], right[..., feats * cols :]], -1)
    stats = block[:, 3 * rows : 3 * rows + 8]
    slab = block[:, 3 * rows + 8 :]

    def whole(operand):
        operand = operand[..., : feats * cols].reshape(n, n, rows, feats, cols)
        return operand.transpose(3, 0, 2, 1, 4).reshape(feats, n * rows, n * cols)

    product = jnp.einsum("fik,fjk->fij", whole(left), whole(right), preferred_element_type=f32)
    product = product.astype(bf16).reshape(feats, n, rows, n, cols)
    product = product.transpose(1, 3, 2, 0, 4).reshape(parts, rows, feats * cols)
    product = jnp.pad(product, ((0, 0), (0, 0), (0, 128 - feats * cols)))
    stats = stats[..., : rows // 8 * 3 * heads].reshape(parts, 8, rows // 8, 3, heads)
    peak = stats.astype(f32).sum(3).transpose(0, 2, 1, 3).reshape(n, n, rows, heads)
    expo = expo.reshape(n, n, rows, heads, cols).astype(f32)
    top = jnp.max(peak, 1, keepdims=True)
    factor = jnp.exp(peak - top)
    total = jnp.sum(factor * jnp.sum(expo, -1), 1, keepdims=True)
    weights = (expo * (factor / total)[..., None]).astype(bf16)
    weights = weights.transpose(3, 0, 2, 1, 4).reshape(heads, n * rows, n * cols)
    groups = slab.shape[1] // 8
    tokens = slab.reshape(parts, groups, 8, 128 // ch, ch).transpose(2, 0, 1, 3, 4).reshape(8, n * rows, ch)
    normed = standardize_features(tokens, seq_scale).astype(bf16)
    values = jnp.dot(normed, content, preferred_element_type=f32).astype(bf16)
    gates = jax.nn.sigmoid(jnp.dot(normed, sigmoid_matrix, preferred_element_type=f32))
    values = values.reshape(8, n * rows, heads, -1)
    averaged = jnp.einsum("hij,sjhe->sihe", weights, values, preferred_element_type=f32)
    gated = gates * averaged.reshape(8, n * rows, -1)
    delta = jnp.dot(gated, final.astype(f32), precision=lax.Precision.HIGHEST)
    revised = (tokens.astype(f32) + delta).astype(bf16)
    revised = revised.reshape(8, parts, groups, 128 // ch, ch).transpose(1, 2, 0, 3, 4)
    revised = revised.reshape(parts, groups * 8, 128)
    return jnp.concatenate([product, revised], 1)


def final_stage(product, pair_one, tri_scale, entry, result_scale, final):
    rows, cols, width = pair_one.shape
    depth, parts = product.shape[:2]
    feats = width // (depth * parts)
    product = product[..., : feats * cols].reshape(depth, parts, rows, feats, cols)
    product = product.transpose(2, 4, 0, 1, 3).reshape(rows, cols, width)
    normed = standardize_features(pair_one, tri_scale).astype(bf16)
    gate = jax.nn.sigmoid(jnp.dot(normed, entry[:, 4 * width :], preferred_element_type=f32))
    final = gate * jnp.dot(
        standardize_features(product, result_scale).astype(bf16), final, preferred_element_type=f32
    )
    return (pair_one.astype(f32) + final).astype(bf16)


def on_device(
    sequence_stack,
    present_sequence_flags,
    genuine_residue_flags,
    couple_state,
    tensor_scale,
    tensor_entry_matrix,
    tensor_final_matrix,
    tensor_offset,
    mean_sequence_scale,
    mean_couple_scale,
    mean_score_matrix,
    mean_content_matrix,
    mean_sigmoid_matrix,
    mean_final_matrix,
    trimul_scale,
    trimul_entry_matrix,
    trimul_result_scale,
    trimul_final_matrix,
):
    n = lax.axis_size("row")
    parts = n * n
    row_index = lax.axis_index("row")
    col_index = lax.axis_index("col")
    half = lax.axis_index("depth")
    rows, cols, width = couple_state.shape
    count, t, ch = sequence_stack.shape
    hidden = tensor_entry_matrix.shape[1] // 2
    heads = mean_score_matrix.shape[1]
    token_weight = genuine_residue_flags.astype(f32)
    flags = present_sequence_flags.astype(f32)
    inverse = 1.0 / (jnp.sum(flags) + 0.001)
    my_flags = lax.dynamic_slice_in_dim(flags, half * count, count)
    tokens = sequence_stack.transpose(1, 2, 0)
    factors = factor_stage(tokens, my_flags, tensor_scale, tensor_entry_matrix)
    left, right = factors[:, :hidden], factors[:, hidden:]

    def move(array, where):
        pairs = [(r * n + c, where(r, c)[0] * n + where(r, c)[1]) for r in range(n) for c in range(n)]
        return lax.ppermute(array, ("row", "col"), pairs)

    lefts = [left] + [move(left, lambda r, c, k=k: (r, (c + k) % n)) for k in range(1, n)]
    rights = [move(right, lambda r, c, k=k: ((c + k) % n, r)) for k in range(n)]
    place = jnp.stack([(col_index - k) % n for k in range(n)] + [(row_index - k) % n for k in range(n)])
    update = outer_stage(place.astype(jnp.int32), lefts, rights, tensor_final_matrix)
    update = update + lax.ppermute(update, "depth", [(0, 1), (1, 0)])
    row_tokens = lax.dynamic_slice_in_dim(token_weight, row_index * rows, rows)
    col_tokens = lax.dynamic_slice_in_dim(token_weight, col_index * cols, cols)
    pair_one, block = pair_stage(
        update.reshape(rows, cols, width), couple_state, inverse, tensor_offset, row_tokens, col_tokens, mean_couple_scale,
        mean_score_matrix, trimul_scale, trimul_entry_matrix, half, parts,
    )
    slab = sequence_stack.reshape(parts, 8, t * ch // 128, 128).transpose(0, 2, 1, 3)
    slab = slab.reshape(parts, -1, 128)
    block = lax.all_to_all(jnp.concatenate([block, slab], 1), ("row", "col"), 0, 0, tiled=True)
    block = middle_stage(
        block, n, rows, cols, heads, mean_sequence_scale, mean_content_matrix, mean_sigmoid_matrix,
        mean_final_matrix,
    )
    block = lax.all_to_all(block, ("row", "col"), 0, 0, tiled=True)
    product = block[:, :rows]
    other = lax.ppermute(product, "depth", [(0, 1), (1, 0)])
    first = half == 0
    product = jnp.stack([jnp.where(first, product, other), jnp.where(first, other, product)])
    revised = block[:, rows:].reshape(parts, t * ch // 128, 8, 128).transpose(0, 2, 1, 3)
    revised = revised.reshape(count, t, ch)
    pair_output = final_stage(
        product, pair_one, trimul_scale, trimul_entry_matrix, trimul_result_scale, trimul_final_matrix
    )
    return (revised, pair_output)


def suits(mesh):
    return mesh.shape["row"] == mesh.shape["col"] and mesh.shape["depth"] == 2


def solution(mesh):
    placed = (P("depth", ("row", "col"), None), P(), P(), P("row", "col", None)) + (P(),) * 14
    return jax.shard_map(
        on_device if suits(mesh) else on_device_generic,
        mesh=mesh,
        in_specs=placed,
        out_specs=(P("depth", ("row", "col"), None), P("row", "col", None)),
        check_vma=False,
    )
```

```python
import functools

import jax
import jax.numpy as jnp
from jax import lax
from jax.experimental import pallas as pl
from jax.experimental.pallas import tpu as pltpu
from jax.sharding import PartitionSpec as P

epsilon = 1e-05
bf16 = jnp.bfloat16
f32 = jnp.float32


def from_root(array, axis, root):
    mine = lax.axis_index(axis) == root
    return lax.psum(jnp.where(mine, array, jnp.zeros_like(array)), axis)


def standardize_features(value_rows, scale):
    value_rows = value_rows.astype(jnp.float32)
    average = jnp.mean(value_rows, -1, keepdims=True)
    centred = value_rows - average
    variance = jnp.mean(centred * centred, -1, keepdims=True)
    return centred * lax.rsqrt(variance + epsilon) * scale


def on_device_generic(
    sequence_stack,
    present_sequence_flags,
    genuine_residue_flags,
    couple_state,
    tensor_scale,
    tensor_entry_matrix,
    tensor_final_matrix,
    tensor_offset,
    mean_sequence_scale,
    mean_couple_scale,
    mean_score_matrix,
    mean_content_matrix,
    mean_sigmoid_matrix,
    mean_final_matrix,
    trimul_scale,
    trimul_entry_matrix,
    trimul_result_scale,
    trimul_final_matrix,
):
    n_row = lax.axis_size("row")
    n_col = lax.axis_size("col")
    row_index = lax.axis_index("row")
    col_index = lax.axis_index("col")
    depth_position = lax.axis_index("depth")
    piece_rows, piece_columns, width = couple_state.shape
    sequence_count, shard_residues, ignored_quantity = sequence_stack.shape
    hidden = tensor_entry_matrix.shape[1] // 2
    head_split = mean_score_matrix.shape[1]
    head_channels = mean_content_matrix.shape[1] // head_split
    token_weight = genuine_residue_flags.astype(jnp.float32)
    mask_as_float = present_sequence_flags.astype(jnp.float32)
    row_softmax_weight = lax.dynamic_slice_in_dim(
        mask_as_float, depth_position * sequence_count, sequence_count
    )
    row_count = jnp.sum(mask_as_float)
    entire_sequences = lax.all_gather(sequence_stack, "col", axis=1, tiled=True)
    root_row = col_index * n_row // n_col
    offset = col_index * piece_columns - root_row * piece_rows
    column_piece = lax.dynamic_slice_in_dim(entire_sequences, offset, piece_columns, 1)
    whole_cols = from_root(column_piece, "row", root_row)
    opm_rows = standardize_features(entire_sequences, tensor_scale).astype(jnp.bfloat16)
    opm_cols = standardize_features(whole_cols, tensor_scale).astype(jnp.bfloat16)
    left_projection = (
        jnp.dot(opm_rows, tensor_entry_matrix[:, :hidden], preferred_element_type=jnp.float32)
        * row_softmax_weight[:, None, None]
    ).astype(jnp.bfloat16)
    right_proj = (
        jnp.dot(opm_cols, tensor_entry_matrix[:, hidden:], preferred_element_type=jnp.float32)
        * row_softmax_weight[:, None, None]
    ).astype(jnp.bfloat16)
    outer_sum = jnp.einsum(
        "sic,sjd->ijcd", left_projection, right_proj, preferred_element_type=jnp.float32
    )
    outer_sum = outer_sum.reshape(piece_rows, piece_columns, hidden * hidden)
    out_float = tensor_final_matrix.astype(jnp.float32)
    outer_share = lax.psum_scatter(outer_sum, "depth", scatter_dimension=0, tiled=True)
    share_rows = outer_share.shape[0]
    pair_share = lax.dynamic_slice_in_dim(couple_state, depth_position * share_rows, share_rows, 0)
    update = (
        jnp.dot(outer_share, out_float, precision=lax.Precision.HIGHEST) / (row_count + 0.001)
        + tensor_offset
    )
    new_share = (pair_share.astype(jnp.float32) + update).astype(jnp.bfloat16)
    pair_one = lax.all_gather(new_share, "depth", axis=0, tiled=True)
    row_tokens = lax.dynamic_slice_in_dim(token_weight, row_index * piece_rows, piece_rows)
    col_tokens = lax.dynamic_slice_in_dim(token_weight, col_index * piece_columns, piece_columns)
    logits = jnp.einsum(
        "ijc,ch->ijh",
        standardize_features(pair_one, mean_couple_scale),
        mean_score_matrix,
        precision=lax.Precision.HIGHEST,
    )
    logits = logits + 1000000000.0 * (col_tokens - 1.0)[None, :, None]
    peak = lax.pmax(jnp.max(logits, axis=1), "col")
    expo = jnp.exp(logits - peak[:, None, :])
    total = lax.psum(jnp.sum(expo, axis=1), "col")
    weights = (expo / total[:, None, :]).astype(jnp.bfloat16)
    col_normed = standardize_features(whole_cols, mean_sequence_scale).astype(jnp.bfloat16)
    value_rows = jnp.dot(
        col_normed, mean_content_matrix, preferred_element_type=jnp.float32
    ).astype(jnp.bfloat16)
    value_rows = value_rows.reshape(sequence_count, piece_columns, head_split, head_channels)
    averaged_values = jnp.einsum(
        "ijh,sjhe->sihe", weights, value_rows, preferred_element_type=jnp.float32
    )
    averaged_values = averaged_values.reshape(
        sequence_count, piece_rows, head_split * head_channels
    )
    output_weight = mean_final_matrix.astype(jnp.float32)
    local_portion = lax.psum_scatter(
        averaged_values.astype(jnp.bfloat16), "col", scatter_dimension=1, tiled=True
    ).astype(jnp.float32)
    shard_standardized = standardize_features(sequence_stack, mean_sequence_scale).astype(
        jnp.bfloat16
    )
    gate_values = jax.nn.sigmoid(
        jnp.dot(shard_standardized, mean_sigmoid_matrix, preferred_element_type=jnp.float32)
    )
    sequence_delta = jnp.dot(
        gate_values * local_portion, output_weight, precision=lax.Precision.HIGHEST
    )
    revised_sequences = (sequence_stack.astype(jnp.float32) + sequence_delta).astype(jnp.bfloat16)
    tri_normed = standardize_features(pair_one, trimul_scale).astype(jnp.bfloat16)
    projected = jnp.dot(tri_normed, trimul_entry_matrix, preferred_element_type=jnp.float32)
    pair_mask = (row_tokens[:, None] * col_tokens[None, :])[..., None]
    tri_left = (
        jax.nn.sigmoid(projected[..., 0:width]) * projected[..., width : 2 * width] * pair_mask
    ).astype(jnp.bfloat16)
    tri_right = (
        jax.nn.sigmoid(projected[..., 2 * width : 3 * width])
        * projected[..., 3 * width : 4 * width]
        * pair_mask
    ).astype(jnp.bfloat16)
    out_gate = jax.nn.sigmoid(projected[..., 4 * width : 5 * width])
    left_rows, right_rows = (
        lax.all_gather(tri_left, "col", axis=1, tiled=True),
        lax.all_gather(tri_right, "col", axis=1, tiled=True),
    )
    right_piece = lax.dynamic_slice_in_dim(right_rows, offset, piece_columns, 0)
    right_needed = from_root(right_piece, "row", root_row)
    product = jnp.einsum(
        "ikc,jkc->ijc", left_rows, right_needed, preferred_element_type=jnp.float32
    )
    final = out_gate * jnp.dot(
        standardize_features(product, trimul_result_scale).astype(jnp.bfloat16),
        trimul_final_matrix,
        preferred_element_type=jnp.float32,
    )
    pair_output = (pair_one.astype(jnp.float32) + final).astype(jnp.bfloat16)
    return (revised_sequences, pair_output)


def split_pieces(value, count):
    pieces = []
    for _ in range(count):
        piece = lax.reduce_precision(value, 8, 7)
        pieces.append(piece.astype(bf16))
        value = value - piece
    return pieces


def factor_stage(tokens, flags, scale, entry):
    value = tokens.astype(f32)
    average = jnp.mean(value, 1, keepdims=True)
    centred = value - average
    variance = jnp.mean(centred * centred, 1, keepdims=True)
    normed = (centred * lax.rsqrt(variance + epsilon) * scale[None, :, None]).astype(bf16)
    factors = jnp.einsum("tcs,cf->tfs", normed, entry, preferred_element_type=f32)
    return (factors * flags[None, None, :]).astype(bf16)


def outer_kernel(place, *refs):
    n, t, hidden = place.shape[0] // 2, refs[0].shape[0], refs[0].shape[1]
    s = refs[0].shape[2]
    lefts, rights = refs[:n], refs[n : 2 * n]
    final, out, left, pieces, right, plain, turned, outer, high, low = refs[2 * n :]
    tokens, ratio = n * t, 128 // hidden
    for k in range(n):
        left[place[k]] = lefts[k][...].reshape(t * hidden, s)
        pieces[place[n + k]] = rights[k][...].reshape(t * hidden, s).astype(f32)
    for k in range(n):
        for u in range(t):
            right[pl.ds(k * t + u, hidden, stride=tokens), :] = pieces[k, u * hidden : (u + 1) * hidden, :]
    plain[...] = final[...].astype(f32)
    for d in range(hidden):
        turned[d * hidden : (d + 1) * hidden, :] = plain[pl.ds(d, hidden, stride=hidden), :].astype(bf16)
    outer[...] = lax.dot_general(
        right[...].astype(bf16),
        left[...].reshape(tokens * hidden, s),
        (((1,), (1,)), ((), ())),
        preferred_element_type=f32,
    )
    lane = lax.broadcasted_iota(jnp.int32, (tokens, 128), 1)
    for g in range(tokens // ratio):
        for q in range(hidden // ratio):
            tiles = [
                outer[(q * ratio + d) * tokens : (q * ratio + d + 1) * tokens, g * 128 : (g + 1) * 128]
                for d in range(ratio)
            ]
            bit = 1
            while bit < ratio:
                upper = (lane // (hidden * bit)) % 2 == 1
                for x in range(ratio):
                    if x & bit:
                        continue
                    a, b = tiles[x], tiles[x | bit]
                    tiles[x] = jnp.where(upper, pltpu.roll(b, hidden * bit, 1), a)
                    tiles[x | bit] = jnp.where(upper, b, pltpu.roll(a, 128 - hidden * bit, 1))
                bit *= 2
            for x in range(ratio):
                i = g * ratio + x
                rounded = tiles[x].astype(bf16)
                high[i * tokens : (i + 1) * tokens, q * 128 : (q + 1) * 128] = rounded
                low[i * tokens : (i + 1) * tokens, q * 128 : (q + 1) * 128] = (
                    tiles[x] - rounded.astype(f32)
                ).astype(bf16)
    out[...] = jnp.dot(high[...], turned[...], preferred_element_type=f32) + jnp.dot(
        low[...], turned[...], preferred_element_type=f32
    )


def outer_stage(place, lefts, rights, final):
    n = len(lefts)
    t, hidden, s = lefts[0].shape
    tokens, width = n * t, final.shape[1]
    vmem = pl.BlockSpec(memory_space=pltpu.VMEM)
    return pl.pallas_call(
        outer_kernel,
        out_shape=jax.ShapeDtypeStruct((tokens * tokens, width), f32),
        in_specs=[pl.BlockSpec(memory_space=pltpu.SMEM)] + [vmem] * (2 * n + 1),
        out_specs=vmem,
        scratch_shapes=[
            pltpu.VMEM((n, t * hidden, s), bf16),
            pltpu.VMEM((n, t * hidden, s), f32),
            pltpu.VMEM((tokens * hidden, s), f32),
            pltpu.VMEM((hidden * hidden, width), f32),
            pltpu.VMEM((hidden * hidden, width), bf16),
            pltpu.VMEM((tokens * hidden, tokens * hidden), f32),
            pltpu.VMEM((tokens * tokens, hidden * hidden), bf16),
            pltpu.VMEM((tokens * tokens, hidden * hidden), bf16),
        ],
        name="outer_stage",
    )(place, *lefts, *rights, final)


def pair_stage(update, couple, inverse, offset, row_tokens, col_tokens, couple_scale, score, tri_scale, entry, half, parts):
    rows, cols, width = couple.shape
    pair_one = (couple.astype(f32) + update * inverse + offset).astype(bf16)
    value = pair_one.astype(f32)
    average = jnp.mean(value, -1, keepdims=True)
    centred = value - average
    variance = jnp.mean(centred * centred, -1, keepdims=True)
    unit = centred * lax.rsqrt(variance + epsilon)
    logits = jnp.einsum("ijc,ch->ihj", unit * couple_scale, score, precision=lax.Precision.HIGHEST)
    logits = logits + 1000000000.0 * (col_tokens - 1.0)[None, None, :]
    peak = jnp.max(logits, -1)
    expo = jnp.exp(logits - peak[..., None]).astype(bf16).reshape(rows, -1)
    normed = (unit * tri_scale).astype(bf16)
    mine = lax.dynamic_slice_in_dim(
        entry[:, : 4 * width].reshape(width, 4, 2, width // 2), half, 1, 2
    ).reshape(width, 2 * width)
    projected = jnp.einsum("ijz,zc->cij", normed, mine, preferred_element_type=f32)
    projected = projected.reshape(4, width // 2, rows, cols)
    mask = (row_tokens[:, None] * col_tokens[None, :])[None]
    left = (jax.nn.sigmoid(projected[0]) * projected[1] * mask).astype(bf16)
    right = (jax.nn.sigmoid(projected[2]) * projected[3] * mask).astype(bf16)

    def by_peer(operand):
        operand = operand.reshape(parts, -1, rows, cols)
        return operand.transpose(0, 2, 1, 3).reshape(parts, rows, -1)

    left, right = by_peer(left), by_peer(right)
    spare = 128 - left.shape[-1]

    def everyone(piece):
        return jnp.broadcast_to(piece[None], (parts,) + piece.shape)

    stats = jnp.concatenate(split_pieces(peak, 3), -1)
    lanes = stats.shape[-1]
    stats = stats.reshape(rows // 8, 8, lanes).transpose(1, 0, 2).reshape(8, -1)
    stats = jnp.pad(stats, ((0, 0), (0, 128 - stats.shape[-1])))
    block = jnp.concatenate(
        [
            jnp.concatenate([left, everyone(expo[:, 128 : 128 + spare])], -1),
            jnp.concatenate([right, everyone(expo[:, 128 + spare : 128 + 2 * spare])], -1),
            everyone(expo[:, :128]),
            everyone(stats),
        ],
        1,
    )
    return pair_one, block


def halves(value):
    high = value.astype(bf16)
    return high, (value - high.astype(f32)).astype(bf16)


def two_pass_dot(value, matrix, axis=0):
    high, low = halves(value)
    over = (((1,), (axis,)), ((), ()))
    return lax.dot_general(high, matrix, over, preferred_element_type=f32) + lax.dot_general(
        low, matrix, over, preferred_element_type=f32
    )


def middle_kernel(sizes, block, seq_scale, content, sigmoid_matrix, final, out, wide, lhs, rhs, product, weights, x, values, gated, masked, revised):
    n, rows, cols, heads, feats, groups, order = sizes
    parts, tokens, ch = n * n, n * rows, final.shape[0]
    s, per = 8, 128 // final.shape[0]
    t = rows // n
    wide[...] = block[...].astype(f32)
    lane = lax.broadcasted_iota(jnp.int32, (tokens, 128), 1)
    small = lax.broadcasted_iota(jnp.int32, (rows, 128), 1)
    tiny = lax.broadcasted_iota(jnp.int32, (8, 128), 1)
    spare = 128 - feats * cols

    def stacked(c, start, count):
        return jnp.concatenate([wide[r * n + c, start : start + count] for r in range(n)], 0)

    rhs[...] = jnp.zeros_like(rhs)
    for c in range(n):
        mine = stacked(c, 0, rows)
        for f in range(feats):
            keep = (lane >= f * cols) & (lane < (f + 1) * cols)
            lhs[f * tokens : (f + 1) * tokens, c * 128 : (c + 1) * 128] = jnp.where(keep, mine, 0.0).astype(bf16)
        rhs[:tokens, c * 128 : (c + 1) * 128] = stacked(c, rows, rows).astype(bf16)
    product[...] = lax.dot_general(lhs[...], rhs[...], (((1,), (1,)), ((), ())), preferred_element_type=f32)
    up = lax.broadcasted_iota(jnp.int32, (256, 128), 0)
    across = lax.broadcasted_iota(jnp.int32, (256, 128), 1)
    gather = ((up >= across * cols) & (up < (across + 1) * cols) & (across < heads)).astype(bf16)
    up = lax.broadcasted_iota(jnp.int32, (128, 256), 0)
    across = lax.broadcasted_iota(jnp.int32, (128, 256), 1)
    spread = ((across >= up * cols) & (across < (up + 1) * cols) & (up < heads)).astype(bf16)
    expos, peaks = [], []
    for c in range(n):
        a, b = stacked(c, 0, rows), stacked(c, rows, rows)
        rest = jnp.where(lane < spare, pltpu.roll(a, spare, 1), jnp.where(lane < 2 * spare, pltpu.roll(b, 2 * spare, 1), 0.0))
        expos.append(jnp.concatenate([stacked(c, 2 * rows, rows), rest], 1))
        peak = []
        for r in range(n):
            stats = wide[r * n + c, 3 * rows : 3 * rows + 8]
            for q in range(rows // 8):
                one = pltpu.roll(stats, (128 - 3 * heads * q) % 128, 1) if q else stats
                peak.append(one + pltpu.roll(one, 128 - heads, 1) + pltpu.roll(one, 128 - 2 * heads, 1))
        peaks.append(jnp.concatenate(peak, 0))
    top = peaks[0]
    for c in range(1, n):
        top = jnp.maximum(top, peaks[c])
    factors = [jnp.exp(peak - top) for peak in peaks]
    total = jnp.zeros_like(top)
    for c in range(n):
        total = total + factors[c] * jnp.dot(expos[c].astype(bf16), gather, preferred_element_type=f32)
    for c in range(n):
        scale = jnp.where(lane < heads, factors[c] / jnp.where(lane < heads, total, 1.0), 0.0)
        weights[:, c * 256 : (c + 1) * 256] = (expos[c] * two_pass_dot(scale, spread)).astype(bf16)
    for p in range(parts):
        for g in range(groups):
            pair = wide[p, 3 * rows + 8 + 8 * g : 3 * rows + 16 + 8 * g]
            for k in range(per):
                x[pl.ds(p * t + g * per + k, s, stride=tokens), :] = pltpu.roll(pair, 128 - k * ch, 1) if k else pair
    raw = x[...][:, :ch]
    centred = raw - jnp.mean(raw, -1, keepdims=True)
    variance = jnp.mean(centred * centred, -1, keepdims=True)
    normed = (centred * lax.rsqrt(variance + epsilon) * seq_scale[...]).astype(bf16)
    values[...] = jnp.dot(normed, content[...], preferred_element_type=f32).astype(bf16).astype(f32)
    gates = jax.nn.sigmoid(jnp.dot(normed, sigmoid_matrix[...], preferred_element_type=f32))
    width = gates.shape[1]
    head_of = lax.broadcasted_iota(jnp.int32, (cols, width), 1) // (width // heads)
    used = heads * cols
    masked[...] = jnp.zeros_like(masked)
    for q in range(s):
        for c in range(n):
            local = jnp.concatenate([values[q * tokens + a : q * tokens + a + m] for a, m in order[c]], 0)
            spread_out = jnp.concatenate([jnp.where(head_of == h, local, 0.0) for h in range(heads)], 0)
            masked[q, c * 256 : c * 256 + used] = spread_out.astype(bf16)
        averaged = jnp.dot(weights[...], masked[q], preferred_element_type=f32)
        gated[q * tokens : (q + 1) * tokens] = gates[q * tokens : (q + 1) * tokens] * averaged
    delta = two_pass_dot(gated[...], final[...], 1)
    revised[:, :ch] = raw + delta
    for p in range(parts):
        r, c = p // n, p % n
        slab = jnp.zeros((rows, 128), f32)
        for f in range(feats):
            shift = ((f - c) * cols) % 128
            piece = product[f * tokens + r * rows : f * tokens + (r + 1) * rows]
            piece = pltpu.roll(piece, shift, 1) if shift else piece
            slab = jnp.where((small >= f * cols) & (small < (f + 1) * cols), piece, slab)
        slabs = [slab]
        for g in range(groups):
            merged = revised[pl.ds(p * t + g * per, s, stride=tokens), :]
            for k in range(1, per):
                piece = revised[pl.ds(p * t + g * per + k, s, stride=tokens), :]
                merged = jnp.where(tiny >= k * ch, pltpu.roll(piece, k * ch, 1), merged)
            slabs.append(merged)
        out[p] = jnp.concatenate(slabs, 0).astype(bf16)


def middle_stage(block, n, rows, cols, heads, feats, order, seq_scale, content, sigmoid_matrix, final):
    parts, tokens = n * n, n * rows
    groups = (block.shape[1] - 3 * rows - 8) // 8
    width = content.shape[1]
    vmem = pl.BlockSpec(memory_space=pltpu.VMEM)
    return pl.pallas_call(
        functools.partial(middle_kernel, (n, rows, cols, heads, feats, groups, order)),
        out_shape=jax.ShapeDtypeStruct((parts, rows + 8 * groups, 128), bf16),
        in_specs=[vmem] * 5,
        out_specs=vmem,
        scratch_shapes=[
            pltpu.VMEM(block.shape, f32),
            pltpu.VMEM((feats * tokens, n * 128), bf16),
            pltpu.VMEM((128, n * 128), bf16),
            pltpu.VMEM((feats * tokens, 128), f32),
            pltpu.VMEM((tokens, n * 256), bf16),
            pltpu.VMEM((8 * tokens, 128), f32),
            pltpu.VMEM((8 * tokens, width), f32),
            pltpu.VMEM((8 * tokens, width), f32),
            pltpu.VMEM((8, n * 256, width), bf16),
            pltpu.VMEM((8 * tokens, 128), f32),
        ],
        name="middle_stage",
    )(block, seq_scale.reshape(1, -1), content, sigmoid_matrix, final.T)


def final_stage(product, pair_one, tri_scale, entry, result_scale, final):
    rows, cols, width = pair_one.shape
    depth, parts = product.shape[:2]
    feats = width // (depth * parts)
    product = product[..., : feats * cols].reshape(depth, parts, rows, feats, cols)
    product = product.transpose(2, 4, 0, 1, 3).reshape(rows, cols, width)
    normed = standardize_features(pair_one, tri_scale).astype(bf16)
    gate = jax.nn.sigmoid(jnp.dot(normed, entry[:, 4 * width :], preferred_element_type=f32))
    final = gate * jnp.dot(
        standardize_features(product, result_scale).astype(bf16), final, preferred_element_type=f32
    )
    return (pair_one.astype(f32) + final).astype(bf16)


def on_device(
    sequence_stack,
    present_sequence_flags,
    genuine_residue_flags,
    couple_state,
    tensor_scale,
    tensor_entry_matrix,
    tensor_final_matrix,
    tensor_offset,
    mean_sequence_scale,
    mean_couple_scale,
    mean_score_matrix,
    mean_content_matrix,
    mean_sigmoid_matrix,
    mean_final_matrix,
    trimul_scale,
    trimul_entry_matrix,
    trimul_result_scale,
    trimul_final_matrix,
):
    n = lax.axis_size("row")
    parts = n * n
    row_index = lax.axis_index("row")
    col_index = lax.axis_index("col")
    half = lax.axis_index("depth")
    rows, cols, width = couple_state.shape
    count, t, ch = sequence_stack.shape
    hidden = tensor_entry_matrix.shape[1] // 2
    heads = mean_score_matrix.shape[1]
    feats = width // (2 * parts)
    order = tuple(((c * cols, cols),) for c in range(n))
    token_weight = genuine_residue_flags.astype(f32)
    flags = present_sequence_flags.astype(f32)
    inverse = 1.0 / (jnp.sum(flags) + 0.001)
    my_flags = lax.dynamic_slice_in_dim(flags, half * count, count)
    tokens = sequence_stack.transpose(1, 2, 0)
    factors = factor_stage(tokens, my_flags, tensor_scale, tensor_entry_matrix)
    left, right = factors[:, :hidden], factors[:, hidden:]

    def move(array, where):
        pairs = [(r * n + c, where(r, c)[0] * n + where(r, c)[1]) for r in range(n) for c in range(n)]
        return lax.ppermute(array, ("row", "col"), pairs)

    lefts = [left] + [move(left, lambda r, c, k=k: (r, (c + k) % n)) for k in range(1, n)]
    rights = [move(right, lambda r, c, k=k: ((c + k) % n, r)) for k in range(n)]
    place = jnp.stack([(col_index - k) % n for k in range(n)] + [(row_index - k) % n for k in range(n)])
    update = outer_stage(place.astype(jnp.int32), lefts, rights, tensor_final_matrix)
    update = update + lax.ppermute(update, "depth", [(0, 1), (1, 0)])
    row_tokens = lax.dynamic_slice_in_dim(token_weight, row_index * rows, rows)
    col_tokens = lax.dynamic_slice_in_dim(token_weight, col_index * cols, cols)
    pair_one, block = pair_stage(
        update.reshape(rows, cols, width), couple_state, inverse, tensor_offset, row_tokens, col_tokens, mean_couple_scale,
        mean_score_matrix, trimul_scale, trimul_entry_matrix, half, parts,
    )
    slab = sequence_stack.reshape(parts, 8, t * ch // 128, 128).transpose(0, 2, 1, 3)
    slab = slab.reshape(parts, -1, 128)
    block = lax.all_to_all(jnp.concatenate([block, slab], 1), ("row", "col"), 0, 0, tiled=True)
    block = middle_stage(
        block, n, rows, cols, heads, feats, order, mean_sequence_scale, mean_content_matrix, mean_sigmoid_matrix,
        mean_final_matrix,
    )
    block = lax.all_to_all(block, ("row", "col"), 0, 0, tiled=True)
    product = block[:, :rows]
    other = lax.ppermute(product, "depth", [(0, 1), (1, 0)])
    first = half == 0
    product = jnp.stack([jnp.where(first, product, other), jnp.where(first, other, product)])
    revised = block[:, rows:].reshape(parts, t * ch // 128, 8, 128).transpose(0, 2, 1, 3)
    revised = revised.reshape(count, t, ch)
    pair_output = final_stage(
        product, pair_one, trimul_scale, trimul_entry_matrix, trimul_result_scale, trimul_final_matrix
    )
    return (revised, pair_output)


def suits(mesh):
    return mesh.shape["row"] == mesh.shape["col"] and mesh.shape["depth"] == 2


def solution(mesh):
    placed = (P("depth", ("row", "col"), None), P(), P(), P("row", "col", None)) + (P(),) * 14
    return jax.shard_map(
        on_device if suits(mesh) else on_device_generic,
        mesh=mesh,
        in_specs=placed,
        out_specs=(P("depth", ("row", "col"), None), P("row", "col", None)),
        check_vma=False,
    )
```

```python
import functools

import jax
import jax.numpy as jnp
from jax import lax
from jax.experimental import pallas as pl
from jax.experimental.pallas import tpu as pltpu
from jax.sharding import PartitionSpec as P

epsilon = 1e-05
bf16 = jnp.bfloat16
f32 = jnp.float32


def from_root(array, axis, root):
    mine = lax.axis_index(axis) == root
    return lax.psum(jnp.where(mine, array, jnp.zeros_like(array)), axis)


def standardize_features(value_rows, scale):
    value_rows = value_rows.astype(jnp.float32)
    average = jnp.mean(value_rows, -1, keepdims=True)
    centred = value_rows - average
    variance = jnp.mean(centred * centred, -1, keepdims=True)
    return centred * lax.rsqrt(variance + epsilon) * scale


def on_device_generic(
    sequence_stack,
    present_sequence_flags,
    genuine_residue_flags,
    couple_state,
    tensor_scale,
    tensor_entry_matrix,
    tensor_final_matrix,
    tensor_offset,
    mean_sequence_scale,
    mean_couple_scale,
    mean_score_matrix,
    mean_content_matrix,
    mean_sigmoid_matrix,
    mean_final_matrix,
    trimul_scale,
    trimul_entry_matrix,
    trimul_result_scale,
    trimul_final_matrix,
):
    n_row = lax.axis_size("row")
    n_col = lax.axis_size("col")
    row_index = lax.axis_index("row")
    col_index = lax.axis_index("col")
    depth_position = lax.axis_index("depth")
    piece_rows, piece_columns, width = couple_state.shape
    sequence_count, shard_residues, ignored_quantity = sequence_stack.shape
    hidden = tensor_entry_matrix.shape[1] // 2
    head_split = mean_score_matrix.shape[1]
    head_channels = mean_content_matrix.shape[1] // head_split
    token_weight = genuine_residue_flags.astype(jnp.float32)
    mask_as_float = present_sequence_flags.astype(jnp.float32)
    row_softmax_weight = lax.dynamic_slice_in_dim(
        mask_as_float, depth_position * sequence_count, sequence_count
    )
    row_count = jnp.sum(mask_as_float)
    entire_sequences = lax.all_gather(sequence_stack, "col", axis=1, tiled=True)
    root_row = col_index * n_row // n_col
    offset = col_index * piece_columns - root_row * piece_rows
    column_piece = lax.dynamic_slice_in_dim(entire_sequences, offset, piece_columns, 1)
    whole_cols = from_root(column_piece, "row", root_row)
    opm_rows = standardize_features(entire_sequences, tensor_scale).astype(jnp.bfloat16)
    opm_cols = standardize_features(whole_cols, tensor_scale).astype(jnp.bfloat16)
    left_projection = (
        jnp.dot(opm_rows, tensor_entry_matrix[:, :hidden], preferred_element_type=jnp.float32)
        * row_softmax_weight[:, None, None]
    ).astype(jnp.bfloat16)
    right_proj = (
        jnp.dot(opm_cols, tensor_entry_matrix[:, hidden:], preferred_element_type=jnp.float32)
        * row_softmax_weight[:, None, None]
    ).astype(jnp.bfloat16)
    outer_sum = jnp.einsum(
        "sic,sjd->ijcd", left_projection, right_proj, preferred_element_type=jnp.float32
    )
    outer_sum = outer_sum.reshape(piece_rows, piece_columns, hidden * hidden)
    out_float = tensor_final_matrix.astype(jnp.float32)
    outer_share = lax.psum_scatter(outer_sum, "depth", scatter_dimension=0, tiled=True)
    share_rows = outer_share.shape[0]
    pair_share = lax.dynamic_slice_in_dim(couple_state, depth_position * share_rows, share_rows, 0)
    update = (
        jnp.dot(outer_share, out_float, precision=lax.Precision.HIGHEST) / (row_count + 0.001)
        + tensor_offset
    )
    new_share = (pair_share.astype(jnp.float32) + update).astype(jnp.bfloat16)
    pair_one = lax.all_gather(new_share, "depth", axis=0, tiled=True)
    row_tokens = lax.dynamic_slice_in_dim(token_weight, row_index * piece_rows, piece_rows)
    col_tokens = lax.dynamic_slice_in_dim(token_weight, col_index * piece_columns, piece_columns)
    logits = jnp.einsum(
        "ijc,ch->ijh",
        standardize_features(pair_one, mean_couple_scale),
        mean_score_matrix,
        precision=lax.Precision.HIGHEST,
    )
    logits = logits + 1000000000.0 * (col_tokens - 1.0)[None, :, None]
    peak = lax.pmax(jnp.max(logits, axis=1), "col")
    expo = jnp.exp(logits - peak[:, None, :])
    total = lax.psum(jnp.sum(expo, axis=1), "col")
    weights = (expo / total[:, None, :]).astype(jnp.bfloat16)
    col_normed = standardize_features(whole_cols, mean_sequence_scale).astype(jnp.bfloat16)
    value_rows = jnp.dot(
        col_normed, mean_content_matrix, preferred_element_type=jnp.float32
    ).astype(jnp.bfloat16)
    value_rows = value_rows.reshape(sequence_count, piece_columns, head_split, head_channels)
    averaged_values = jnp.einsum(
        "ijh,sjhe->sihe", weights, value_rows, preferred_element_type=jnp.float32
    )
    averaged_values = averaged_values.reshape(
        sequence_count, piece_rows, head_split * head_channels
    )
    output_weight = mean_final_matrix.astype(jnp.float32)
    local_portion = lax.psum_scatter(
        averaged_values.astype(jnp.bfloat16), "col", scatter_dimension=1, tiled=True
    ).astype(jnp.float32)
    shard_standardized = standardize_features(sequence_stack, mean_sequence_scale).astype(
        jnp.bfloat16
    )
    gate_values = jax.nn.sigmoid(
        jnp.dot(shard_standardized, mean_sigmoid_matrix, preferred_element_type=jnp.float32)
    )
    sequence_delta = jnp.dot(
        gate_values * local_portion, output_weight, precision=lax.Precision.HIGHEST
    )
    revised_sequences = (sequence_stack.astype(jnp.float32) + sequence_delta).astype(jnp.bfloat16)
    tri_normed = standardize_features(pair_one, trimul_scale).astype(jnp.bfloat16)
    projected = jnp.dot(tri_normed, trimul_entry_matrix, preferred_element_type=jnp.float32)
    pair_mask = (row_tokens[:, None] * col_tokens[None, :])[..., None]
    tri_left = (
        jax.nn.sigmoid(projected[..., 0:width]) * projected[..., width : 2 * width] * pair_mask
    ).astype(jnp.bfloat16)
    tri_right = (
        jax.nn.sigmoid(projected[..., 2 * width : 3 * width])
        * projected[..., 3 * width : 4 * width]
        * pair_mask
    ).astype(jnp.bfloat16)
    out_gate = jax.nn.sigmoid(projected[..., 4 * width : 5 * width])
    left_rows, right_rows = (
        lax.all_gather(tri_left, "col", axis=1, tiled=True),
        lax.all_gather(tri_right, "col", axis=1, tiled=True),
    )
    right_piece = lax.dynamic_slice_in_dim(right_rows, offset, piece_columns, 0)
    right_needed = from_root(right_piece, "row", root_row)
    product = jnp.einsum(
        "ikc,jkc->ijc", left_rows, right_needed, preferred_element_type=jnp.float32
    )
    final = out_gate * jnp.dot(
        standardize_features(product, trimul_result_scale).astype(jnp.bfloat16),
        trimul_final_matrix,
        preferred_element_type=jnp.float32,
    )
    pair_output = (pair_one.astype(jnp.float32) + final).astype(jnp.bfloat16)
    return (revised_sequences, pair_output)


def in_vmem(array):
    return pltpu.with_memory_space_constraint(array, pltpu.VMEM)


def place_lanes(source, start, count, target, lane, base):
    block, offset = start // 128, start % 128
    shift = (target - offset) % 128
    piece = source[:, block * 128 : (block + 1) * 128]
    piece = pltpu.roll(piece, shift, 1) if shift else piece
    if offset + count > 128:
        rest = source[:, (block + 1) * 128 : (block + 2) * 128]
        rest = pltpu.roll(rest, shift, 1) if shift else rest
        piece = jnp.where(lane < target + 128 - offset, piece, rest)
    return jnp.where((lane >= target) & (lane < target + count), piece, base)


def unit_rows(value):
    centred = value - jnp.mean(value, -1, keepdims=True)
    variance = jnp.mean(centred * centred, -1, keepdims=True)
    return centred * lax.rsqrt(variance + epsilon)


def first_kernel(tokens_hbm, flags, scale, entry, couple_hbm, *refs):
    n = len(refs) - 5
    sends, right, pieces, tokens, couple, arrived = refs[:n], refs[n], *refs[n + 1 :]
    t, ch, s = tokens.shape
    hidden, part = entry.shape[1] // 2, couple.shape[0]
    half, place = lax.axis_index("depth"), lax.axis_index("col")
    copies = [
        pltpu.make_async_copy(tokens_hbm, tokens, arrived.at[0]),
        pltpu.make_async_copy(couple_hbm.at[pl.ds(half * part, part)], couple, arrived.at[1]),
    ]
    for copy in copies:
        copy.start()
    mask = flags[pl.ds(half, 1), :].astype(f32)
    square = (ch, ch)
    diagonal = lax.broadcasted_iota(jnp.int32, square, 0) == lax.broadcasted_iota(jnp.int32, square, 1)
    column = jnp.sum(jnp.where(diagonal, scale[...], 0.0), 1, keepdims=True)
    copies[0].wait()
    lefts = []
    for u in range(t):
        value = tokens[u].astype(f32)
        centred = value - jnp.mean(value, 0, keepdims=True)
        variance = jnp.mean(centred * centred, 0, keepdims=True)
        normed = (centred * lax.rsqrt(variance + epsilon) * column).astype(bf16)
        factor = lax.dot_general(entry[...], normed, (((0,), (0,)), ((), ())), preferred_element_type=f32) * mask
        lefts.append(factor[:hidden])
        right[u] = factor[hidden:].astype(bf16)
    copies[1].wait()
    for i in range(part):
        row = couple[i].astype(f32)
        for k in range(n):
            pieces[k, i * t : (i + 1) * t] = row[k * t : (k + 1) * t]
    for k in range(n):
        sends[k][...] = jnp.concatenate(lefts + [pieces[lax.rem(place + k, n)]], 0).astype(bf16)


def first_stage(tokens, flags, scale, entry, couple, n):
    t, ch, s = tokens.shape
    rows, cols, width = couple.shape
    hidden = entry.shape[1] // 2
    vmem, hbm = pl.BlockSpec(memory_space=pltpu.VMEM), pl.BlockSpec(memory_space=pl.ANY)
    length = t * hidden + rows // 2 * t
    return pl.pallas_call(
        first_kernel,
        out_shape=[pltpu.VMEM((length, s), bf16)] * n + [pltpu.VMEM((t, hidden, s), bf16)],
        in_specs=[hbm, vmem, vmem, vmem, hbm],
        out_specs=[vmem] * (n + 1),
        scratch_shapes=[
            pltpu.VMEM((n, rows // 2 * t, width), f32),
            pltpu.VMEM(tokens.shape, bf16),
            pltpu.VMEM((rows // 2, cols, width), bf16),
            pltpu.SemaphoreType.DMA((2,)),
        ],
        name="first_stage",
    )(tokens, flags, scale, entry, couple)


def outer_kernel(n, *refs):
    half, row_index, col_index = lax.axis_index("depth"), lax.axis_index("row"), lax.axis_index("col")
    lefts, rights = refs[:n], refs[n : 2 * n]
    t, hidden, s = rights[0].shape
    flags, final_hbm, out, left, pieces, right, plain, turned, outer, high, low, couples, couple, final, arrived = refs[2 * n :]
    tokens, ratio = n * t, 128 // hidden
    copy = pltpu.make_async_copy(final_hbm, final, arrived)
    copy.start()
    for k in range(n):
        sent = lefts[k][...].astype(f32)
        place = lax.rem(col_index + (n - k), n)
        left[place] = sent[: t * hidden].astype(bf16)
        couples[place] = sent[t * hidden :]
        pieces[row_index ^ k] = rights[k][...].reshape(t * hidden, s).astype(f32)
    for k in range(n):
        for u in range(t):
            right[pl.ds(k * t + u, hidden, stride=tokens), :] = pieces[k, u * hidden : (u + 1) * hidden, :]
    outer[...] = lax.dot_general(
        right[...].astype(bf16),
        left[...].reshape(tokens * hidden, s),
        (((1,), (1,)), ((), ())),
        preferred_element_type=f32,
    )
    copy.wait()
    plain[...] = final[...].astype(f32)
    for d in range(hidden):
        turned[d * hidden : (d + 1) * hidden, :] = plain[pl.ds(d, hidden, stride=hidden), :].astype(bf16)
    lane = lax.broadcasted_iota(jnp.int32, (tokens, 128), 1)
    for g in range(tokens // ratio):
        for q in range(hidden // ratio):
            tiles = [
                outer[(q * ratio + d) * tokens : (q * ratio + d + 1) * tokens, g * 128 : (g + 1) * 128]
                for d in range(ratio)
            ]
            bit = 1
            while bit < ratio:
                upper = (lane // (hidden * bit)) % 2 == 1
                for x in range(ratio):
                    if x & bit:
                        continue
                    a, b = tiles[x], tiles[x | bit]
                    tiles[x] = jnp.where(upper, pltpu.roll(b, hidden * bit, 1), a)
                    tiles[x | bit] = jnp.where(upper, b, pltpu.roll(a, 128 - hidden * bit, 1))
                bit *= 2
            for x in range(ratio):
                i = g * ratio + x
                rounded = tiles[x].astype(bf16)
                high[i * tokens : (i + 1) * tokens, q * 128 : (q + 1) * 128] = rounded
                low[i * tokens : (i + 1) * tokens, q * 128 : (q + 1) * 128] = (
                    tiles[x] - rounded.astype(f32)
                ).astype(bf16)
    part = tokens // 2
    for k in range(n):
        for i in range(part):
            couple[i * tokens + k * t : i * tokens + (k + 1) * t] = couples[k, i * t : (i + 1) * t]
    total = jnp.sum(flags[...].astype(f32)) + 0.001
    update = jnp.dot(high[...], turned[...], preferred_element_type=f32) + jnp.dot(
        low[...], turned[...], preferred_element_type=f32
    )
    out[...] = update / total
    mine = pl.ds(pl.multiple_of(half * (part * tokens), 8), part * tokens)
    out[mine, :] = out[mine, :] + couple[...]


def outer_stage(lefts, rights, flags, final):
    n = len(lefts)
    t, hidden, s = rights[0].shape
    tokens, width = n * t, final.shape[1]
    vmem = pl.BlockSpec(memory_space=pltpu.VMEM)
    return pl.pallas_call(
        functools.partial(outer_kernel, n),
        out_shape=pltpu.VMEM((tokens * tokens, width), f32),
        in_specs=[vmem] * (2 * n + 1) + [pl.BlockSpec(memory_space=pl.ANY)],
        out_specs=vmem,
        scratch_shapes=[
            pltpu.VMEM((n, t * hidden, s), bf16),
            pltpu.VMEM((n, t * hidden, s), f32),
            pltpu.VMEM((tokens * hidden, s), f32),
            pltpu.VMEM((hidden * hidden, width), f32),
            pltpu.VMEM((hidden * hidden, width), bf16),
            pltpu.VMEM((tokens * hidden, tokens * hidden), f32),
            pltpu.VMEM((tokens * tokens, hidden * hidden), bf16),
            pltpu.VMEM((tokens * tokens, hidden * hidden), bf16),
            pltpu.VMEM((n, tokens // 2 * t, width), f32),
            pltpu.VMEM((tokens // 2 * tokens, width), f32),
            pltpu.VMEM(final.shape, bf16),
            pltpu.SemaphoreType.DMA,
        ],
        name="outer_stage",
    )(*map(in_vmem, lefts), *map(in_vmem, rights), flags, final)


def pair_kernel(sizes, genuine, own, other, offset, couple_scale, score, tri_scale, entry_hbm, tokens_hbm, block, value, normed, projected, logits, tri, head_rows, entry, tokens, turned_entry, picked, arrived):
    n, rows, cols, heads, feats = sizes
    half, row_index, col_index = lax.axis_index("depth"), lax.axis_index("row"), lax.axis_index("col")
    copies = [
        pltpu.make_async_copy(entry_hbm.at[:, pl.ds(0, entry.shape[1])], entry, arrived.at[0]),
        pltpu.make_async_copy(tokens_hbm, tokens, arrived.at[1]),
    ]
    for copy in copies:
        copy.start()
    parts, width = n * n, own.shape[1]
    part, spare = rows // 2, 128 - feats * cols
    total = own[...] + other[...] + offset[...]
    value[...] = total.astype(bf16).astype(f32)
    unit = unit_rows(value[...])
    size = rows * cols
    padded = normed.shape[0]
    wide = lax.dot_general(
        score[...], unit * couple_scale[...], (((1,), (1,)), ((), ())),
        precision=lax.Precision.HIGHEST, preferred_element_type=f32,
    )
    logits[:, :size] = wide
    lane8 = lax.broadcasted_iota(jnp.int32, (heads, 128), 1)
    low = jnp.full((heads, 128), -jnp.inf, f32)
    for i in range(rows):
        head_rows[pl.ds(i, heads, stride=rows), :] = place_lanes(logits, i * cols, cols, 0, lane8, low)
    t, ch, s = tokens.shape
    line = lax.broadcasted_iota(jnp.int32, (8, 128), 1)
    bias = jnp.zeros((8, 128), f32)
    open_lanes = jnp.zeros((8, 128), f32)
    for j in range(cols):
        flag = genuine[j // t * rows + col_index * t + j % t].astype(f32)
        bias = jnp.where(line == j, 1000000000.0 * (flag - 1.0), bias)
        here = line == j
        for f in range(1, feats):
            here = here | (line == f * cols + j)
        open_lanes = jnp.where(here, flag, open_lanes)
    score_rows = head_rows[...] + bias[:1]
    peak = jnp.max(score_rows, -1, keepdims=True)
    expo = jnp.exp(score_rows - peak).astype(bf16).astype(f32)
    lane = lax.broadcasted_iota(jnp.int32, (rows, 128), 1)
    zero = jnp.zeros((rows, 128), f32)
    tail = zero
    flat = zero
    for h in range(heads):
        mine = expo[h * rows : (h + 1) * rows]
        start = h * cols
        if start < 128:
            shifted = pltpu.roll(mine, start, 1) if start else mine
            flat = jnp.where((lane >= start) & (lane < start + cols), shifted, flat)
            if start + cols > 128:
                tail = jnp.where(lane < start + cols - 128, shifted, tail)
        else:
            start -= 128
            shifted = pltpu.roll(mine, start, 1) if start else mine
            tail = jnp.where((lane >= start) & (lane < start + cols), shifted, tail)
    first, second = pltpu.roll(tail, 128 - spare, 1), pltpu.roll(tail, 128 - 2 * spare, 1)
    wide_peak = jnp.broadcast_to(peak, (heads * rows, 128))
    tiny = lax.broadcasted_iota(jnp.int32, (8, 128), 1)
    stats = jnp.zeros((8, 128), f32)
    for q in range(3):
        piece = wide_peak.astype(bf16).astype(f32)
        wide_peak = wide_peak - piece
        for a in range(rows // 8):
            for h in range(heads):
                stats = jnp.where(
                    tiny == a * 3 * heads + q * heads + h, piece[h * rows + a * 8 : h * rows + a * 8 + 8], stats
                )
    normed[:size] = (unit * tri_scale[...]).astype(bf16)
    normed[size:] = jnp.zeros((padded - size, width), bf16)
    copies[0].wait()
    turned_entry[...] = entry[...].astype(f32).T
    group = feats * parts
    for k in range(4):
        start = pl.multiple_of(k * width + half * group, 8)
        turned_entry[k * group : (k + 1) * group] = turned_entry[pl.ds(start, group), :]
    for k in range(4):
        for f in range(feats):
            picked[(k * feats + f) * parts : (k * feats + f + 1) * parts] = turned_entry[
                pl.ds(k * group + f, parts, stride=feats), :
            ].astype(bf16)
    raw = lax.dot_general(picked[...], normed[...], (((1,), (1,)), ((), ())), preferred_element_type=f32)
    cut = lax.broadcasted_iota(jnp.int32, (parts, 128), 1)
    empty = jnp.zeros((parts, 128), f32)
    for side in range(2):
        base = side * 2 * group
        projected[...] = jax.nn.sigmoid(raw[base : base + group]) * raw[base + group : base + 2 * group]
        for i in range(rows):
            packed = empty
            for f in range(feats):
                packed = place_lanes(projected.at[f * parts : (f + 1) * parts], i * cols, cols, f * cols, cut, packed)
            flag = genuine[row_index * rows + i].astype(f32)
            tri[side, pl.ds(i, parts, stride=rows), :] = packed * (open_lanes[:1] * flag)
    copies[1].wait()
    turned = tokens[...].astype(f32).reshape(t * ch, s).T
    keep = lane < feats * cols
    for p in range(parts):
        slabs = [
            jnp.where(keep, tri[0, p * rows : (p + 1) * rows], first),
            jnp.where(keep, tri[1, p * rows : (p + 1) * rows], second),
            flat,
            stats,
        ]
        slabs += [turned[p * 8 : (p + 1) * 8, a * 128 : (a + 1) * 128] for a in range(t * ch // 128)]
        if p < part:
            slabs.append(value[pl.ds(pl.multiple_of((half * part + p) * cols, 8), cols), :])
        else:
            slabs.append(jnp.zeros((cols, width), f32))
        block[p] = jnp.concatenate(slabs, 0).astype(bf16)


def pair_stage(genuine, own, other, offset, couple_scale, score, tri_scale, entry, tokens, n, rows, cols):
    parts, width = n * n, own.shape[1]
    heads = score.shape[0]
    feats = width // (2 * parts)
    t, ch, s = tokens.shape
    padded = (rows * cols + 127) // 128 * 128
    vmem, hbm = pl.BlockSpec(memory_space=pltpu.VMEM), pl.BlockSpec(memory_space=pl.ANY)
    length = 3 * rows + 8 + t * ch // 128 * 8 + cols
    return pl.pallas_call(
        functools.partial(pair_kernel, (n, rows, cols, heads, feats)),
        out_shape=pltpu.VMEM((parts, length, 128), bf16),
        in_specs=[pl.BlockSpec(memory_space=pltpu.SMEM)] + [vmem] * 6 + [hbm] * 2,
        out_specs=vmem,
        scratch_shapes=[
            pltpu.VMEM((rows * cols, width), f32),
            pltpu.VMEM((padded, width), bf16),
            pltpu.VMEM((feats * parts, padded), f32),
            pltpu.VMEM((heads, padded), f32),
            pltpu.VMEM((2, parts * rows, 128), f32),
            pltpu.VMEM((heads * rows, 128), f32),
            pltpu.VMEM((width, 4 * width), bf16),
            pltpu.VMEM(tokens.shape, bf16),
            pltpu.VMEM((4 * width, width), f32),
            pltpu.VMEM((4 * feats * parts, width), bf16),
            pltpu.SemaphoreType.DMA((2,)),
        ],
        name="pair_stage",
    )(
        genuine, in_vmem(own), in_vmem(other), offset.reshape(1, -1), couple_scale.reshape(1, -1), score, tri_scale.reshape(1, -1),
        entry, tokens,
    )


def halves(value):
    high = value.astype(bf16)
    return high, (value - high.astype(f32)).astype(bf16)


def two_pass_dot(value, matrix, axis=0):
    high, low = halves(value)
    over = (((1,), (axis,)), ((), ()))
    return lax.dot_general(high, matrix, over, preferred_element_type=f32) + lax.dot_general(
        low, matrix, over, preferred_element_type=f32
    )


def middle_kernel(sizes, block, seq_scale, content, sigmoid_matrix, final, out, wide, lhs, rhs, product, weights, x, values, gated, masked, revised):
    n, rows, cols, heads, feats, groups, order = sizes
    parts, tokens, ch = n * n, n * rows, final.shape[0]
    s, per = 8, 128 // final.shape[0]
    t = rows // n
    wide[...] = block[...].astype(f32)
    lane = lax.broadcasted_iota(jnp.int32, (tokens, 128), 1)
    small = lax.broadcasted_iota(jnp.int32, (rows, 128), 1)
    tiny = lax.broadcasted_iota(jnp.int32, (8, 128), 1)
    spare = 128 - feats * cols

    def stacked(c, start, count):
        return jnp.concatenate([wide[r * n + c, start : start + count] for r in range(n)], 0)

    rhs[...] = jnp.zeros_like(rhs)
    for c in range(n):
        mine = stacked(c, 0, rows)
        for f in range(feats):
            keep = (lane >= f * cols) & (lane < (f + 1) * cols)
            lhs[f * tokens : (f + 1) * tokens, c * 128 : (c + 1) * 128] = jnp.where(keep, mine, 0.0).astype(bf16)
        rhs[:tokens, c * 128 : (c + 1) * 128] = stacked(c, rows, rows).astype(bf16)
    product[...] = lax.dot_general(lhs[...], rhs[...], (((1,), (1,)), ((), ())), preferred_element_type=f32)
    up = lax.broadcasted_iota(jnp.int32, (256, 128), 0)
    across = lax.broadcasted_iota(jnp.int32, (256, 128), 1)
    gather = ((up >= across * cols) & (up < (across + 1) * cols) & (across < heads)).astype(bf16)
    up = lax.broadcasted_iota(jnp.int32, (128, 256), 0)
    across = lax.broadcasted_iota(jnp.int32, (128, 256), 1)
    spread = ((across >= up * cols) & (across < (up + 1) * cols) & (up < heads)).astype(bf16)
    expos, peaks = [], []
    for c in range(n):
        a, b = stacked(c, 0, rows), stacked(c, rows, rows)
        rest = jnp.where(lane < spare, pltpu.roll(a, spare, 1), jnp.where(lane < 2 * spare, pltpu.roll(b, 2 * spare, 1), 0.0))
        expos.append(jnp.concatenate([stacked(c, 2 * rows, rows), rest], 1))
        peak = []
        for r in range(n):
            stats = wide[r * n + c, 3 * rows : 3 * rows + 8]
            for q in range(rows // 8):
                one = pltpu.roll(stats, (128 - 3 * heads * q) % 128, 1) if q else stats
                peak.append(one + pltpu.roll(one, 128 - heads, 1) + pltpu.roll(one, 128 - 2 * heads, 1))
        peaks.append(jnp.concatenate(peak, 0))
    top = peaks[0]
    for c in range(1, n):
        top = jnp.maximum(top, peaks[c])
    factors = [jnp.exp(peak - top) for peak in peaks]
    total = jnp.zeros_like(top)
    for c in range(n):
        total = total + factors[c] * jnp.dot(expos[c].astype(bf16), gather, preferred_element_type=f32)
    for c in range(n):
        scale = jnp.where(lane < heads, factors[c] / jnp.where(lane < heads, total, 1.0), 0.0)
        weights[:, c * 256 : (c + 1) * 256] = (expos[c] * two_pass_dot(scale, spread)).astype(bf16)
    for p in range(parts):
        for g in range(groups):
            pair = wide[p, 3 * rows + 8 + 8 * g : 3 * rows + 16 + 8 * g]
            for k in range(per):
                x[pl.ds(p * t + g * per + k, s, stride=tokens), :] = pltpu.roll(pair, 128 - k * ch, 1) if k else pair
    raw = x[...][:, :ch]
    centred = raw - jnp.mean(raw, -1, keepdims=True)
    variance = jnp.mean(centred * centred, -1, keepdims=True)
    normed = (centred * lax.rsqrt(variance + epsilon) * seq_scale[...]).astype(bf16)
    values[...] = jnp.dot(normed, content[...], preferred_element_type=f32).astype(bf16).astype(f32)
    gates = jax.nn.sigmoid(jnp.dot(normed, sigmoid_matrix[...], preferred_element_type=f32))
    width = gates.shape[1]
    head_of = lax.broadcasted_iota(jnp.int32, (cols, width), 1) // (width // heads)
    used = heads * cols
    masked[...] = jnp.zeros_like(masked)
    for q in range(s):
        for c in range(n):
            local = jnp.concatenate([values[q * tokens + a : q * tokens + a + m] for a, m in order[c]], 0)
            spread_out = jnp.concatenate([jnp.where(head_of == h, local, 0.0) for h in range(heads)], 0)
            masked[q, c * 256 : c * 256 + used] = spread_out.astype(bf16)
        averaged = jnp.dot(weights[...], masked[q], preferred_element_type=f32)
        gated[q * tokens : (q + 1) * tokens] = gates[q * tokens : (q + 1) * tokens] * averaged
    delta = two_pass_dot(gated[...], final[...], 1)
    revised[:, :ch] = raw + delta
    for p in range(parts):
        r, c = p // n, p % n
        slab = jnp.zeros((rows, 128), f32)
        for f in range(feats):
            shift = ((f - c) * cols) % 128
            piece = product[f * tokens + r * rows : f * tokens + (r + 1) * rows]
            piece = pltpu.roll(piece, shift, 1) if shift else piece
            slab = jnp.where((small >= f * cols) & (small < (f + 1) * cols), piece, slab)
        start = 3 * rows + 8 + 8 * groups + c * t
        slabs = [slab] + [wide[r * n + k, start : start + t] for k in range(n)]
        for g in range(groups):
            merged = revised[pl.ds(p * t + g * per, s, stride=tokens), :]
            for k in range(1, per):
                piece = revised[pl.ds(p * t + g * per + k, s, stride=tokens), :]
                merged = jnp.where(tiny >= k * ch, pltpu.roll(piece, k * ch, 1), merged)
            slabs.append(merged)
        out[p] = jnp.concatenate(slabs, 0).astype(bf16)


def middle_stage(block, n, rows, cols, heads, feats, order, seq_scale, content, sigmoid_matrix, final):
    parts, tokens = n * n, n * rows
    groups = (block.shape[1] - 3 * rows - 8 - cols) // 8
    width = content.shape[1]
    vmem = pl.BlockSpec(memory_space=pltpu.VMEM)
    return pl.pallas_call(
        functools.partial(middle_kernel, (n, rows, cols, heads, feats, groups, order)),
        out_shape=pltpu.VMEM((parts, rows + cols + 8 * groups, 128), bf16),
        in_specs=[vmem] * 5,
        out_specs=vmem,
        scratch_shapes=[
            pltpu.VMEM(block.shape, f32),
            pltpu.VMEM((feats * tokens, n * 128), bf16),
            pltpu.VMEM((128, n * 128), bf16),
            pltpu.VMEM((feats * tokens, 128), f32),
            pltpu.VMEM((tokens, n * 256), bf16),
            pltpu.VMEM((8 * tokens, 128), f32),
            pltpu.VMEM((8 * tokens, width), f32),
            pltpu.VMEM((8 * tokens, width), f32),
            pltpu.VMEM((8, n * 256, width), bf16),
            pltpu.VMEM((8 * tokens, 128), f32),
        ],
        name="middle_stage",
    )(in_vmem(block), seq_scale.reshape(1, -1), content, sigmoid_matrix, final.T)


def last_kernel(sizes, own, other, tri_scale, result_scale, entry_hbm, final_hbm, pair_output, revised, product, turned, pair, entry, final, plain, mixed, arrived):
    n, rows, cols, feats = sizes
    copies = [
        pltpu.make_async_copy(entry_hbm.at[:, pl.ds(4 * final.shape[1], final.shape[1])], entry, arrived.at[0]),
        pltpu.make_async_copy(final_hbm, final, arrived.at[1]),
    ]
    for copy in copies:
        copy.start()
    parts, width = n * n, final.shape[1]
    part, wide = rows // 2, 2 * n * n
    mine = lax.axis_index("depth")
    theirs = 1 - mine
    for p in range(parts):
        here, there = own[p].astype(f32), other[p].astype(f32)
        product[mine, p * rows : (p + 1) * rows] = here[:rows]
        product[theirs, p * rows : (p + 1) * rows] = there[:rows]
        if p < part:
            pair[pl.ds(pl.multiple_of((mine * part + p) * cols, 8), cols), :] = here[rows : rows + cols]
            pair[pl.ds(pl.multiple_of((theirs * part + p) * cols, 8), cols), :] = there[rows : rows + cols]
    lane = lax.broadcasted_iota(jnp.int32, (cols, 128), 1)
    per = 128 // wide
    for g in range(rows // per):
        stacked = []
        for k in range(per):
            for d in range(2):
                stacked.append(product[d, pl.ds(g * per + k, parts, stride=rows), :])
        flipped = jnp.concatenate(stacked, 0).T
        for k in range(per):
            merged = jnp.zeros((cols, 128), f32)
            for f in range(feats):
                merged = place_lanes(flipped[f * cols : (f + 1) * cols], k * wide, wide, f * wide, lane, merged)
            turned[(g * per + k) * cols : (g * per + k + 1) * cols] = merged
    value = pair[...]
    normed = (unit_rows(value) * tri_scale[...]).astype(bf16)
    for copy in copies:
        copy.wait()
    gate = jax.nn.sigmoid(jnp.dot(normed, entry[...], preferred_element_type=f32))
    plain[...] = final[...].astype(f32)
    for f in range(feats):
        mixed[f * wide : (f + 1) * wide] = plain[pl.ds(f, wide, stride=feats), :].astype(bf16)
    at = lax.broadcasted_iota(jnp.int32, (width, width), 1)
    origin = lax.broadcasted_iota(jnp.int32, (width, width), 0)
    goal = lax.rem(origin, feats) * wide + lax.div(origin, feats)
    scale = jnp.dot(
        result_scale[...], (at == goal).astype(f32), precision=lax.Precision.HIGHEST, preferred_element_type=f32
    )
    result = (unit_rows(turned[...]) * scale).astype(bf16)
    pair_output[...] = (value + gate * jnp.dot(result, mixed[...], preferred_element_type=f32)).astype(bf16)
    for a in range((own.shape[1] - rows - cols) // 8):
        start = rows + cols + 8 * a
        flipped = jnp.concatenate([own[p, start : start + 8].astype(f32) for p in range(parts)], 0).T
        revised[a * 128 : (a + 1) * 128] = flipped.astype(bf16)


def last_stage(own, other, tri_scale, entry, result_scale, final, n, rows, cols, t, ch):
    parts, width = n * n, final.shape[1]
    feats = width // (2 * parts)
    vmem, hbm = pl.BlockSpec(memory_space=pltpu.VMEM), pl.BlockSpec(memory_space=pl.ANY)
    pair_output, revised = pl.pallas_call(
        functools.partial(last_kernel, (n, rows, cols, feats)),
        out_shape=[
            jax.ShapeDtypeStruct((rows * cols, width), bf16),
            jax.ShapeDtypeStruct((t * ch, 8 * parts), bf16),
        ],
        in_specs=[vmem] * 4 + [hbm] * 2,
        out_specs=[vmem] * 2,
        scratch_shapes=[
            pltpu.VMEM((2, parts * rows, 128), f32),
            pltpu.VMEM((rows * cols, 128), f32),
            pltpu.VMEM((rows * cols, width), f32),
            pltpu.VMEM((width, width), bf16),
            pltpu.VMEM((width, width), bf16),
            pltpu.VMEM((width, width), f32),
            pltpu.VMEM((width, width), bf16),
            pltpu.SemaphoreType.DMA((2,)),
        ],
        name="last_stage",
    )(in_vmem(own), in_vmem(other), tri_scale.reshape(1, -1), result_scale.reshape(1, -1), entry, final)
    return revised.reshape(t, ch, 8 * parts).transpose(2, 0, 1), pair_output.reshape(rows, cols, width)


def on_device(
    sequence_stack,
    present_sequence_flags,
    genuine_residue_flags,
    couple_state,
    tensor_scale,
    tensor_entry_matrix,
    tensor_final_matrix,
    tensor_offset,
    mean_sequence_scale,
    mean_couple_scale,
    mean_score_matrix,
    mean_content_matrix,
    mean_sigmoid_matrix,
    mean_final_matrix,
    trimul_scale,
    trimul_entry_matrix,
    trimul_result_scale,
    trimul_final_matrix,
):
    n = lax.axis_size("row")
    parts = n * n
    rows, cols, width = couple_state.shape
    count, t, ch = sequence_stack.shape
    hidden = tensor_entry_matrix.shape[1] // 2
    heads = mean_score_matrix.shape[1]
    feats = width // (2 * parts)
    order = tuple(tuple((r * rows + c * t, t) for r in range(n)) for c in range(n))
    flags = present_sequence_flags.reshape(2, count)
    tokens = sequence_stack.transpose(1, 2, 0)
    *sends, right = first_stage(tokens, flags, tensor_scale.reshape(1, ch), tensor_entry_matrix, couple_state, n)

    def move(array, where):
        pairs = [(r * n + c, where(r, c)[0] * n + where(r, c)[1]) for r in range(n) for c in range(n)]
        return lax.ppermute(array, ("row", "col"), pairs)

    rights = [right] + [move(right, lambda r, c, k=k: (r ^ k, c)) for k in range(1, n)]
    lefts = [sends[0]] + [move(sends[k], lambda r, c, k=k: (r, (c + k) % n)) for k in range(1, n)]
    share = outer_stage(lefts, rights, flags, tensor_final_matrix)
    other = lax.ppermute(share, "depth", [(0, 1), (1, 0)])
    block = pair_stage(
        genuine_residue_flags, share, other, tensor_offset, mean_couple_scale, mean_score_matrix.T, trimul_scale,
        trimul_entry_matrix, tokens, n, rows, cols,
    )
    block = lax.all_to_all(block, ("row", "col"), 0, 0, tiled=True)
    block = middle_stage(
        block, n, rows, cols, heads, feats, order, mean_sequence_scale, mean_content_matrix, mean_sigmoid_matrix,
        mean_final_matrix,
    )
    block = lax.all_to_all(block, ("row", "col"), 0, 0, tiled=True)
    other = lax.ppermute(block[:, : rows + cols], "depth", [(0, 1), (1, 0)])
    return last_stage(
        block, other, trimul_scale, trimul_entry_matrix, trimul_result_scale, trimul_final_matrix, n, rows, cols, t, ch
    )


def suits(mesh):
    return mesh.shape["row"] == mesh.shape["col"] and mesh.shape["depth"] == 2


def solution(mesh):
    placed = (P("depth", ("row", "col"), None), P(), P(), P("row", "col", None)) + (P(),) * 14
    return jax.shard_map(
        on_device if suits(mesh) else on_device_generic,
        mesh=mesh,
        in_specs=placed,
        out_specs=(P("depth", ("row", "col"), None), P("row", "col", None)),
        check_vma=False,
    )
```

```python
import functools

import jax
import jax.numpy as jnp
from jax import lax
from jax.experimental import pallas as pl
from jax.experimental.pallas import tpu as pltpu
from jax.sharding import PartitionSpec as P

epsilon = 1e-05
bf16 = jnp.bfloat16
f32 = jnp.float32


def from_root(array, axis, root):
    mine = lax.axis_index(axis) == root
    return lax.psum(jnp.where(mine, array, jnp.zeros_like(array)), axis)


def standardize_features(value_rows, scale):
    value_rows = value_rows.astype(jnp.float32)
    average = jnp.mean(value_rows, -1, keepdims=True)
    centred = value_rows - average
    variance = jnp.mean(centred * centred, -1, keepdims=True)
    return centred * lax.rsqrt(variance + epsilon) * scale


def on_device_generic(
    sequence_stack,
    present_sequence_flags,
    genuine_residue_flags,
    couple_state,
    tensor_scale,
    tensor_entry_matrix,
    tensor_final_matrix,
    tensor_offset,
    mean_sequence_scale,
    mean_couple_scale,
    mean_score_matrix,
    mean_content_matrix,
    mean_sigmoid_matrix,
    mean_final_matrix,
    trimul_scale,
    trimul_entry_matrix,
    trimul_result_scale,
    trimul_final_matrix,
):
    n_row = lax.axis_size("row")
    n_col = lax.axis_size("col")
    row_index = lax.axis_index("row")
    col_index = lax.axis_index("col")
    depth_position = lax.axis_index("depth")
    piece_rows, piece_columns, width = couple_state.shape
    sequence_count, shard_residues, ignored_quantity = sequence_stack.shape
    hidden = tensor_entry_matrix.shape[1] // 2
    head_split = mean_score_matrix.shape[1]
    head_channels = mean_content_matrix.shape[1] // head_split
    token_weight = genuine_residue_flags.astype(jnp.float32)
    mask_as_float = present_sequence_flags.astype(jnp.float32)
    row_softmax_weight = lax.dynamic_slice_in_dim(
        mask_as_float, depth_position * sequence_count, sequence_count
    )
    row_count = jnp.sum(mask_as_float)
    entire_sequences = lax.all_gather(sequence_stack, "col", axis=1, tiled=True)
    root_row = col_index * n_row // n_col
    offset = col_index * piece_columns - root_row * piece_rows
    column_piece = lax.dynamic_slice_in_dim(entire_sequences, offset, piece_columns, 1)
    whole_cols = from_root(column_piece, "row", root_row)
    opm_rows = standardize_features(entire_sequences, tensor_scale).astype(jnp.bfloat16)
    opm_cols = standardize_features(whole_cols, tensor_scale).astype(jnp.bfloat16)
    left_projection = (
        jnp.dot(opm_rows, tensor_entry_matrix[:, :hidden], preferred_element_type=jnp.float32)
        * row_softmax_weight[:, None, None]
    ).astype(jnp.bfloat16)
    right_proj = (
        jnp.dot(opm_cols, tensor_entry_matrix[:, hidden:], preferred_element_type=jnp.float32)
        * row_softmax_weight[:, None, None]
    ).astype(jnp.bfloat16)
    outer_sum = jnp.einsum(
        "sic,sjd->ijcd", left_projection, right_proj, preferred_element_type=jnp.float32
    )
    outer_sum = outer_sum.reshape(piece_rows, piece_columns, hidden * hidden)
    out_float = tensor_final_matrix.astype(jnp.float32)
    outer_share = lax.psum_scatter(outer_sum, "depth", scatter_dimension=0, tiled=True)
    share_rows = outer_share.shape[0]
    pair_share = lax.dynamic_slice_in_dim(couple_state, depth_position * share_rows, share_rows, 0)
    update = (
        jnp.dot(outer_share, out_float, precision=lax.Precision.HIGHEST) / (row_count + 0.001)
        + tensor_offset
    )
    new_share = (pair_share.astype(jnp.float32) + update).astype(jnp.bfloat16)
    pair_one = lax.all_gather(new_share, "depth", axis=0, tiled=True)
    row_tokens = lax.dynamic_slice_in_dim(token_weight, row_index * piece_rows, piece_rows)
    col_tokens = lax.dynamic_slice_in_dim(token_weight, col_index * piece_columns, piece_columns)
    logits = jnp.einsum(
        "ijc,ch->ijh",
        standardize_features(pair_one, mean_couple_scale),
        mean_score_matrix,
        precision=lax.Precision.HIGHEST,
    )
    logits = logits + 1000000000.0 * (col_tokens - 1.0)[None, :, None]
    peak = lax.pmax(jnp.max(logits, axis=1), "col")
    expo = jnp.exp(logits - peak[:, None, :])
    total = lax.psum(jnp.sum(expo, axis=1), "col")
    weights = (expo / total[:, None, :]).astype(jnp.bfloat16)
    col_normed = standardize_features(whole_cols, mean_sequence_scale).astype(jnp.bfloat16)
    value_rows = jnp.dot(
        col_normed, mean_content_matrix, preferred_element_type=jnp.float32
    ).astype(jnp.bfloat16)
    value_rows = value_rows.reshape(sequence_count, piece_columns, head_split, head_channels)
    averaged_values = jnp.einsum(
        "ijh,sjhe->sihe", weights, value_rows, preferred_element_type=jnp.float32
    )
    averaged_values = averaged_values.reshape(
        sequence_count, piece_rows, head_split * head_channels
    )
    output_weight = mean_final_matrix.astype(jnp.float32)
    local_portion = lax.psum_scatter(
        averaged_values.astype(jnp.bfloat16), "col", scatter_dimension=1, tiled=True
    ).astype(jnp.float32)
    shard_standardized = standardize_features(sequence_stack, mean_sequence_scale).astype(
        jnp.bfloat16
    )
    gate_values = jax.nn.sigmoid(
        jnp.dot(shard_standardized, mean_sigmoid_matrix, preferred_element_type=jnp.float32)
    )
    sequence_delta = jnp.dot(
        gate_values * local_portion, output_weight, precision=lax.Precision.HIGHEST
    )
    revised_sequences = (sequence_stack.astype(jnp.float32) + sequence_delta).astype(jnp.bfloat16)
    tri_normed = standardize_features(pair_one, trimul_scale).astype(jnp.bfloat16)
    projected = jnp.dot(tri_normed, trimul_entry_matrix, preferred_element_type=jnp.float32)
    pair_mask = (row_tokens[:, None] * col_tokens[None, :])[..., None]
    tri_left = (
        jax.nn.sigmoid(projected[..., 0:width]) * projected[..., width : 2 * width] * pair_mask
    ).astype(jnp.bfloat16)
    tri_right = (
        jax.nn.sigmoid(projected[..., 2 * width : 3 * width])
        * projected[..., 3 * width : 4 * width]
        * pair_mask
    ).astype(jnp.bfloat16)
    out_gate = jax.nn.sigmoid(projected[..., 4 * width : 5 * width])
    left_rows, right_rows = (
        lax.all_gather(tri_left, "col", axis=1, tiled=True),
        lax.all_gather(tri_right, "col", axis=1, tiled=True),
    )
    right_piece = lax.dynamic_slice_in_dim(right_rows, offset, piece_columns, 0)
    right_needed = from_root(right_piece, "row", root_row)
    product = jnp.einsum(
        "ikc,jkc->ijc", left_rows, right_needed, preferred_element_type=jnp.float32
    )
    final = out_gate * jnp.dot(
        standardize_features(product, trimul_result_scale).astype(jnp.bfloat16),
        trimul_final_matrix,
        preferred_element_type=jnp.float32,
    )
    pair_output = (pair_one.astype(jnp.float32) + final).astype(jnp.bfloat16)
    return (revised_sequences, pair_output)


def in_vmem(array):
    return pltpu.with_memory_space_constraint(array, pltpu.VMEM)


def place_lanes(source, start, count, target, lane, base):
    block, offset = start // 128, start % 128
    shift = (target - offset) % 128
    piece = source[:, block * 128 : (block + 1) * 128]
    piece = pltpu.roll(piece, shift, 1) if shift else piece
    if offset + count > 128:
        rest = source[:, (block + 1) * 128 : (block + 2) * 128]
        rest = pltpu.roll(rest, shift, 1) if shift else rest
        piece = jnp.where(lane < target + 128 - offset, piece, rest)
    return jnp.where((lane >= target) & (lane < target + count), piece, base)


def unit_rows(value):
    centred = value - jnp.mean(value, -1, keepdims=True)
    variance = jnp.mean(centred * centred, -1, keepdims=True)
    return centred * lax.rsqrt(variance + epsilon)


def first_kernel(tokens_hbm, flags, scale, entry, couple_hbm, *refs):
    n = len(refs) - 5
    sends, right, pieces, tokens, couple, arrived = refs[:n], refs[n], *refs[n + 1 :]
    t, ch, s = tokens.shape
    hidden, part = entry.shape[1] // 2, couple.shape[0]
    half, place = lax.axis_index("depth"), lax.axis_index("col")
    copies = [
        pltpu.make_async_copy(tokens_hbm, tokens, arrived.at[0]),
        pltpu.make_async_copy(couple_hbm.at[pl.ds(half * part, part)], couple, arrived.at[1]),
    ]
    for copy in copies:
        copy.start()
    mask = flags[pl.ds(half, 1), :].astype(f32)
    square = (ch, ch)
    diagonal = lax.broadcasted_iota(jnp.int32, square, 0) == lax.broadcasted_iota(jnp.int32, square, 1)
    column = jnp.sum(jnp.where(diagonal, scale[...], 0.0), 1, keepdims=True)
    copies[0].wait()
    lefts = []
    for u in range(t):
        value = tokens[u].astype(f32)
        centred = value - jnp.mean(value, 0, keepdims=True)
        variance = jnp.mean(centred * centred, 0, keepdims=True)
        normed = (centred * lax.rsqrt(variance + epsilon) * column).astype(bf16)
        factor = lax.dot_general(entry[...], normed, (((0,), (0,)), ((), ())), preferred_element_type=f32) * mask
        lefts.append(factor[:hidden])
        right[u] = factor[hidden:].astype(bf16)
    copies[1].wait()
    for i in range(part):
        row = couple[i].astype(f32)
        for k in range(n):
            pieces[k, i * t : (i + 1) * t] = row[k * t : (k + 1) * t]
    for k in range(n):
        sends[k][...] = jnp.concatenate(lefts + [pieces[lax.rem(place + k, n)]], 0).astype(bf16)


def first_stage(tokens, flags, scale, entry, couple, n):
    t, ch, s = tokens.shape
    rows, cols, width = couple.shape
    hidden = entry.shape[1] // 2
    vmem, hbm = pl.BlockSpec(memory_space=pltpu.VMEM), pl.BlockSpec(memory_space=pl.ANY)
    length = t * hidden + rows // 2 * t
    return pl.pallas_call(
        first_kernel,
        out_shape=[pltpu.VMEM((length, s), bf16)] * n + [pltpu.VMEM((t, hidden, s), bf16)],
        in_specs=[hbm, vmem, vmem, vmem, hbm],
        out_specs=[vmem] * (n + 1),
        scratch_shapes=[
            pltpu.VMEM((n, rows // 2 * t, width), f32),
            pltpu.VMEM(tokens.shape, bf16),
            pltpu.VMEM((rows // 2, cols, width), bf16),
            pltpu.SemaphoreType.DMA((2,)),
        ],
        name="first_stage",
    )(tokens, flags, scale, entry, couple)


def ready_kernel(sizes, *refs):
    n, rows, cols, feats = sizes
    parts = n * n
    kept = (len(refs) - 17) // 2
    after, result_scale_hbm, entry_hbm, tokens_hbm, final_hbm = refs[:5]
    picked, slab, gate_entry, mixed, scale = refs[5 + kept : 10 + kept]
    entry, tokens, turned_entry, final, plain, result_scale, arrived = refs[10 + 2 * kept :]
    half = lax.axis_index("depth")
    width, group, wide = entry.shape[0], feats * parts, 2 * parts
    copies = [
        pltpu.make_async_copy(entry_hbm.at[:, pl.ds(0, 4 * width)], entry, arrived.at[0]),
        pltpu.make_async_copy(tokens_hbm, tokens, arrived.at[1]),
        pltpu.make_async_copy(entry_hbm.at[:, pl.ds(4 * width, width)], gate_entry, arrived.at[2]),
        pltpu.make_async_copy(final_hbm, final, arrived.at[3]),
        pltpu.make_async_copy(result_scale_hbm, result_scale, arrived.at[4]),
    ]
    for k in range(kept):
        copies.append(pltpu.make_async_copy(refs[5 + k], refs[10 + kept + k], arrived.at[5 + k]))
    for copy in copies:
        copy.start()
    t, ch, s = tokens.shape
    copies[4].wait()
    at = lax.broadcasted_iota(jnp.int32, (width, width), 1)
    origin = lax.broadcasted_iota(jnp.int32, (width, width), 0)
    goal = lax.rem(origin, feats) * wide + lax.div(origin, feats)
    scale[...] = jnp.dot(
        result_scale[...], (at == goal).astype(f32), precision=lax.Precision.HIGHEST, preferred_element_type=f32
    )
    copies[0].wait()
    turned_entry[...] = entry[...].astype(f32).T
    for k in range(4):
        start = pl.multiple_of(k * width + half * group, 8)
        turned_entry[k * group : (k + 1) * group] = turned_entry[pl.ds(start, group), :]
    for k in range(4):
        for f in range(feats):
            picked[(k * feats + f) * parts : (k * feats + f + 1) * parts] = turned_entry[
                pl.ds(k * group + f, parts, stride=feats), :
            ].astype(bf16)
    copies[1].wait()
    turned = tokens[...].astype(f32).reshape(t * ch, s).T
    for p in range(parts):
        slab[p] = jnp.concatenate(
            [turned[p * 8 : (p + 1) * 8, a * 128 : (a + 1) * 128] for a in range(t * ch // 128)], 0
        )
    for copy in copies[2:4] + copies[5:]:
        copy.wait()
    plain[...] = final[...].astype(f32)
    for f in range(feats):
        mixed[f * wide : (f + 1) * wide] = plain[pl.ds(f, wide, stride=feats), :].astype(bf16)


def ready_stage(after, entry, tokens, result_scale, final, kept, n, rows, cols):
    parts, width = n * n, entry.shape[0]
    feats = width // (2 * parts)
    t, ch, s = tokens.shape
    vmem, hbm = pl.BlockSpec(memory_space=pltpu.VMEM), pl.BlockSpec(memory_space=pl.ANY)
    return pl.pallas_call(
        functools.partial(ready_kernel, (n, rows, cols, feats)),
        out_shape=[
            pltpu.VMEM((4 * feats * parts, width), bf16),
            pltpu.VMEM((parts, t * ch // 128 * 8, 128), f32),
            pltpu.VMEM((width, width), bf16),
            pltpu.VMEM((width, width), bf16),
            pltpu.VMEM((1, width), f32),
        ]
        + [pltpu.VMEM(array.shape, array.dtype) for array in kept],
        in_specs=[hbm] * (5 + len(kept)),
        out_specs=[vmem] * (5 + len(kept)),
        scratch_shapes=[
            pltpu.VMEM((width, 4 * width), bf16),
            pltpu.VMEM(tokens.shape, bf16),
            pltpu.VMEM((4 * width, width), f32),
            pltpu.VMEM((width, width), bf16),
            pltpu.VMEM((width, width), f32),
            pltpu.VMEM((1, width), f32),
            pltpu.SemaphoreType.DMA((5 + len(kept),)),
        ],
        name="ready_stage",
    )(in_vmem(after), result_scale.reshape(1, -1), entry, tokens, final, *kept)


def outer_kernel(n, *refs):
    half, row_index, col_index = lax.axis_index("depth"), lax.axis_index("row"), lax.axis_index("col")
    lefts, rights = refs[:n], refs[n : 2 * n]
    t, hidden, s = rights[0].shape
    flags, final, out, left, pieces, right, plain, turned, outer, high, low, couples, couple = refs[2 * n :]
    tokens, ratio = n * t, 128 // hidden
    for k in range(n):
        sent = lefts[k][...].astype(f32)
        place = lax.rem(col_index + (n - k), n)
        left[place] = sent[: t * hidden].astype(bf16)
        couples[place] = sent[t * hidden :]
        pieces[row_index ^ k] = rights[k][...].reshape(t * hidden, s).astype(f32)
    for k in range(n):
        for u in range(t):
            right[pl.ds(k * t + u, hidden, stride=tokens), :] = pieces[k, u * hidden : (u + 1) * hidden, :]
    outer[...] = lax.dot_general(
        right[...].astype(bf16),
        left[...].reshape(tokens * hidden, s),
        (((1,), (1,)), ((), ())),
        preferred_element_type=f32,
    )
    plain[...] = final[...].astype(f32)
    for d in range(hidden):
        turned[d * hidden : (d + 1) * hidden, :] = plain[pl.ds(d, hidden, stride=hidden), :].astype(bf16)
    lane = lax.broadcasted_iota(jnp.int32, (tokens, 128), 1)
    for g in range(tokens // ratio):
        for q in range(hidden // ratio):
            tiles = [
                outer[(q * ratio + d) * tokens : (q * ratio + d + 1) * tokens, g * 128 : (g + 1) * 128]
                for d in range(ratio)
            ]
            bit = 1
            while bit < ratio:
                upper = (lane // (hidden * bit)) % 2 == 1
                for x in range(ratio):
                    if x & bit:
                        continue
                    a, b = tiles[x], tiles[x | bit]
                    tiles[x] = jnp.where(upper, pltpu.roll(b, hidden * bit, 1), a)
                    tiles[x | bit] = jnp.where(upper, b, pltpu.roll(a, 128 - hidden * bit, 1))
                bit *= 2
            for x in range(ratio):
                i = g * ratio + x
                rounded = tiles[x].astype(bf16)
                high[i * tokens : (i + 1) * tokens, q * 128 : (q + 1) * 128] = rounded
                low[i * tokens : (i + 1) * tokens, q * 128 : (q + 1) * 128] = (
                    tiles[x] - rounded.astype(f32)
                ).astype(bf16)
    part = tokens // 2
    for k in range(n):
        for i in range(part):
            couple[i * tokens + k * t : i * tokens + (k + 1) * t] = couples[k, i * t : (i + 1) * t]
    total = jnp.sum(flags[...].astype(f32)) + 0.001
    update = jnp.dot(high[...], turned[...], preferred_element_type=f32) + jnp.dot(
        low[...], turned[...], preferred_element_type=f32
    )
    out[...] = update / total
    mine = pl.ds(pl.multiple_of(half * (part * tokens), 8), part * tokens)
    out[mine, :] = out[mine, :] + couple[...]


def outer_stage(lefts, rights, flags, final):
    n = len(lefts)
    t, hidden, s = rights[0].shape
    tokens, width = n * t, final.shape[1]
    vmem = pl.BlockSpec(memory_space=pltpu.VMEM)
    return pl.pallas_call(
        functools.partial(outer_kernel, n),
        out_shape=pltpu.VMEM((tokens * tokens, width), f32),
        in_specs=[vmem] * (2 * n + 2),
        out_specs=vmem,
        scratch_shapes=[
            pltpu.VMEM((n, t * hidden, s), bf16),
            pltpu.VMEM((n, t * hidden, s), f32),
            pltpu.VMEM((tokens * hidden, s), f32),
            pltpu.VMEM((hidden * hidden, width), f32),
            pltpu.VMEM((hidden * hidden, width), bf16),
            pltpu.VMEM((tokens * hidden, tokens * hidden), f32),
            pltpu.VMEM((tokens * tokens, hidden * hidden), bf16),
            pltpu.VMEM((tokens * tokens, hidden * hidden), bf16),
            pltpu.VMEM((n, tokens // 2 * t, width), f32),
            pltpu.VMEM((tokens // 2 * tokens, width), f32),
        ],
        name="outer_stage",
    )(*map(in_vmem, lefts), *map(in_vmem, rights), in_vmem(flags), in_vmem(final))


def pair_kernel(sizes, genuine_hbm, own, other, offset, couple_scale, score, tri_scale, picked, slab, block, value, normed, projected, logits, tri, head_rows, genuine, arrived):
    n, rows, cols, heads, feats = sizes
    half, row_index, col_index = lax.axis_index("depth"), lax.axis_index("row"), lax.axis_index("col")
    parts, width = n * n, own.shape[1]
    part, spare = rows // 2, 128 - feats * cols
    copy = pltpu.make_async_copy(genuine_hbm, genuine, arrived)
    copy.start()
    total = own[...] + other[...] + offset[...]
    value[...] = total.astype(bf16).astype(f32)
    unit = unit_rows(value[...])
    size = rows * cols
    padded = normed.shape[0]
    wide = lax.dot_general(
        score[...], unit * couple_scale[...], (((1,), (1,)), ((), ())),
        precision=lax.Precision.HIGHEST, preferred_element_type=f32,
    )
    logits[:, :size] = wide
    lane8 = lax.broadcasted_iota(jnp.int32, (heads, 128), 1)
    low = jnp.full((heads, 128), -jnp.inf, f32)
    for i in range(rows):
        head_rows[pl.ds(i, heads, stride=rows), :] = place_lanes(logits, i * cols, cols, 0, lane8, low)
    t = cols // n
    copy.wait()
    line = lax.broadcasted_iota(jnp.int32, (8, 128), 1)
    bias = jnp.zeros((8, 128), f32)
    open_lanes = jnp.zeros((8, 128), f32)
    for j in range(cols):
        flag = genuine[j // t * rows + col_index * t + j % t].astype(f32)
        bias = jnp.where(line == j, 1000000000.0 * (flag - 1.0), bias)
        here = line == j
        for f in range(1, feats):
            here = here | (line == f * cols + j)
        open_lanes = jnp.where(here, flag, open_lanes)
    score_rows = head_rows[...] + bias[:1]
    peak = jnp.max(score_rows, -1, keepdims=True)
    expo = jnp.exp(score_rows - peak).astype(bf16).astype(f32)
    lane = lax.broadcasted_iota(jnp.int32, (rows, 128), 1)
    zero = jnp.zeros((rows, 128), f32)
    tail = zero
    flat = zero
    for h in range(heads):
        mine = expo[h * rows : (h + 1) * rows]
        start = h * cols
        if start < 128:
            shifted = pltpu.roll(mine, start, 1) if start else mine
            flat = jnp.where((lane >= start) & (lane < start + cols), shifted, flat)
            if start + cols > 128:
                tail = jnp.where(lane < start + cols - 128, shifted, tail)
        else:
            start -= 128
            shifted = pltpu.roll(mine, start, 1) if start else mine
            tail = jnp.where((lane >= start) & (lane < start + cols), shifted, tail)
    first, second = pltpu.roll(tail, 128 - spare, 1), pltpu.roll(tail, 128 - 2 * spare, 1)
    wide_peak = jnp.broadcast_to(peak, (heads * rows, 128))
    tiny = lax.broadcasted_iota(jnp.int32, (8, 128), 1)
    stats = jnp.zeros((8, 128), f32)
    for q in range(3):
        piece = wide_peak.astype(bf16).astype(f32)
        wide_peak = wide_peak - piece
        for a in range(rows // 8):
            for h in range(heads):
                stats = jnp.where(
                    tiny == a * 3 * heads + q * heads + h, piece[h * rows + a * 8 : h * rows + a * 8 + 8], stats
                )
    normed[:size] = (unit * tri_scale[...]).astype(bf16)
    normed[size:] = jnp.zeros((padded - size, width), bf16)
    group = feats * parts
    raw = lax.dot_general(picked[...], normed[...], (((1,), (1,)), ((), ())), preferred_element_type=f32)
    cut = lax.broadcasted_iota(jnp.int32, (parts, 128), 1)
    empty = jnp.zeros((parts, 128), f32)
    for side in range(2):
        base = side * 2 * group
        projected[...] = jax.nn.sigmoid(raw[base : base + group]) * raw[base + group : base + 2 * group]
        for i in range(rows):
            packed = empty
            for f in range(feats):
                packed = place_lanes(projected.at[f * parts : (f + 1) * parts], i * cols, cols, f * cols, cut, packed)
            flag = genuine[row_index * rows + i].astype(f32)
            tri[side, pl.ds(i, parts, stride=rows), :] = packed * (open_lanes[:1] * flag)
    keep = lane < feats * cols
    for p in range(parts):
        slabs = [
            jnp.where(keep, tri[0, p * rows : (p + 1) * rows], first),
            jnp.where(keep, tri[1, p * rows : (p + 1) * rows], second),
            flat,
            stats,
            slab[p],
        ]
        if p < part:
            slabs.append(value[pl.ds(pl.multiple_of((half * part + p) * cols, 8), cols), :])
        else:
            slabs.append(jnp.zeros((cols, width), f32))
        block[p] = jnp.concatenate(slabs, 0).astype(bf16)


def pair_stage(genuine, own, other, offset, couple_scale, score, tri_scale, picked, slab, n, rows, cols):
    parts, width = n * n, own.shape[1]
    heads = score.shape[0]
    feats = width // (2 * parts)
    padded = (rows * cols + 127) // 128 * 128
    vmem = pl.BlockSpec(memory_space=pltpu.VMEM)
    length = 3 * rows + 8 + slab.shape[1] + cols
    return pl.pallas_call(
        functools.partial(pair_kernel, (n, rows, cols, heads, feats)),
        out_shape=pltpu.VMEM((parts, length, 128), bf16),
        in_specs=[pl.BlockSpec(memory_space=pl.ANY)] + [vmem] * 8,
        out_specs=vmem,
        scratch_shapes=[
            pltpu.VMEM((rows * cols, width), f32),
            pltpu.VMEM((padded, width), bf16),
            pltpu.VMEM((feats * parts, padded), f32),
            pltpu.VMEM((heads, padded), f32),
            pltpu.VMEM((2, parts * rows, 128), f32),
            pltpu.VMEM((heads * rows, 128), f32),
            pltpu.SMEM(genuine.shape, genuine.dtype),
            pltpu.SemaphoreType.DMA,
        ],
        name="pair_stage",
    )(genuine, *map(in_vmem, (own, other, offset, couple_scale, score, tri_scale, picked, slab)))


def halves(value):
    high = value.astype(bf16)
    return high, (value - high.astype(f32)).astype(bf16)


def two_pass_dot(value, matrix, axis=0):
    high, low = halves(value)
    over = (((1,), (axis,)), ((), ()))
    return lax.dot_general(high, matrix, over, preferred_element_type=f32) + lax.dot_general(
        low, matrix, over, preferred_element_type=f32
    )


def middle_kernel(sizes, block, seq_scale, content, sigmoid_matrix, final, out, wide, lhs, rhs, product, weights, x, values, gated, masked, revised):
    n, rows, cols, heads, feats, groups, order = sizes
    parts, tokens, ch = n * n, n * rows, final.shape[0]
    s, per = 8, 128 // final.shape[0]
    t = rows // n
    wide[...] = block[...].astype(f32)
    lane = lax.broadcasted_iota(jnp.int32, (tokens, 128), 1)
    small = lax.broadcasted_iota(jnp.int32, (rows, 128), 1)
    tiny = lax.broadcasted_iota(jnp.int32, (8, 128), 1)
    spare = 128 - feats * cols

    def stacked(c, start, count):
        return jnp.concatenate([wide[r * n + c, start : start + count] for r in range(n)], 0)

    rhs[...] = jnp.zeros_like(rhs)
    for c in range(n):
        mine = stacked(c, 0, rows)
        for f in range(feats):
            keep = (lane >= f * cols) & (lane < (f + 1) * cols)
            lhs[f * tokens : (f + 1) * tokens, c * 128 : (c + 1) * 128] = jnp.where(keep, mine, 0.0).astype(bf16)
        rhs[:tokens, c * 128 : (c + 1) * 128] = stacked(c, rows, rows).astype(bf16)
    product[...] = lax.dot_general(lhs[...], rhs[...], (((1,), (1,)), ((), ())), preferred_element_type=f32)
    up = lax.broadcasted_iota(jnp.int32, (256, 128), 0)
    across = lax.broadcasted_iota(jnp.int32, (256, 128), 1)
    gather = ((up >= across * cols) & (up < (across + 1) * cols) & (across < heads)).astype(bf16)
    up = lax.broadcasted_iota(jnp.int32, (128, 256), 0)
    across = lax.broadcasted_iota(jnp.int32, (128, 256), 1)
    spread = ((across >= up * cols) & (across < (up + 1) * cols) & (up < heads)).astype(bf16)
    expos, peaks = [], []
    for c in range(n):
        a, b = stacked(c, 0, rows), stacked(c, rows, rows)
        rest = jnp.where(lane < spare, pltpu.roll(a, spare, 1), jnp.where(lane < 2 * spare, pltpu.roll(b, 2 * spare, 1), 0.0))
        expos.append(jnp.concatenate([stacked(c, 2 * rows, rows), rest], 1))
        peak = []
        for r in range(n):
            stats = wide[r * n + c, 3 * rows : 3 * rows + 8]
            for q in range(rows // 8):
                one = pltpu.roll(stats, (128 - 3 * heads * q) % 128, 1) if q else stats
                peak.append(one + pltpu.roll(one, 128 - heads, 1) + pltpu.roll(one, 128 - 2 * heads, 1))
        peaks.append(jnp.concatenate(peak, 0))
    top = peaks[0]
    for c in range(1, n):
        top = jnp.maximum(top, peaks[c])
    factors = [jnp.exp(peak - top) for peak in peaks]
    total = jnp.zeros_like(top)
    for c in range(n):
        total = total + factors[c] * jnp.dot(expos[c].astype(bf16), gather, preferred_element_type=f32)
    for c in range(n):
        scale = jnp.where(lane < heads, factors[c] / jnp.where(lane < heads, total, 1.0), 0.0)
        weights[:, c * 256 : (c + 1) * 256] = (expos[c] * two_pass_dot(scale, spread)).astype(bf16)
    for p in range(parts):
        for g in range(groups):
            pair = wide[p, 3 * rows + 8 + 8 * g : 3 * rows + 16 + 8 * g]
            for k in range(per):
                x[pl.ds(p * t + g * per + k, s, stride=tokens), :] = pltpu.roll(pair, 128 - k * ch, 1) if k else pair
    raw = x[...][:, :ch]
    centred = raw - jnp.mean(raw, -1, keepdims=True)
    variance = jnp.mean(centred * centred, -1, keepdims=True)
    normed = (centred * lax.rsqrt(variance + epsilon) * seq_scale[...]).astype(bf16)
    values[...] = jnp.dot(normed, content[...], preferred_element_type=f32).astype(bf16).astype(f32)
    gates = jax.nn.sigmoid(jnp.dot(normed, sigmoid_matrix[...], preferred_element_type=f32))
    width = gates.shape[1]
    head_of = lax.broadcasted_iota(jnp.int32, (cols, width), 1) // (width // heads)
    used = heads * cols
    masked[...] = jnp.zeros_like(masked)
    for q in range(s):
        for c in range(n):
            local = jnp.concatenate([values[q * tokens + a : q * tokens + a + m] for a, m in order[c]], 0)
            spread_out = jnp.concatenate([jnp.where(head_of == h, local, 0.0) for h in range(heads)], 0)
            masked[q, c * 256 : c * 256 + used] = spread_out.astype(bf16)
        averaged = jnp.dot(weights[...], masked[q], preferred_element_type=f32)
        gated[q * tokens : (q + 1) * tokens] = gates[q * tokens : (q + 1) * tokens] * averaged
    delta = two_pass_dot(gated[...], final[...], 1)
    revised[:, :ch] = raw + delta
    for p in range(parts):
        r, c = p // n, p % n
        slab = jnp.zeros((rows, 128), f32)
        for f in range(feats):
            shift = ((f - c) * cols) % 128
            piece = product[f * tokens + r * rows : f * tokens + (r + 1) * rows]
            piece = pltpu.roll(piece, shift, 1) if shift else piece
            slab = jnp.where((small >= f * cols) & (small < (f + 1) * cols), piece, slab)
        start = 3 * rows + 8 + 8 * groups + c * t
        slabs = [slab] + [wide[r * n + k, start : start + t] for k in range(n)]
        for g in range(groups):
            merged = revised[pl.ds(p * t + g * per, s, stride=tokens), :]
            for k in range(1, per):
                piece = revised[pl.ds(p * t + g * per + k, s, stride=tokens), :]
                merged = jnp.where(tiny >= k * ch, pltpu.roll(piece, k * ch, 1), merged)
            slabs.append(merged)
        out[p] = jnp.concatenate(slabs, 0).astype(bf16)


def middle_stage(block, n, rows, cols, heads, feats, order, seq_scale, content, sigmoid_matrix, final):
    parts, tokens = n * n, n * rows
    groups = (block.shape[1] - 3 * rows - 8 - cols) // 8
    width = content.shape[1]
    vmem = pl.BlockSpec(memory_space=pltpu.VMEM)
    return pl.pallas_call(
        functools.partial(middle_kernel, (n, rows, cols, heads, feats, groups, order)),
        out_shape=pltpu.VMEM((parts, rows + cols + 8 * groups, 128), bf16),
        in_specs=[vmem] * 5,
        out_specs=vmem,
        scratch_shapes=[
            pltpu.VMEM(block.shape, f32),
            pltpu.VMEM((feats * tokens, n * 128), bf16),
            pltpu.VMEM((128, n * 128), bf16),
            pltpu.VMEM((feats * tokens, 128), f32),
            pltpu.VMEM((tokens, n * 256), bf16),
            pltpu.VMEM((8 * tokens, 128), f32),
            pltpu.VMEM((8 * tokens, width), f32),
            pltpu.VMEM((8 * tokens, width), f32),
            pltpu.VMEM((8, n * 256, width), bf16),
            pltpu.VMEM((8 * tokens, 128), f32),
        ],
        name="middle_stage",
    )(*map(in_vmem, (block, seq_scale, content, sigmoid_matrix, final)))


def turn_kernel(start, own, revised):
    for a in range((own.shape[1] - start) // 8):
        piece = [own[p, start + 8 * a : start + 8 * a + 8].astype(f32) for p in range(own.shape[0])]
        revised[a * 128 : (a + 1) * 128] = jnp.concatenate(piece, 0).T.astype(bf16)


def last_kernel(sizes, own, other, tri_scale, scale, entry, mixed, pair_output, product, turned, pair):
    n, rows, cols, feats = sizes
    parts = n * n
    part, wide = rows // 2, 2 * n * n
    mine = lax.axis_index("depth")
    theirs = 1 - mine
    for p in range(parts):
        here, there = own[p].astype(f32), other[p].astype(f32)
        product[mine, p * rows : (p + 1) * rows] = here[:rows]
        product[theirs, p * rows : (p + 1) * rows] = there[:rows]
        if p < part:
            pair[pl.ds(pl.multiple_of((mine * part + p) * cols, 8), cols), :] = here[rows : rows + cols]
            pair[pl.ds(pl.multiple_of((theirs * part + p) * cols, 8), cols), :] = there[rows : rows + cols]
    lane = lax.broadcasted_iota(jnp.int32, (cols, 128), 1)
    per = 128 // wide
    for g in range(rows // per):
        stacked = []
        for k in range(per):
            for d in range(2):
                stacked.append(product[d, pl.ds(g * per + k, parts, stride=rows), :])
        flipped = jnp.concatenate(stacked, 0).T
        for k in range(per):
            merged = jnp.zeros((cols, 128), f32)
            for f in range(feats):
                merged = place_lanes(flipped[f * cols : (f + 1) * cols], k * wide, wide, f * wide, lane, merged)
            turned[(g * per + k) * cols : (g * per + k + 1) * cols] = merged
    value = pair[...]
    normed = (unit_rows(value) * tri_scale[...]).astype(bf16)
    gate = jax.nn.sigmoid(jnp.dot(normed, entry[...], preferred_element_type=f32))
    result = (unit_rows(turned[...]) * scale[...]).astype(bf16)
    pair_output[...] = (value + gate * jnp.dot(result, mixed[...], preferred_element_type=f32)).astype(bf16)


def last_stage(own, other, tri_scale, gate_entry, scale, mixed, n, rows, cols, t, ch):
    parts, width = n * n, mixed.shape[1]
    feats = width // (2 * parts)
    vmem = pl.BlockSpec(memory_space=pltpu.VMEM)
    revised = pl.pallas_call(
        functools.partial(turn_kernel, rows + cols),
        out_shape=jax.ShapeDtypeStruct((t * ch, 8 * parts), bf16),
        in_specs=[vmem],
        out_specs=vmem,
        name="turn_stage",
    )(in_vmem(own))
    pair_output = pl.pallas_call(
        functools.partial(last_kernel, (n, rows, cols, feats)),
        out_shape=jax.ShapeDtypeStruct((rows * cols, width), bf16),
        in_specs=[vmem] * 6,
        out_specs=vmem,
        scratch_shapes=[
            pltpu.VMEM((2, parts * rows, 128), f32),
            pltpu.VMEM((rows * cols, 128), f32),
            pltpu.VMEM((rows * cols, width), f32),
        ],
        name="last_stage",
    )(*map(in_vmem, (own, other, tri_scale, scale, gate_entry, mixed)))
    return revised.reshape(t, ch, 8 * parts).transpose(2, 0, 1), pair_output.reshape(rows, cols, width)


def on_device(
    sequence_stack,
    present_sequence_flags,
    genuine_residue_flags,
    couple_state,
    tensor_scale,
    tensor_entry_matrix,
    tensor_final_matrix,
    tensor_offset,
    mean_sequence_scale,
    mean_couple_scale,
    mean_score_matrix,
    mean_content_matrix,
    mean_sigmoid_matrix,
    mean_final_matrix,
    trimul_scale,
    trimul_entry_matrix,
    trimul_result_scale,
    trimul_final_matrix,
):
    n = lax.axis_size("row")
    parts = n * n
    rows, cols, width = couple_state.shape
    count, t, ch = sequence_stack.shape
    heads = mean_score_matrix.shape[1]
    feats = width // (2 * parts)
    order = tuple(tuple((r * rows + c * t, t) for r in range(n)) for c in range(n))
    flags = present_sequence_flags.reshape(2, count)
    tokens = sequence_stack.transpose(1, 2, 0)
    *sends, right = first_stage(tokens, flags, tensor_scale.reshape(1, ch), tensor_entry_matrix, couple_state, n)

    def move(array, where):
        pairs = [(r * n + c, where(r, c)[0] * n + where(r, c)[1]) for r in range(n) for c in range(n)]
        return lax.ppermute(array, ("row", "col"), pairs)

    rights = [right] + [move(right, lambda r, c, k=k: (r ^ k, c)) for k in range(1, n)]
    lefts = [sends[0]] + [move(sends[k], lambda r, c, k=k: (r, (c + k) % n)) for k in range(1, n)]
    kept = (
        flags,
        tensor_final_matrix,
        tensor_offset.reshape(1, -1),
        mean_couple_scale.reshape(1, -1),
        mean_score_matrix.T,
        trimul_scale.reshape(1, -1),
        mean_sequence_scale.reshape(1, -1),
        mean_content_matrix,
        mean_sigmoid_matrix,
        mean_final_matrix.T,
    )
    ready = ready_stage(
        right, trimul_entry_matrix, tokens, trimul_result_scale, trimul_final_matrix, kept, n, rows, cols
    )
    lefts, ready = lax.optimization_barrier((lefts, ready))
    picked, slab, gate_entry, mixed, scale, *kept = ready
    flags, outer_final, offset, couple_scale, score, tri_scale, seq_scale, content, sigmoid_matrix, mean_final = kept
    share = outer_stage(lefts, rights, flags, outer_final)
    other = lax.ppermute(share, "depth", [(0, 1), (1, 0)])
    block = pair_stage(
        genuine_residue_flags, share, other, offset, couple_scale, score, tri_scale, picked, slab, n, rows, cols
    )
    block = lax.all_to_all(block, ("row", "col"), 0, 0, tiled=True)
    block = middle_stage(
        block, n, rows, cols, heads, feats, order, seq_scale, content, sigmoid_matrix, mean_final
    )
    block = lax.all_to_all(block, ("row", "col"), 0, 0, tiled=True)
    other = lax.ppermute(block[:, : rows + cols], "depth", [(0, 1), (1, 0)])
    return last_stage(block, other, tri_scale, gate_entry, scale, mixed, n, rows, cols, t, ch)


def suits(mesh):
    return mesh.shape["row"] == mesh.shape["col"] and mesh.shape["depth"] == 2


def solution(mesh):
    placed = (P("depth", ("row", "col"), None), P(), P(), P("row", "col", None)) + (P(),) * 14
    return jax.shard_map(
        on_device if suits(mesh) else on_device_generic,
        mesh=mesh,
        in_specs=placed,
        out_specs=(P("depth", ("row", "col"), None), P("row", "col", None)),
        check_vma=False,
    )
```

```python
import functools

import jax
import jax.numpy as jnp
from jax import lax
from jax.experimental import pallas as pl
from jax.experimental.pallas import tpu as pltpu
from jax.sharding import PartitionSpec as P

epsilon = 1e-05
bf16 = jnp.bfloat16
f32 = jnp.float32


def from_root(array, axis, root):
    mine = lax.axis_index(axis) == root
    return lax.psum(jnp.where(mine, array, jnp.zeros_like(array)), axis)


def standardize_features(value_rows, scale):
    value_rows = value_rows.astype(jnp.float32)
    average = jnp.mean(value_rows, -1, keepdims=True)
    centred = value_rows - average
    variance = jnp.mean(centred * centred, -1, keepdims=True)
    return centred * lax.rsqrt(variance + epsilon) * scale


def on_device_generic(
    sequence_stack,
    present_sequence_flags,
    genuine_residue_flags,
    couple_state,
    tensor_scale,
    tensor_entry_matrix,
    tensor_final_matrix,
    tensor_offset,
    mean_sequence_scale,
    mean_couple_scale,
    mean_score_matrix,
    mean_content_matrix,
    mean_sigmoid_matrix,
    mean_final_matrix,
    trimul_scale,
    trimul_entry_matrix,
    trimul_result_scale,
    trimul_final_matrix,
):
    n_row = lax.axis_size("row")
    n_col = lax.axis_size("col")
    row_index = lax.axis_index("row")
    col_index = lax.axis_index("col")
    depth_position = lax.axis_index("depth")
    piece_rows, piece_columns, width = couple_state.shape
    sequence_count, shard_residues, ignored_quantity = sequence_stack.shape
    hidden = tensor_entry_matrix.shape[1] // 2
    head_split = mean_score_matrix.shape[1]
    head_channels = mean_content_matrix.shape[1] // head_split
    token_weight = genuine_residue_flags.astype(jnp.float32)
    mask_as_float = present_sequence_flags.astype(jnp.float32)
    row_softmax_weight = lax.dynamic_slice_in_dim(
        mask_as_float, depth_position * sequence_count, sequence_count
    )
    row_count = jnp.sum(mask_as_float)
    entire_sequences = lax.all_gather(sequence_stack, "col", axis=1, tiled=True)
    root_row = col_index * n_row // n_col
    offset = col_index * piece_columns - root_row * piece_rows
    column_piece = lax.dynamic_slice_in_dim(entire_sequences, offset, piece_columns, 1)
    whole_cols = from_root(column_piece, "row", root_row)
    opm_rows = standardize_features(entire_sequences, tensor_scale).astype(jnp.bfloat16)
    opm_cols = standardize_features(whole_cols, tensor_scale).astype(jnp.bfloat16)
    left_projection = (
        jnp.dot(opm_rows, tensor_entry_matrix[:, :hidden], preferred_element_type=jnp.float32)
        * row_softmax_weight[:, None, None]
    ).astype(jnp.bfloat16)
    right_proj = (
        jnp.dot(opm_cols, tensor_entry_matrix[:, hidden:], preferred_element_type=jnp.float32)
        * row_softmax_weight[:, None, None]
    ).astype(jnp.bfloat16)
    outer_sum = jnp.einsum(
        "sic,sjd->ijcd", left_projection, right_proj, preferred_element_type=jnp.float32
    )
    outer_sum = outer_sum.reshape(piece_rows, piece_columns, hidden * hidden)
    out_float = tensor_final_matrix.astype(jnp.float32)
    outer_share = lax.psum_scatter(outer_sum, "depth", scatter_dimension=0, tiled=True)
    share_rows = outer_share.shape[0]
    pair_share = lax.dynamic_slice_in_dim(couple_state, depth_position * share_rows, share_rows, 0)
    update = (
        jnp.dot(outer_share, out_float, precision=lax.Precision.HIGHEST) / (row_count + 0.001)
        + tensor_offset
    )
    new_share = (pair_share.astype(jnp.float32) + update).astype(jnp.bfloat16)
    pair_one = lax.all_gather(new_share, "depth", axis=0, tiled=True)
    row_tokens = lax.dynamic_slice_in_dim(token_weight, row_index * piece_rows, piece_rows)
    col_tokens = lax.dynamic_slice_in_dim(token_weight, col_index * piece_columns, piece_columns)
    logits = jnp.einsum(
        "ijc,ch->ijh",
        standardize_features(pair_one, mean_couple_scale),
        mean_score_matrix,
        precision=lax.Precision.HIGHEST,
    )
    logits = logits + 1000000000.0 * (col_tokens - 1.0)[None, :, None]
    peak = lax.pmax(jnp.max(logits, axis=1), "col")
    expo = jnp.exp(logits - peak[:, None, :])
    total = lax.psum(jnp.sum(expo, axis=1), "col")
    weights = (expo / total[:, None, :]).astype(jnp.bfloat16)
    col_normed = standardize_features(whole_cols, mean_sequence_scale).astype(jnp.bfloat16)
    value_rows = jnp.dot(
        col_normed, mean_content_matrix, preferred_element_type=jnp.float32
    ).astype(jnp.bfloat16)
    value_rows = value_rows.reshape(sequence_count, piece_columns, head_split, head_channels)
    averaged_values = jnp.einsum(
        "ijh,sjhe->sihe", weights, value_rows, preferred_element_type=jnp.float32
    )
    averaged_values = averaged_values.reshape(
        sequence_count, piece_rows, head_split * head_channels
    )
    output_weight = mean_final_matrix.astype(jnp.float32)
    local_portion = lax.psum_scatter(
        averaged_values.astype(jnp.bfloat16), "col", scatter_dimension=1, tiled=True
    ).astype(jnp.float32)
    shard_standardized = standardize_features(sequence_stack, mean_sequence_scale).astype(
        jnp.bfloat16
    )
    gate_values = jax.nn.sigmoid(
        jnp.dot(shard_standardized, mean_sigmoid_matrix, preferred_element_type=jnp.float32)
    )
    sequence_delta = jnp.dot(
        gate_values * local_portion, output_weight, precision=lax.Precision.HIGHEST
    )
    revised_sequences = (sequence_stack.astype(jnp.float32) + sequence_delta).astype(jnp.bfloat16)
    tri_normed = standardize_features(pair_one, trimul_scale).astype(jnp.bfloat16)
    projected = jnp.dot(tri_normed, trimul_entry_matrix, preferred_element_type=jnp.float32)
    pair_mask = (row_tokens[:, None] * col_tokens[None, :])[..., None]
    tri_left = (
        jax.nn.sigmoid(projected[..., 0:width]) * projected[..., width : 2 * width] * pair_mask
    ).astype(jnp.bfloat16)
    tri_right = (
        jax.nn.sigmoid(projected[..., 2 * width : 3 * width])
        * projected[..., 3 * width : 4 * width]
        * pair_mask
    ).astype(jnp.bfloat16)
    out_gate = jax.nn.sigmoid(projected[..., 4 * width : 5 * width])
    left_rows, right_rows = (
        lax.all_gather(tri_left, "col", axis=1, tiled=True),
        lax.all_gather(tri_right, "col", axis=1, tiled=True),
    )
    right_piece = lax.dynamic_slice_in_dim(right_rows, offset, piece_columns, 0)
    right_needed = from_root(right_piece, "row", root_row)
    product = jnp.einsum(
        "ikc,jkc->ijc", left_rows, right_needed, preferred_element_type=jnp.float32
    )
    final = out_gate * jnp.dot(
        standardize_features(product, trimul_result_scale).astype(jnp.bfloat16),
        trimul_final_matrix,
        preferred_element_type=jnp.float32,
    )
    pair_output = (pair_one.astype(jnp.float32) + final).astype(jnp.bfloat16)
    return (revised_sequences, pair_output)


def in_vmem(array):
    return pltpu.with_memory_space_constraint(array, pltpu.VMEM)


def place_lanes(source, start, count, target, lane, base):
    block, offset = start // 128, start % 128
    shift = (target - offset) % 128
    piece = source[:, block * 128 : (block + 1) * 128]
    piece = pltpu.roll(piece, shift, 1) if shift else piece
    if offset + count > 128:
        rest = source[:, (block + 1) * 128 : (block + 2) * 128]
        rest = pltpu.roll(rest, shift, 1) if shift else rest
        piece = jnp.where(lane < target + 128 - offset, piece, rest)
    return jnp.where((lane >= target) & (lane < target + count), piece, base)


def unit_rows(value):
    centred = value - jnp.mean(value, -1, keepdims=True)
    variance = jnp.mean(centred * centred, -1, keepdims=True)
    return centred * lax.rsqrt(variance + epsilon)


def first_kernel(tokens_hbm, flags_hbm, scale_hbm, entry_hbm, couple_hbm, *refs):
    n = len(refs) - 8
    sends, right, pieces, tokens, couple, flags, scale, entry, arrived = refs[:n], refs[n], *refs[n + 1 :]
    t, ch, s = tokens.shape
    hidden, part = entry.shape[1] // 2, couple.shape[0]
    half, place = lax.axis_index("depth"), lax.axis_index("col")
    copies = [
        pltpu.make_async_copy(tokens_hbm, tokens, arrived.at[0]),
        pltpu.make_async_copy(couple_hbm.at[pl.ds(half * part, part)], couple, arrived.at[1]),
        pltpu.make_async_copy(flags_hbm, flags, arrived.at[2]),
        pltpu.make_async_copy(scale_hbm, scale, arrived.at[3]),
        pltpu.make_async_copy(entry_hbm, entry, arrived.at[4]),
    ]
    for copy in copies:
        copy.start()
    for copy in copies[2:]:
        copy.wait()
    mask = flags[pl.ds(half, 1), :].astype(f32)
    square = (ch, ch)
    diagonal = lax.broadcasted_iota(jnp.int32, square, 0) == lax.broadcasted_iota(jnp.int32, square, 1)
    column = jnp.sum(jnp.where(diagonal, scale[...], 0.0), 1, keepdims=True)
    copies[0].wait()
    lefts = []
    for u in range(t):
        value = tokens[u].astype(f32)
        centred = value - jnp.mean(value, 0, keepdims=True)
        variance = jnp.mean(centred * centred, 0, keepdims=True)
        normed = (centred * lax.rsqrt(variance + epsilon) * column).astype(bf16)
        factor = lax.dot_general(entry[...], normed, (((0,), (0,)), ((), ())), preferred_element_type=f32) * mask
        lefts.append(factor[:hidden])
        right[u] = factor[hidden:].astype(bf16)
    copies[1].wait()
    for i in range(part):
        row = couple[i].astype(f32)
        for k in range(n):
            pieces[k, i * t : (i + 1) * t] = row[k * t : (k + 1) * t]
    for k in range(n):
        sends[k][...] = jnp.concatenate(lefts + [pieces[lax.rem(place + k, n)]], 0).astype(bf16)


def first_stage(tokens, flags, scale, entry, couple, n):
    t, ch, s = tokens.shape
    rows, cols, width = couple.shape
    hidden = entry.shape[1] // 2
    vmem, hbm = pl.BlockSpec(memory_space=pltpu.VMEM), pl.BlockSpec(memory_space=pl.ANY)
    length = t * hidden + rows // 2 * t
    return pl.pallas_call(
        first_kernel,
        out_shape=[pltpu.VMEM((length, s), bf16)] * n + [pltpu.VMEM((t, hidden, s), bf16)],
        in_specs=[hbm] * 5,
        out_specs=[vmem] * (n + 1),
        scratch_shapes=[
            pltpu.VMEM((n, rows // 2 * t, width), f32),
            pltpu.VMEM(tokens.shape, bf16),
            pltpu.VMEM((rows // 2, cols, width), bf16),
            pltpu.VMEM(flags.shape, flags.dtype),
            pltpu.VMEM(scale.shape, f32),
            pltpu.VMEM(entry.shape, bf16),
            pltpu.SemaphoreType.DMA((5,)),
        ],
        name="first_stage",
    )(tokens, flags, scale, entry, couple)


def ready_kernel(sizes, *refs):
    n, rows, cols, feats = sizes
    parts = n * n
    kept = (len(refs) - 17) // 2
    after, result_scale_hbm, entry_hbm, tokens_hbm, final_hbm = refs[:5]
    picked, slab, gate_entry, mixed, scale = refs[5 + kept : 10 + kept]
    entry, tokens, turned_entry, final, plain, result_scale, arrived = refs[10 + 2 * kept :]
    half = lax.axis_index("depth")
    width, group, wide = entry.shape[0], feats * parts, 2 * parts
    copies = [
        pltpu.make_async_copy(entry_hbm.at[:, pl.ds(0, 4 * width)], entry, arrived.at[0]),
        pltpu.make_async_copy(tokens_hbm, tokens, arrived.at[1]),
        pltpu.make_async_copy(entry_hbm.at[:, pl.ds(4 * width, width)], gate_entry, arrived.at[2]),
        pltpu.make_async_copy(final_hbm, final, arrived.at[3]),
        pltpu.make_async_copy(result_scale_hbm, result_scale, arrived.at[4]),
    ]
    for k in range(kept):
        copies.append(pltpu.make_async_copy(refs[5 + k], refs[10 + kept + k], arrived.at[5 + k]))
    for copy in copies:
        copy.start()
    t, ch, s = tokens.shape
    copies[4].wait()
    at = lax.broadcasted_iota(jnp.int32, (width, width), 1)
    origin = lax.broadcasted_iota(jnp.int32, (width, width), 0)
    goal = lax.rem(origin, feats) * wide + lax.div(origin, feats)
    scale[...] = jnp.dot(
        result_scale[...], (at == goal).astype(f32), precision=lax.Precision.HIGHEST, preferred_element_type=f32
    )
    copies[0].wait()
    turned_entry[...] = entry[...].astype(f32).T
    for k in range(4):
        start = pl.multiple_of(k * width + half * group, 8)
        turned_entry[k * group : (k + 1) * group] = turned_entry[pl.ds(start, group), :]
    for k in range(4):
        for f in range(feats):
            picked[(k * feats + f) * parts : (k * feats + f + 1) * parts] = turned_entry[
                pl.ds(k * group + f, parts, stride=feats), :
            ].astype(bf16)
    copies[1].wait()
    turned = tokens[...].astype(f32).reshape(t * ch, s).T
    for p in range(parts):
        slab[p] = jnp.concatenate(
            [turned[p * 8 : (p + 1) * 8, a * 128 : (a + 1) * 128] for a in range(t * ch // 128)], 0
        )
    for copy in copies[2:4] + copies[5:]:
        copy.wait()
    plain[...] = final[...].astype(f32)
    for f in range(feats):
        mixed[f * wide : (f + 1) * wide] = plain[pl.ds(f, wide, stride=feats), :].astype(bf16)


def ready_stage(after, entry, tokens, result_scale, final, kept, n, rows, cols):
    parts, width = n * n, entry.shape[0]
    feats = width // (2 * parts)
    t, ch, s = tokens.shape
    vmem, hbm = pl.BlockSpec(memory_space=pltpu.VMEM), pl.BlockSpec(memory_space=pl.ANY)
    return pl.pallas_call(
        functools.partial(ready_kernel, (n, rows, cols, feats)),
        out_shape=[
            pltpu.VMEM((4 * feats * parts, width), bf16),
            pltpu.VMEM((parts, t * ch // 128 * 8, 128), f32),
            pltpu.VMEM((width, width), bf16),
            pltpu.VMEM((width, width), bf16),
            pltpu.VMEM((1, width), f32),
        ]
        + [pltpu.VMEM(array.shape, array.dtype) for array in kept],
        in_specs=[hbm] * (5 + len(kept)),
        out_specs=[vmem] * (5 + len(kept)),
        scratch_shapes=[
            pltpu.VMEM((width, 4 * width), bf16),
            pltpu.VMEM(tokens.shape, bf16),
            pltpu.VMEM((4 * width, width), f32),
            pltpu.VMEM((width, width), bf16),
            pltpu.VMEM((width, width), f32),
            pltpu.VMEM((1, width), f32),
            pltpu.SemaphoreType.DMA((5 + len(kept),)),
        ],
        name="ready_stage",
    )(in_vmem(after), result_scale.reshape(1, -1), entry, tokens, final, *kept)


def outer_kernel(n, *refs):
    half, row_index, col_index = lax.axis_index("depth"), lax.axis_index("row"), lax.axis_index("col")
    lefts, rights = refs[:n], refs[n : 2 * n]
    t, hidden, s = rights[0].shape
    flags, final, out, left, pieces, right, plain, turned, outer, high, low, couples, couple = refs[2 * n :]
    tokens, ratio = n * t, 128 // hidden
    for k in range(n):
        sent = lefts[k][...].astype(f32)
        place = lax.rem(col_index + (n - k), n)
        left[place] = sent[: t * hidden].astype(bf16)
        couples[place] = sent[t * hidden :]
        pieces[row_index ^ k] = rights[k][...].reshape(t * hidden, s).astype(f32)
    for k in range(n):
        for u in range(t):
            right[pl.ds(k * t + u, hidden, stride=tokens), :] = pieces[k, u * hidden : (u + 1) * hidden, :]
    outer[...] = lax.dot_general(
        right[...].astype(bf16),
        left[...].reshape(tokens * hidden, s),
        (((1,), (1,)), ((), ())),
        preferred_element_type=f32,
    )
    plain[...] = final[...].astype(f32)
    for d in range(hidden):
        turned[d * hidden : (d + 1) * hidden, :] = plain[pl.ds(d, hidden, stride=hidden), :].astype(bf16)
    lane = lax.broadcasted_iota(jnp.int32, (tokens, 128), 1)
    for g in range(tokens // ratio):
        for q in range(hidden // ratio):
            tiles = [
                outer[(q * ratio + d) * tokens : (q * ratio + d + 1) * tokens, g * 128 : (g + 1) * 128]
                for d in range(ratio)
            ]
            bit = 1
            while bit < ratio:
                upper = (lane // (hidden * bit)) % 2 == 1
                for x in range(ratio):
                    if x & bit:
                        continue
                    a, b = tiles[x], tiles[x | bit]
                    tiles[x] = jnp.where(upper, pltpu.roll(b, hidden * bit, 1), a)
                    tiles[x | bit] = jnp.where(upper, b, pltpu.roll(a, 128 - hidden * bit, 1))
                bit *= 2
            for x in range(ratio):
                i = g * ratio + x
                rounded = tiles[x].astype(bf16)
                high[i * tokens : (i + 1) * tokens, q * 128 : (q + 1) * 128] = rounded
                low[i * tokens : (i + 1) * tokens, q * 128 : (q + 1) * 128] = (
                    tiles[x] - rounded.astype(f32)
                ).astype(bf16)
    part = tokens // 2
    for k in range(n):
        for i in range(part):
            couple[i * tokens + k * t : i * tokens + (k + 1) * t] = couples[k, i * t : (i + 1) * t]
    total = jnp.sum(flags[...].astype(f32)) + 0.001
    update = jnp.dot(high[...], turned[...], preferred_element_type=f32) + jnp.dot(
        low[...], turned[...], preferred_element_type=f32
    )
    out[...] = update / total
    mine = pl.ds(pl.multiple_of(half * (part * tokens), 8), part * tokens)
    out[mine, :] = out[mine, :] + couple[...]


def outer_stage(lefts, rights, flags, final):
    n = len(lefts)
    t, hidden, s = rights[0].shape
    tokens, width = n * t, final.shape[1]
    vmem = pl.BlockSpec(memory_space=pltpu.VMEM)
    return pl.pallas_call(
        functools.partial(outer_kernel, n),
        out_shape=pltpu.VMEM((tokens * tokens, width), f32),
        in_specs=[vmem] * (2 * n + 2),
        out_specs=vmem,
        scratch_shapes=[
            pltpu.VMEM((n, t * hidden, s), bf16),
            pltpu.VMEM((n, t * hidden, s), f32),
            pltpu.VMEM((tokens * hidden, s), f32),
            pltpu.VMEM((hidden * hidden, width), f32),
            pltpu.VMEM((hidden * hidden, width), bf16),
            pltpu.VMEM((tokens * hidden, tokens * hidden), f32),
            pltpu.VMEM((tokens * tokens, hidden * hidden), bf16),
            pltpu.VMEM((tokens * tokens, hidden * hidden), bf16),
            pltpu.VMEM((n, tokens // 2 * t, width), f32),
            pltpu.VMEM((tokens // 2 * tokens, width), f32),
        ],
        name="outer_stage",
    )(*map(in_vmem, lefts), *map(in_vmem, rights), in_vmem(flags), in_vmem(final))


def pair_kernel(sizes, genuine_hbm, own, other, offset, couple_scale, score, tri_scale, picked, slab, block, value, normed, projected, logits, tri, head_rows, genuine, arrived):
    n, rows, cols, heads, feats = sizes
    half, row_index, col_index = lax.axis_index("depth"), lax.axis_index("row"), lax.axis_index("col")
    parts, width = n * n, own.shape[1]
    part, spare = rows // 2, 128 - feats * cols
    copy = pltpu.make_async_copy(genuine_hbm, genuine, arrived)
    copy.start()
    total = own[...] + other[...] + offset[...]
    value[...] = total.astype(bf16).astype(f32)
    unit = unit_rows(value[...])
    size = rows * cols
    padded = normed.shape[0]
    wide = lax.dot_general(
        score[...], unit * couple_scale[...], (((1,), (1,)), ((), ())),
        precision=lax.Precision.HIGHEST, preferred_element_type=f32,
    )
    logits[:, :size] = wide
    lane8 = lax.broadcasted_iota(jnp.int32, (heads, 128), 1)
    low = jnp.full((heads, 128), -jnp.inf, f32)
    for i in range(rows):
        head_rows[pl.ds(i, heads, stride=rows), :] = place_lanes(logits, i * cols, cols, 0, lane8, low)
    t = cols // n
    copy.wait()
    line = lax.broadcasted_iota(jnp.int32, (8, 128), 1)
    bias = jnp.zeros((8, 128), f32)
    open_lanes = jnp.zeros((8, 128), f32)
    for j in range(cols):
        flag = genuine[j // t * rows + col_index * t + j % t].astype(f32)
        bias = jnp.where(line == j, 1000000000.0 * (flag - 1.0), bias)
        here = line == j
        for f in range(1, feats):
            here = here | (line == f * cols + j)
        open_lanes = jnp.where(here, flag, open_lanes)
    score_rows = head_rows[...] + bias[:1]
    peak = jnp.max(score_rows, -1, keepdims=True)
    expo = jnp.exp(score_rows - peak).astype(bf16).astype(f32)
    lane = lax.broadcasted_iota(jnp.int32, (rows, 128), 1)
    zero = jnp.zeros((rows, 128), f32)
    tail = zero
    flat = zero
    for h in range(heads):
        mine = expo[h * rows : (h + 1) * rows]
        start = h * cols
        if start < 128:
            shifted = pltpu.roll(mine, start, 1) if start else mine
            flat = jnp.where((lane >= start) & (lane < start + cols), shifted, flat)
            if start + cols > 128:
                tail = jnp.where(lane < start + cols - 128, shifted, tail)
        else:
            start -= 128
            shifted = pltpu.roll(mine, start, 1) if start else mine
            tail = jnp.where((lane >= start) & (lane < start + cols), shifted, tail)
    first, second = pltpu.roll(tail, 128 - spare, 1), pltpu.roll(tail, 128 - 2 * spare, 1)
    wide_peak = jnp.broadcast_to(peak, (heads * rows, 128))
    tiny = lax.broadcasted_iota(jnp.int32, (8, 128), 1)
    stats = jnp.zeros((8, 128), f32)
    for q in range(3):
        piece = wide_peak.astype(bf16).astype(f32)
        wide_peak = wide_peak - piece
        for a in range(rows // 8):
            for h in range(heads):
                stats = jnp.where(
                    tiny == a * 3 * heads + q * heads + h, piece[h * rows + a * 8 : h * rows + a * 8 + 8], stats
                )
    normed[:size] = (unit * tri_scale[...]).astype(bf16)
    normed[size:] = jnp.zeros((padded - size, width), bf16)
    group = feats * parts
    raw = lax.dot_general(picked[...], normed[...], (((1,), (1,)), ((), ())), preferred_element_type=f32)
    cut = lax.broadcasted_iota(jnp.int32, (parts, 128), 1)
    empty = jnp.zeros((parts, 128), f32)
    for side in range(2):
        base = side * 2 * group
        projected[...] = jax.nn.sigmoid(raw[base : base + group]) * raw[base + group : base + 2 * group]
        for i in range(rows):
            packed = empty
            for f in range(feats):
                packed = place_lanes(projected.at[f * parts : (f + 1) * parts], i * cols, cols, f * cols, cut, packed)
            flag = genuine[row_index * rows + i].astype(f32)
            tri[side, pl.ds(i, parts, stride=rows), :] = packed * (open_lanes[:1] * flag)
    keep = lane < feats * cols
    for p in range(parts):
        slabs = [
            jnp.where(keep, tri[0, p * rows : (p + 1) * rows], first),
            jnp.where(keep, tri[1, p * rows : (p + 1) * rows], second),
            flat,
            stats,
            slab[p],
        ]
        if p < part:
            slabs.append(value[pl.ds(pl.multiple_of((half * part + p) * cols, 8), cols), :])
        else:
            slabs.append(jnp.zeros((cols, width), f32))
        block[p] = jnp.concatenate(slabs, 0).astype(bf16)


def pair_stage(genuine, own, other, offset, couple_scale, score, tri_scale, picked, slab, n, rows, cols):
    parts, width = n * n, own.shape[1]
    heads = score.shape[0]
    feats = width // (2 * parts)
    padded = (rows * cols + 127) // 128 * 128
    vmem = pl.BlockSpec(memory_space=pltpu.VMEM)
    length = 3 * rows + 8 + slab.shape[1] + cols
    return pl.pallas_call(
        functools.partial(pair_kernel, (n, rows, cols, heads, feats)),
        out_shape=pltpu.VMEM((parts, length, 128), bf16),
        in_specs=[pl.BlockSpec(memory_space=pl.ANY)] + [vmem] * 8,
        out_specs=vmem,
        scratch_shapes=[
            pltpu.VMEM((rows * cols, width), f32),
            pltpu.VMEM((padded, width), bf16),
            pltpu.VMEM((feats * parts, padded), f32),
            pltpu.VMEM((heads, padded), f32),
            pltpu.VMEM((2, parts * rows, 128), f32),
            pltpu.VMEM((heads * rows, 128), f32),
            pltpu.SMEM(genuine.shape, genuine.dtype),
            pltpu.SemaphoreType.DMA,
        ],
        name="pair_stage",
    )(genuine, *map(in_vmem, (own, other, offset, couple_scale, score, tri_scale, picked, slab)))


def halves(value):
    high = value.astype(bf16)
    return high, (value - high.astype(f32)).astype(bf16)


def two_pass_dot(value, matrix, axis=0):
    high, low = halves(value)
    over = (((1,), (axis,)), ((), ()))
    return lax.dot_general(high, matrix, over, preferred_element_type=f32) + lax.dot_general(
        low, matrix, over, preferred_element_type=f32
    )


def middle_kernel(sizes, block, seq_scale, content, sigmoid_matrix, final, out, wide, lhs, rhs, product, weights, x, values, gated, masked, revised):
    n, rows, cols, heads, feats, groups, order = sizes
    parts, tokens, ch = n * n, n * rows, final.shape[0]
    s, per = 8, 128 // final.shape[0]
    t = rows // n
    wide[...] = block[...].astype(f32)
    lane = lax.broadcasted_iota(jnp.int32, (tokens, 128), 1)
    small = lax.broadcasted_iota(jnp.int32, (rows, 128), 1)
    tiny = lax.broadcasted_iota(jnp.int32, (8, 128), 1)
    spare = 128 - feats * cols

    def stacked(c, start, count):
        return jnp.concatenate([wide[c * n + r, start : start + count] for r in range(n)], 0)

    rhs[...] = jnp.zeros_like(rhs)
    for c in range(n):
        mine = stacked(c, 0, rows)
        for f in range(feats):
            keep = (lane >= f * cols) & (lane < (f + 1) * cols)
            lhs[f * tokens : (f + 1) * tokens, c * 128 : (c + 1) * 128] = jnp.where(keep, mine, 0.0).astype(bf16)
        rhs[:tokens, c * 128 : (c + 1) * 128] = stacked(c, rows, rows).astype(bf16)
    product[...] = lax.dot_general(lhs[...], rhs[...], (((1,), (1,)), ((), ())), preferred_element_type=f32)
    up = lax.broadcasted_iota(jnp.int32, (256, 128), 0)
    across = lax.broadcasted_iota(jnp.int32, (256, 128), 1)
    gather = ((up >= across * cols) & (up < (across + 1) * cols) & (across < heads)).astype(bf16)
    up = lax.broadcasted_iota(jnp.int32, (128, 256), 0)
    across = lax.broadcasted_iota(jnp.int32, (128, 256), 1)
    spread = ((across >= up * cols) & (across < (up + 1) * cols) & (up < heads)).astype(bf16)
    expos, peaks = [], []
    for c in range(n):
        a, b = stacked(c, 0, rows), stacked(c, rows, rows)
        rest = jnp.where(lane < spare, pltpu.roll(a, spare, 1), jnp.where(lane < 2 * spare, pltpu.roll(b, 2 * spare, 1), 0.0))
        expos.append(jnp.concatenate([stacked(c, 2 * rows, rows), rest], 1))
        peak = []
        for r in range(n):
            stats = wide[c * n + r, 3 * rows : 3 * rows + 8]
            for q in range(rows // 8):
                one = pltpu.roll(stats, (128 - 3 * heads * q) % 128, 1) if q else stats
                peak.append(one + pltpu.roll(one, 128 - heads, 1) + pltpu.roll(one, 128 - 2 * heads, 1))
        peaks.append(jnp.concatenate(peak, 0))
    top = peaks[0]
    for c in range(1, n):
        top = jnp.maximum(top, peaks[c])
    factors = [jnp.exp(peak - top) for peak in peaks]
    total = jnp.zeros_like(top)
    for c in range(n):
        total = total + factors[c] * jnp.dot(expos[c].astype(bf16), gather, preferred_element_type=f32)
    for c in range(n):
        scale = jnp.where(lane < heads, factors[c] / jnp.where(lane < heads, total, 1.0), 0.0)
        weights[:, c * 256 : (c + 1) * 256] = (expos[c] * two_pass_dot(scale, spread)).astype(bf16)
    first_token = [((p % n) * n + p // n) * t for p in range(parts)]
    for p in range(parts):
        for g in range(groups):
            pair = wide[p, 3 * rows + 8 + 8 * g : 3 * rows + 16 + 8 * g]
            for k in range(per):
                x[pl.ds(first_token[p] + g * per + k, s, stride=tokens), :] = pltpu.roll(pair, 128 - k * ch, 1) if k else pair
    raw = x[...][:, :ch]
    centred = raw - jnp.mean(raw, -1, keepdims=True)
    variance = jnp.mean(centred * centred, -1, keepdims=True)
    normed = (centred * lax.rsqrt(variance + epsilon) * seq_scale[...]).astype(bf16)
    values[...] = jnp.dot(normed, content[...], preferred_element_type=f32).astype(bf16).astype(f32)
    gates = jax.nn.sigmoid(jnp.dot(normed, sigmoid_matrix[...], preferred_element_type=f32))
    width = gates.shape[1]
    head_of = lax.broadcasted_iota(jnp.int32, (cols, width), 1) // (width // heads)
    used = heads * cols
    masked[...] = jnp.zeros_like(masked)
    for q in range(s):
        for c in range(n):
            local = jnp.concatenate([values[q * tokens + a : q * tokens + a + m] for a, m in order[c]], 0)
            spread_out = jnp.concatenate([jnp.where(head_of == h, local, 0.0) for h in range(heads)], 0)
            masked[q, c * 256 : c * 256 + used] = spread_out.astype(bf16)
        averaged = jnp.dot(weights[...], masked[q], preferred_element_type=f32)
        gated[q * tokens : (q + 1) * tokens] = gates[q * tokens : (q + 1) * tokens] * averaged
    delta = two_pass_dot(gated[...], final[...], 1)
    revised[:, :ch] = raw + delta
    for p in range(parts):
        c, r = p // n, p % n
        slab = jnp.zeros((rows, 128), f32)
        for f in range(feats):
            shift = ((f - c) * cols) % 128
            piece = product[f * tokens + r * rows : f * tokens + (r + 1) * rows]
            piece = pltpu.roll(piece, shift, 1) if shift else piece
            slab = jnp.where((small >= f * cols) & (small < (f + 1) * cols), piece, slab)
        start = 3 * rows + 8 + 8 * groups + c * t
        slabs = [slab] + [wide[k * n + r, start : start + t] for k in range(n)]
        for g in range(groups):
            merged = revised[pl.ds(first_token[p] + g * per, s, stride=tokens), :]
            for k in range(1, per):
                piece = revised[pl.ds(first_token[p] + g * per + k, s, stride=tokens), :]
                merged = jnp.where(tiny >= k * ch, pltpu.roll(piece, k * ch, 1), merged)
            slabs.append(merged)
        out[p] = jnp.concatenate(slabs, 0).astype(bf16)


def middle_stage(block, n, rows, cols, heads, feats, order, seq_scale, content, sigmoid_matrix, final):
    parts, tokens = n * n, n * rows
    groups = (block.shape[1] - 3 * rows - 8 - cols) // 8
    width = content.shape[1]
    vmem = pl.BlockSpec(memory_space=pltpu.VMEM)
    return pl.pallas_call(
        functools.partial(middle_kernel, (n, rows, cols, heads, feats, groups, order)),
        out_shape=pltpu.VMEM((parts, rows + cols + 8 * groups, 128), bf16),
        in_specs=[vmem] * 5,
        out_specs=vmem,
        scratch_shapes=[
            pltpu.VMEM(block.shape, f32),
            pltpu.VMEM((feats * tokens, n * 128), bf16),
            pltpu.VMEM((128, n * 128), bf16),
            pltpu.VMEM((feats * tokens, 128), f32),
            pltpu.VMEM((tokens, n * 256), bf16),
            pltpu.VMEM((8 * tokens, 128), f32),
            pltpu.VMEM((8 * tokens, width), f32),
            pltpu.VMEM((8 * tokens, width), f32),
            pltpu.VMEM((8, n * 256, width), bf16),
            pltpu.VMEM((8 * tokens, 128), f32),
        ],
        name="middle_stage",
    )(*map(in_vmem, (block, seq_scale, content, sigmoid_matrix, final)))


def turn_kernel(start, own, revised):
    for a in range((own.shape[1] - start) // 8):
        piece = [own[p, start + 8 * a : start + 8 * a + 8].astype(f32) for p in range(own.shape[0])]
        revised[a * 128 : (a + 1) * 128] = jnp.concatenate(piece, 0).T.astype(bf16)


def last_kernel(sizes, own, other, tri_scale, scale, entry, mixed, pair_output, product, turned, pair):
    n, rows, cols, feats = sizes
    parts = n * n
    part, wide = rows // 2, 2 * n * n
    mine = lax.axis_index("depth")
    theirs = 1 - mine
    for p in range(parts):
        here, there = own[p].astype(f32), other[p].astype(f32)
        product[mine, p * rows : (p + 1) * rows] = here[:rows]
        product[theirs, p * rows : (p + 1) * rows] = there[:rows]
        if p < part:
            pair[pl.ds(pl.multiple_of((mine * part + p) * cols, 8), cols), :] = here[rows : rows + cols]
            pair[pl.ds(pl.multiple_of((theirs * part + p) * cols, 8), cols), :] = there[rows : rows + cols]
    lane = lax.broadcasted_iota(jnp.int32, (cols, 128), 1)
    per = 128 // wide
    for g in range(rows // per):
        stacked = []
        for k in range(per):
            for d in range(2):
                stacked.append(product[d, pl.ds(g * per + k, parts, stride=rows), :])
        flipped = jnp.concatenate(stacked, 0).T
        for k in range(per):
            merged = jnp.zeros((cols, 128), f32)
            for f in range(feats):
                merged = place_lanes(flipped[f * cols : (f + 1) * cols], k * wide, wide, f * wide, lane, merged)
            turned[(g * per + k) * cols : (g * per + k + 1) * cols] = merged
    value = pair[...]
    normed = (unit_rows(value) * tri_scale[...]).astype(bf16)
    gate = jax.nn.sigmoid(jnp.dot(normed, entry[...], preferred_element_type=f32))
    result = (unit_rows(turned[...]) * scale[...]).astype(bf16)
    pair_output[...] = (value + gate * jnp.dot(result, mixed[...], preferred_element_type=f32)).astype(bf16)


def last_stage(own, other, tri_scale, gate_entry, scale, mixed, n, rows, cols, t, ch):
    parts, width = n * n, mixed.shape[1]
    feats = width // (2 * parts)
    vmem = pl.BlockSpec(memory_space=pltpu.VMEM)
    revised = pl.pallas_call(
        functools.partial(turn_kernel, rows + cols),
        out_shape=jax.ShapeDtypeStruct((t * ch, 8 * parts), bf16),
        in_specs=[vmem],
        out_specs=vmem,
        name="turn_stage",
    )(in_vmem(own))
    pair_output = pl.pallas_call(
        functools.partial(last_kernel, (n, rows, cols, feats)),
        out_shape=jax.ShapeDtypeStruct((rows * cols, width), bf16),
        in_specs=[vmem] * 6,
        out_specs=vmem,
        scratch_shapes=[
            pltpu.VMEM((2, parts * rows, 128), f32),
            pltpu.VMEM((rows * cols, 128), f32),
            pltpu.VMEM((rows * cols, width), f32),
        ],
        name="last_stage",
    )(*map(in_vmem, (own, other, tri_scale, scale, gate_entry, mixed)))
    return revised.reshape(t, ch, 8 * parts).transpose(2, 0, 1), pair_output.reshape(rows, cols, width)


def on_device(
    sequence_stack,
    present_sequence_flags,
    genuine_residue_flags,
    couple_state,
    tensor_scale,
    tensor_entry_matrix,
    tensor_final_matrix,
    tensor_offset,
    mean_sequence_scale,
    mean_couple_scale,
    mean_score_matrix,
    mean_content_matrix,
    mean_sigmoid_matrix,
    mean_final_matrix,
    trimul_scale,
    trimul_entry_matrix,
    trimul_result_scale,
    trimul_final_matrix,
):
    n = lax.axis_size("row")
    parts = n * n
    rows, cols, width = couple_state.shape
    count, t, ch = sequence_stack.shape
    heads = mean_score_matrix.shape[1]
    feats = width // (2 * parts)
    order = tuple(tuple((r * rows + c * t, t) for r in range(n)) for c in range(n))
    flags = present_sequence_flags.reshape(2, count)
    tokens = sequence_stack.transpose(1, 2, 0)
    *sends, right = first_stage(tokens, flags, tensor_scale.reshape(1, ch), tensor_entry_matrix, couple_state, n)

    def move(array, where):
        pairs = [(r * n + c, where(r, c)[0] * n + where(r, c)[1]) for r in range(n) for c in range(n)]
        return lax.ppermute(array, ("row", "col"), pairs)

    rights = [right] + [move(right, lambda r, c, k=k: (r ^ k, c)) for k in range(1, n)]
    lefts = [sends[0]] + [move(sends[k], lambda r, c, k=k: (r, (c + k) % n)) for k in range(1, n)]
    kept = (
        flags,
        tensor_final_matrix,
        tensor_offset.reshape(1, -1),
        mean_couple_scale.reshape(1, -1),
        mean_score_matrix.T,
        trimul_scale.reshape(1, -1),
        mean_sequence_scale.reshape(1, -1),
        mean_content_matrix,
        mean_sigmoid_matrix,
        mean_final_matrix.T,
    )
    ready = ready_stage(
        right, trimul_entry_matrix, tokens, trimul_result_scale, trimul_final_matrix, kept, n, rows, cols
    )
    lefts, ready = lax.optimization_barrier((lefts, ready))
    picked, slab, gate_entry, mixed, scale, *kept = ready
    flags, outer_final, offset, couple_scale, score, tri_scale, seq_scale, content, sigmoid_matrix, mean_final = kept
    share = outer_stage(lefts, rights, flags, outer_final)
    other = lax.ppermute(share, "depth", [(0, 1), (1, 0)])
    block = pair_stage(
        genuine_residue_flags, share, other, offset, couple_scale, score, tri_scale, picked, slab, n, rows, cols
    )
    block = lax.all_to_all(block, ("col", "row"), 0, 0, tiled=True)
    block = middle_stage(
        block, n, rows, cols, heads, feats, order, seq_scale, content, sigmoid_matrix, mean_final
    )
    block = lax.all_to_all(block, ("col", "row"), 0, 0, tiled=True)
    other = lax.ppermute(block[:, : rows + cols], "depth", [(0, 1), (1, 0)])
    return last_stage(block, other, tri_scale, gate_entry, scale, mixed, n, rows, cols, t, ch)


def suits(mesh):
    return mesh.shape["row"] == mesh.shape["col"] and mesh.shape["depth"] == 2


def solution(mesh):
    placed = (P("depth", ("row", "col"), None), P(), P(), P("row", "col", None)) + (P(),) * 14
    return jax.shard_map(
        on_device if suits(mesh) else on_device_generic,
        mesh=mesh,
        in_specs=placed,
        out_specs=(P("depth", ("row", "col"), None), P("row", "col", None)),
        check_vma=False,
    )
```

```python
import functools

import jax
import jax.numpy as jnp
from jax import lax
from jax.experimental import pallas as pl
from jax.experimental.pallas import tpu as pltpu
from jax.sharding import PartitionSpec as P

epsilon = 1e-05
bf16 = jnp.bfloat16
f32 = jnp.float32


def from_root(array, axis, root):
    mine = lax.axis_index(axis) == root
    return lax.psum(jnp.where(mine, array, jnp.zeros_like(array)), axis)


def standardize_features(value_rows, scale):
    value_rows = value_rows.astype(jnp.float32)
    average = jnp.mean(value_rows, -1, keepdims=True)
    centred = value_rows - average
    variance = jnp.mean(centred * centred, -1, keepdims=True)
    return centred * lax.rsqrt(variance + epsilon) * scale


def on_device_generic(
    sequence_stack,
    present_sequence_flags,
    genuine_residue_flags,
    couple_state,
    tensor_scale,
    tensor_entry_matrix,
    tensor_final_matrix,
    tensor_offset,
    mean_sequence_scale,
    mean_couple_scale,
    mean_score_matrix,
    mean_content_matrix,
    mean_sigmoid_matrix,
    mean_final_matrix,
    trimul_scale,
    trimul_entry_matrix,
    trimul_result_scale,
    trimul_final_matrix,
):
    n_row = lax.axis_size("row")
    n_col = lax.axis_size("col")
    row_index = lax.axis_index("row")
    col_index = lax.axis_index("col")
    depth_position = lax.axis_index("depth")
    piece_rows, piece_columns, width = couple_state.shape
    sequence_count, shard_residues, ignored_quantity = sequence_stack.shape
    hidden = tensor_entry_matrix.shape[1] // 2
    head_split = mean_score_matrix.shape[1]
    head_channels = mean_content_matrix.shape[1] // head_split
    token_weight = genuine_residue_flags.astype(jnp.float32)
    mask_as_float = present_sequence_flags.astype(jnp.float32)
    row_softmax_weight = lax.dynamic_slice_in_dim(
        mask_as_float, depth_position * sequence_count, sequence_count
    )
    row_count = jnp.sum(mask_as_float)
    entire_sequences = lax.all_gather(sequence_stack, "col", axis=1, tiled=True)
    root_row = col_index * n_row // n_col
    offset = col_index * piece_columns - root_row * piece_rows
    column_piece = lax.dynamic_slice_in_dim(entire_sequences, offset, piece_columns, 1)
    whole_cols = from_root(column_piece, "row", root_row)
    opm_rows = standardize_features(entire_sequences, tensor_scale).astype(jnp.bfloat16)
    opm_cols = standardize_features(whole_cols, tensor_scale).astype(jnp.bfloat16)
    left_projection = (
        jnp.dot(opm_rows, tensor_entry_matrix[:, :hidden], preferred_element_type=jnp.float32)
        * row_softmax_weight[:, None, None]
    ).astype(jnp.bfloat16)
    right_proj = (
        jnp.dot(opm_cols, tensor_entry_matrix[:, hidden:], preferred_element_type=jnp.float32)
        * row_softmax_weight[:, None, None]
    ).astype(jnp.bfloat16)
    outer_sum = jnp.einsum(
        "sic,sjd->ijcd", left_projection, right_proj, preferred_element_type=jnp.float32
    )
    outer_sum = outer_sum.reshape(piece_rows, piece_columns, hidden * hidden)
    out_float = tensor_final_matrix.astype(jnp.float32)
    outer_share = lax.psum_scatter(outer_sum, "depth", scatter_dimension=0, tiled=True)
    share_rows = outer_share.shape[0]
    pair_share = lax.dynamic_slice_in_dim(couple_state, depth_position * share_rows, share_rows, 0)
    update = (
        jnp.dot(outer_share, out_float, precision=lax.Precision.HIGHEST) / (row_count + 0.001)
        + tensor_offset
    )
    new_share = (pair_share.astype(jnp.float32) + update).astype(jnp.bfloat16)
    pair_one = lax.all_gather(new_share, "depth", axis=0, tiled=True)
    row_tokens = lax.dynamic_slice_in_dim(token_weight, row_index * piece_rows, piece_rows)
    col_tokens = lax.dynamic_slice_in_dim(token_weight, col_index * piece_columns, piece_columns)
    logits = jnp.einsum(
        "ijc,ch->ijh",
        standardize_features(pair_one, mean_couple_scale),
        mean_score_matrix,
        precision=lax.Precision.HIGHEST,
    )
    logits = logits + 1000000000.0 * (col_tokens - 1.0)[None, :, None]
    peak = lax.pmax(jnp.max(logits, axis=1), "col")
    expo = jnp.exp(logits - peak[:, None, :])
    total = lax.psum(jnp.sum(expo, axis=1), "col")
    weights = (expo / total[:, None, :]).astype(jnp.bfloat16)
    col_normed = standardize_features(whole_cols, mean_sequence_scale).astype(jnp.bfloat16)
    value_rows = jnp.dot(
        col_normed, mean_content_matrix, preferred_element_type=jnp.float32
    ).astype(jnp.bfloat16)
    value_rows = value_rows.reshape(sequence_count, piece_columns, head_split, head_channels)
    averaged_values = jnp.einsum(
        "ijh,sjhe->sihe", weights, value_rows, preferred_element_type=jnp.float32
    )
    averaged_values = averaged_values.reshape(
        sequence_count, piece_rows, head_split * head_channels
    )
    output_weight = mean_final_matrix.astype(jnp.float32)
    local_portion = lax.psum_scatter(
        averaged_values.astype(jnp.bfloat16), "col", scatter_dimension=1, tiled=True
    ).astype(jnp.float32)
    shard_standardized = standardize_features(sequence_stack, mean_sequence_scale).astype(
        jnp.bfloat16
    )
    gate_values = jax.nn.sigmoid(
        jnp.dot(shard_standardized, mean_sigmoid_matrix, preferred_element_type=jnp.float32)
    )
    sequence_delta = jnp.dot(
        gate_values * local_portion, output_weight, precision=lax.Precision.HIGHEST
    )
    revised_sequences = (sequence_stack.astype(jnp.float32) + sequence_delta).astype(jnp.bfloat16)
    tri_normed = standardize_features(pair_one, trimul_scale).astype(jnp.bfloat16)
    projected = jnp.dot(tri_normed, trimul_entry_matrix, preferred_element_type=jnp.float32)
    pair_mask = (row_tokens[:, None] * col_tokens[None, :])[..., None]
    tri_left = (
        jax.nn.sigmoid(projected[..., 0:width]) * projected[..., width : 2 * width] * pair_mask
    ).astype(jnp.bfloat16)
    tri_right = (
        jax.nn.sigmoid(projected[..., 2 * width : 3 * width])
        * projected[..., 3 * width : 4 * width]
        * pair_mask
    ).astype(jnp.bfloat16)
    out_gate = jax.nn.sigmoid(projected[..., 4 * width : 5 * width])
    left_rows, right_rows = (
        lax.all_gather(tri_left, "col", axis=1, tiled=True),
        lax.all_gather(tri_right, "col", axis=1, tiled=True),
    )
    right_piece = lax.dynamic_slice_in_dim(right_rows, offset, piece_columns, 0)
    right_needed = from_root(right_piece, "row", root_row)
    product = jnp.einsum(
        "ikc,jkc->ijc", left_rows, right_needed, preferred_element_type=jnp.float32
    )
    final = out_gate * jnp.dot(
        standardize_features(product, trimul_result_scale).astype(jnp.bfloat16),
        trimul_final_matrix,
        preferred_element_type=jnp.float32,
    )
    pair_output = (pair_one.astype(jnp.float32) + final).astype(jnp.bfloat16)
    return (revised_sequences, pair_output)


def in_vmem(array):
    return pltpu.with_memory_space_constraint(array, pltpu.VMEM)


def place_lanes(source, start, count, target, lane, base):
    block, offset = start // 128, start % 128
    shift = (target - offset) % 128
    piece = source[:, block * 128 : (block + 1) * 128]
    piece = pltpu.roll(piece, shift, 1) if shift else piece
    if offset + count > 128:
        rest = source[:, (block + 1) * 128 : (block + 2) * 128]
        rest = pltpu.roll(rest, shift, 1) if shift else rest
        piece = jnp.where(lane < target + 128 - offset, piece, rest)
    return jnp.where((lane >= target) & (lane < target + count), piece, base)


def swap_groups(tiles, size, lane):
    ratio = len(tiles)
    masks = [(lane >= g * size) & (lane < (g + 1) * size) for g in range(ratio)]
    turned = []
    for k in range(ratio):
        diagonal = tiles[-k % ratio]
        for g in range(1, ratio):
            diagonal = jnp.where(masks[g], tiles[(g - k) % ratio], diagonal)
        turned.append(pltpu.roll(diagonal, 128 - k * size, 1) if k else diagonal)
    swapped = []
    for x in range(ratio):
        tile = turned[x]
        for g in range(1, ratio):
            tile = jnp.where(masks[g], turned[(x - g) % ratio], tile)
        swapped.append(tile)
    return swapped


def unit_rows(value):
    centred = value - jnp.mean(value, -1, keepdims=True)
    variance = jnp.mean(centred * centred, -1, keepdims=True)
    return centred * lax.rsqrt(variance + epsilon)


def first_kernel(tokens_hbm, flags_hbm, scale_hbm, entry_hbm, couple_hbm, *refs):
    n = len(refs) - 8
    sends, right, pieces, tokens, couple, flags, scale, entry, arrived = refs[:n], refs[n], *refs[n + 1 :]
    t, ch, s = tokens.shape
    hidden, part = entry.shape[1] // 2, couple.shape[0]
    half, place = lax.axis_index("depth"), lax.axis_index("col")
    copies = [
        pltpu.make_async_copy(tokens_hbm, tokens, arrived.at[0]),
        pltpu.make_async_copy(couple_hbm.at[pl.ds(half * part, part)], couple, arrived.at[1]),
        pltpu.make_async_copy(flags_hbm, flags, arrived.at[2]),
        pltpu.make_async_copy(scale_hbm, scale, arrived.at[3]),
        pltpu.make_async_copy(entry_hbm, entry, arrived.at[4]),
    ]
    for copy in copies:
        copy.start()
    for copy in copies[2:]:
        copy.wait()
    mask = flags[pl.ds(half, 1), :].astype(f32)
    square = (ch, ch)
    diagonal = lax.broadcasted_iota(jnp.int32, square, 0) == lax.broadcasted_iota(jnp.int32, square, 1)
    column = jnp.sum(jnp.where(diagonal, scale[...], 0.0), 1, keepdims=True)
    copies[0].wait()
    lefts = []
    for u in range(t):
        value = tokens[u].astype(f32)
        centred = value - jnp.mean(value, 0, keepdims=True)
        variance = jnp.mean(centred * centred, 0, keepdims=True)
        normed = (centred * lax.rsqrt(variance + epsilon) * column).astype(bf16)
        factor = lax.dot_general(entry[...], normed, (((0,), (0,)), ((), ())), preferred_element_type=f32) * mask
        lefts.append(factor[:hidden])
        right[u] = factor[hidden:].astype(bf16)
    copies[1].wait()
    for i in range(part):
        row = couple[i].astype(f32)
        for k in range(n):
            pieces[k, i * t : (i + 1) * t] = row[k * t : (k + 1) * t]
    for k in range(n):
        sends[k][...] = jnp.concatenate(lefts + [pieces[lax.rem(place + k, n)]], 0).astype(bf16)


def first_stage(tokens, flags, scale, entry, couple, n):
    t, ch, s = tokens.shape
    rows, cols, width = couple.shape
    hidden = entry.shape[1] // 2
    vmem, hbm = pl.BlockSpec(memory_space=pltpu.VMEM), pl.BlockSpec(memory_space=pl.ANY)
    length = t * hidden + rows // 2 * t
    return pl.pallas_call(
        first_kernel,
        out_shape=[pltpu.VMEM((length, s), bf16)] * n + [pltpu.VMEM((t, hidden, s), bf16)],
        in_specs=[hbm] * 5,
        out_specs=[vmem] * (n + 1),
        scratch_shapes=[
            pltpu.VMEM((n, rows // 2 * t, width), f32),
            pltpu.VMEM(tokens.shape, bf16),
            pltpu.VMEM((rows // 2, cols, width), bf16),
            pltpu.VMEM(flags.shape, flags.dtype),
            pltpu.VMEM(scale.shape, f32),
            pltpu.VMEM(entry.shape, bf16),
            pltpu.SemaphoreType.DMA((5,)),
        ],
        name="first_stage",
    )(tokens, flags, scale, entry, couple)


def ready_kernel(sizes, *refs):
    n, rows, cols, feats = sizes
    parts = n * n
    kept = (len(refs) - 17) // 2
    after, result_scale_hbm, entry_hbm, tokens_hbm, final_hbm = refs[:5]
    picked, slab, gate_entry, mixed, scale = refs[5 + kept : 10 + kept]
    entry, tokens, turned_entry, final, plain, result_scale, arrived = refs[10 + 2 * kept :]
    half = lax.axis_index("depth")
    width, group, wide = entry.shape[0], feats * parts, 2 * parts
    copies = [
        pltpu.make_async_copy(entry_hbm.at[:, pl.ds(0, 4 * width)], entry, arrived.at[0]),
        pltpu.make_async_copy(tokens_hbm, tokens, arrived.at[1]),
        pltpu.make_async_copy(entry_hbm.at[:, pl.ds(4 * width, width)], gate_entry, arrived.at[2]),
        pltpu.make_async_copy(final_hbm, final, arrived.at[3]),
        pltpu.make_async_copy(result_scale_hbm, result_scale, arrived.at[4]),
    ]
    for k in range(kept):
        copies.append(pltpu.make_async_copy(refs[5 + k], refs[10 + kept + k], arrived.at[5 + k]))
    for copy in copies:
        copy.start()
    t, ch, s = tokens.shape
    copies[4].wait()
    at = lax.broadcasted_iota(jnp.int32, (width, width), 1)
    origin = lax.broadcasted_iota(jnp.int32, (width, width), 0)
    goal = lax.rem(origin, feats) * wide + lax.div(origin, feats)
    scale[...] = jnp.dot(
        result_scale[...], (at == goal).astype(f32), precision=lax.Precision.HIGHEST, preferred_element_type=f32
    )
    copies[0].wait()
    turned_entry[...] = entry[...].astype(f32).T
    for k in range(4):
        start = pl.multiple_of(k * width + half * group, 8)
        turned_entry[k * group : (k + 1) * group] = turned_entry[pl.ds(start, group), :]
    for k in range(4):
        for f in range(feats):
            picked[(k * feats + f) * parts : (k * feats + f + 1) * parts] = turned_entry[
                pl.ds(k * group + f, parts, stride=feats), :
            ].astype(bf16)
    copies[1].wait()
    turned = tokens[...].astype(f32).reshape(t * ch, s).T
    for p in range(parts):
        slab[p] = jnp.concatenate(
            [turned[p * 8 : (p + 1) * 8, a * 128 : (a + 1) * 128] for a in range(t * ch // 128)], 0
        )
    for copy in copies[2:4] + copies[5:]:
        copy.wait()
    plain[...] = final[...].astype(f32)
    for f in range(feats):
        mixed[f * wide : (f + 1) * wide] = plain[pl.ds(f, wide, stride=feats), :].astype(bf16)


def ready_stage(after, entry, tokens, result_scale, final, kept, n, rows, cols):
    parts, width = n * n, entry.shape[0]
    feats = width // (2 * parts)
    t, ch, s = tokens.shape
    vmem, hbm = pl.BlockSpec(memory_space=pltpu.VMEM), pl.BlockSpec(memory_space=pl.ANY)
    return pl.pallas_call(
        functools.partial(ready_kernel, (n, rows, cols, feats)),
        out_shape=[
            pltpu.VMEM((4 * feats * parts, width), bf16),
            pltpu.VMEM((parts, t * ch // 128 * 8, 128), f32),
            pltpu.VMEM((width, width), bf16),
            pltpu.VMEM((width, width), bf16),
            pltpu.VMEM((1, width), f32),
        ]
        + [pltpu.VMEM(array.shape, array.dtype) for array in kept],
        in_specs=[hbm] * (5 + len(kept)),
        out_specs=[vmem] * (5 + len(kept)),
        scratch_shapes=[
            pltpu.VMEM((width, 4 * width), bf16),
            pltpu.VMEM(tokens.shape, bf16),
            pltpu.VMEM((4 * width, width), f32),
            pltpu.VMEM((width, width), bf16),
            pltpu.VMEM((width, width), f32),
            pltpu.VMEM((1, width), f32),
            pltpu.SemaphoreType.DMA((5 + len(kept),)),
        ],
        name="ready_stage",
    )(in_vmem(after), result_scale.reshape(1, -1), entry, tokens, final, *kept)


def outer_kernel(n, *refs):
    half, row_index, col_index = lax.axis_index("depth"), lax.axis_index("row"), lax.axis_index("col")
    lefts, rights = refs[:n], refs[n : 2 * n]
    t, hidden, s = rights[0].shape
    flags, final, out, left, pieces, right, plain, turned, outer, high, low, couples, couple = refs[2 * n :]
    tokens, ratio = n * t, 128 // hidden
    for k in range(n):
        sent = lefts[k][...].astype(f32)
        place = lax.rem(col_index + (n - k), n)
        left[place] = sent[: t * hidden].astype(bf16)
        couples[place] = sent[t * hidden :]
        pieces[row_index ^ k] = rights[k][...].reshape(t * hidden, s).astype(f32)
    for k in range(n):
        for u in range(t):
            right[pl.ds(k * t + u, hidden, stride=tokens), :] = pieces[k, u * hidden : (u + 1) * hidden, :]
    outer[...] = lax.dot_general(
        right[...].astype(bf16),
        left[...].reshape(tokens * hidden, s),
        (((1,), (1,)), ((), ())),
        preferred_element_type=f32,
    )
    plain[...] = final[...].astype(f32)
    for d in range(hidden):
        turned[d * hidden : (d + 1) * hidden, :] = plain[pl.ds(d, hidden, stride=hidden), :].astype(bf16)
    lane = lax.broadcasted_iota(jnp.int32, (tokens, 128), 1)
    for g in range(tokens // ratio):
        for q in range(hidden // ratio):
            tiles = [
                outer[(q * ratio + d) * tokens : (q * ratio + d + 1) * tokens, g * 128 : (g + 1) * 128]
                for d in range(ratio)
            ]
            whole = jnp.concatenate(swap_groups(tiles, hidden, lane), 0)
            rounded = whole.astype(bf16)
            here = slice(g * ratio * tokens, (g + 1) * ratio * tokens), slice(q * 128, (q + 1) * 128)
            high[here] = rounded
            low[here] = (whole - rounded.astype(f32)).astype(bf16)
    part = tokens // 2
    for k in range(n):
        for i in range(part):
            couple[i * tokens + k * t : i * tokens + (k + 1) * t] = couples[k, i * t : (i + 1) * t]
    total = jnp.sum(flags[...].astype(f32)) + 0.001
    update = jnp.dot(high[...], turned[...], preferred_element_type=f32) + jnp.dot(
        low[...], turned[...], preferred_element_type=f32
    )
    out[...] = update / total
    mine = pl.ds(pl.multiple_of(half * (part * tokens), 8), part * tokens)
    out[mine, :] = out[mine, :] + couple[...]


def outer_stage(lefts, rights, flags, final):
    n = len(lefts)
    t, hidden, s = rights[0].shape
    tokens, width = n * t, final.shape[1]
    vmem = pl.BlockSpec(memory_space=pltpu.VMEM)
    return pl.pallas_call(
        functools.partial(outer_kernel, n),
        out_shape=pltpu.VMEM((tokens * tokens, width), f32),
        in_specs=[vmem] * (2 * n + 2),
        out_specs=vmem,
        scratch_shapes=[
            pltpu.VMEM((n, t * hidden, s), bf16),
            pltpu.VMEM((n, t * hidden, s), f32),
            pltpu.VMEM((tokens * hidden, s), f32),
            pltpu.VMEM((hidden * hidden, width), f32),
            pltpu.VMEM((hidden * hidden, width), bf16),
            pltpu.VMEM((tokens * hidden, tokens * hidden), f32),
            pltpu.VMEM((tokens * tokens, hidden * hidden), bf16),
            pltpu.VMEM((tokens * tokens, hidden * hidden), bf16),
            pltpu.VMEM((n, tokens // 2 * t, width), f32),
            pltpu.VMEM((tokens // 2 * tokens, width), f32),
        ],
        name="outer_stage",
    )(*map(in_vmem, lefts), *map(in_vmem, rights), in_vmem(flags), in_vmem(final))


def pair_kernel(sizes, genuine_hbm, own, other, offset, couple_scale, score, tri_scale, picked, slab, block, value, normed, projected, logits, tri, head_rows, genuine, arrived):
    n, rows, cols, heads, feats = sizes
    half, row_index, col_index = lax.axis_index("depth"), lax.axis_index("row"), lax.axis_index("col")
    parts, width = n * n, own.shape[1]
    part, spare = rows // 2, 128 - feats * cols
    copy = pltpu.make_async_copy(genuine_hbm, genuine, arrived)
    copy.start()
    total = own[...] + other[...] + offset[...]
    value[...] = total.astype(bf16).astype(f32)
    unit = unit_rows(value[...])
    size = rows * cols
    padded = normed.shape[0]
    wide = lax.dot_general(
        score[...], unit * couple_scale[...], (((1,), (1,)), ((), ())),
        precision=lax.Precision.HIGHEST, preferred_element_type=f32,
    )
    logits[:, :size] = wide
    lane8 = lax.broadcasted_iota(jnp.int32, (heads, 128), 1)
    low = jnp.full((heads, 128), -jnp.inf, f32)
    for i in range(rows):
        head_rows[pl.ds(i, heads, stride=rows), :] = place_lanes(logits, i * cols, cols, 0, lane8, low)
    t = cols // n
    copy.wait()
    line = lax.broadcasted_iota(jnp.int32, (8, 128), 1)
    bias = jnp.zeros((8, 128), f32)
    open_lanes = jnp.zeros((8, 128), f32)
    for j in range(cols):
        flag = genuine[j // t * rows + col_index * t + j % t].astype(f32)
        bias = jnp.where(line == j, 1000000000.0 * (flag - 1.0), bias)
        here = line == j
        for f in range(1, feats):
            here = here | (line == f * cols + j)
        open_lanes = jnp.where(here, flag, open_lanes)
    score_rows = head_rows[...] + bias[:1]
    peak = jnp.max(score_rows, -1, keepdims=True)
    expo = jnp.exp(score_rows - peak).astype(bf16).astype(f32)
    lane = lax.broadcasted_iota(jnp.int32, (rows, 128), 1)
    zero = jnp.zeros((rows, 128), f32)
    tail = zero
    flat = zero
    for h in range(heads):
        mine = expo[h * rows : (h + 1) * rows]
        start = h * cols
        if start < 128:
            shifted = pltpu.roll(mine, start, 1) if start else mine
            flat = jnp.where((lane >= start) & (lane < start + cols), shifted, flat)
            if start + cols > 128:
                tail = jnp.where(lane < start + cols - 128, shifted, tail)
        else:
            start -= 128
            shifted = pltpu.roll(mine, start, 1) if start else mine
            tail = jnp.where((lane >= start) & (lane < start + cols), shifted, tail)
    first, second = pltpu.roll(tail, 128 - spare, 1), pltpu.roll(tail, 128 - 2 * spare, 1)
    wide_peak = jnp.broadcast_to(peak, (heads * rows, 128))
    tiny = lax.broadcasted_iota(jnp.int32, (8, 128), 1)
    stats = jnp.zeros((8, 128), f32)
    for q in range(3):
        piece = wide_peak.astype(bf16).astype(f32)
        wide_peak = wide_peak - piece
        for a in range(rows // 8):
            for h in range(heads):
                stats = jnp.where(
                    tiny == a * 3 * heads + q * heads + h, piece[h * rows + a * 8 : h * rows + a * 8 + 8], stats
                )
    normed[:size] = (unit * tri_scale[...]).astype(bf16)
    normed[size:] = jnp.zeros((padded - size, width), bf16)
    group = feats * parts
    raw = lax.dot_general(picked[...], normed[...], (((1,), (1,)), ((), ())), preferred_element_type=f32)
    cut = lax.broadcasted_iota(jnp.int32, (parts, 128), 1)
    empty = jnp.zeros((parts, 128), f32)
    for side in range(2):
        base = side * 2 * group
        projected[...] = jax.nn.sigmoid(raw[base : base + group]) * raw[base + group : base + 2 * group]
        for i in range(rows):
            packed = empty
            for f in range(feats):
                packed = place_lanes(projected.at[f * parts : (f + 1) * parts], i * cols, cols, f * cols, cut, packed)
            flag = genuine[row_index * rows + i].astype(f32)
            tri[side, pl.ds(i, parts, stride=rows), :] = packed * (open_lanes[:1] * flag)
    keep = lane < feats * cols
    for p in range(parts):
        slabs = [
            jnp.where(keep, tri[0, p * rows : (p + 1) * rows], first),
            jnp.where(keep, tri[1, p * rows : (p + 1) * rows], second),
            flat,
            stats,
            slab[p],
        ]
        if p < part:
            slabs.append(value[pl.ds(pl.multiple_of((half * part + p) * cols, 8), cols), :])
        else:
            slabs.append(jnp.zeros((cols, width), f32))
        block[p] = jnp.concatenate(slabs, 0).astype(bf16)


def pair_stage(genuine, own, other, offset, couple_scale, score, tri_scale, picked, slab, n, rows, cols):
    parts, width = n * n, own.shape[1]
    heads = score.shape[0]
    feats = width // (2 * parts)
    padded = (rows * cols + 127) // 128 * 128
    vmem = pl.BlockSpec(memory_space=pltpu.VMEM)
    length = 3 * rows + 8 + slab.shape[1] + cols
    return pl.pallas_call(
        functools.partial(pair_kernel, (n, rows, cols, heads, feats)),
        out_shape=pltpu.VMEM((parts, length, 128), bf16),
        in_specs=[pl.BlockSpec(memory_space=pl.ANY)] + [vmem] * 8,
        out_specs=vmem,
        scratch_shapes=[
            pltpu.VMEM((rows * cols, width), f32),
            pltpu.VMEM((padded, width), bf16),
            pltpu.VMEM((feats * parts, padded), f32),
            pltpu.VMEM((heads, padded), f32),
            pltpu.VMEM((2, parts * rows, 128), f32),
            pltpu.VMEM((heads * rows, 128), f32),
            pltpu.SMEM(genuine.shape, genuine.dtype),
            pltpu.SemaphoreType.DMA,
        ],
        name="pair_stage",
    )(genuine, *map(in_vmem, (own, other, offset, couple_scale, score, tri_scale, picked, slab)))


def halves(value):
    high = value.astype(bf16)
    return high, (value - high.astype(f32)).astype(bf16)


def two_pass_dot(value, matrix, axis=0):
    high, low = halves(value)
    over = (((1,), (axis,)), ((), ()))
    return lax.dot_general(high, matrix, over, preferred_element_type=f32) + lax.dot_general(
        low, matrix, over, preferred_element_type=f32
    )


def middle_kernel(sizes, block, seq_scale, content, sigmoid_matrix, final, out, wide, lhs, rhs, product, weights, x, values, gated, masked, revised):
    n, rows, cols, heads, feats, groups, order = sizes
    parts, tokens, ch = n * n, n * rows, final.shape[0]
    s, per = 8, 128 // final.shape[0]
    t = rows // n
    wide[...] = block[...].astype(f32)
    lane = lax.broadcasted_iota(jnp.int32, (tokens, 128), 1)
    small = lax.broadcasted_iota(jnp.int32, (rows, 128), 1)
    tiny = lax.broadcasted_iota(jnp.int32, (8, 128), 1)
    spare = 128 - feats * cols

    def stacked(c, start, count):
        return jnp.concatenate([wide[c * n + r, start : start + count] for r in range(n)], 0)

    rhs[...] = jnp.zeros_like(rhs)
    for c in range(n):
        mine = stacked(c, 0, rows)
        for f in range(feats):
            keep = (lane >= f * cols) & (lane < (f + 1) * cols)
            lhs[f * tokens : (f + 1) * tokens, c * 128 : (c + 1) * 128] = jnp.where(keep, mine, 0.0).astype(bf16)
        rhs[:tokens, c * 128 : (c + 1) * 128] = stacked(c, rows, rows).astype(bf16)
    product[...] = lax.dot_general(lhs[...], rhs[...], (((1,), (1,)), ((), ())), preferred_element_type=f32)
    up = lax.broadcasted_iota(jnp.int32, (256, 128), 0)
    across = lax.broadcasted_iota(jnp.int32, (256, 128), 1)
    gather = ((up >= across * cols) & (up < (across + 1) * cols) & (across < heads)).astype(bf16)
    up = lax.broadcasted_iota(jnp.int32, (128, 256), 0)
    across = lax.broadcasted_iota(jnp.int32, (128, 256), 1)
    spread = ((across >= up * cols) & (across < (up + 1) * cols) & (up < heads)).astype(bf16)
    expos, peaks = [], []
    for c in range(n):
        a, b = stacked(c, 0, rows), stacked(c, rows, rows)
        rest = jnp.where(lane < spare, pltpu.roll(a, spare, 1), jnp.where(lane < 2 * spare, pltpu.roll(b, 2 * spare, 1), 0.0))
        expos.append(jnp.concatenate([stacked(c, 2 * rows, rows), rest], 1))
        peak = []
        for r in range(n):
            stats = wide[c * n + r, 3 * rows : 3 * rows + 8]
            for q in range(rows // 8):
                one = pltpu.roll(stats, (128 - 3 * heads * q) % 128, 1) if q else stats
                peak.append(one + pltpu.roll(one, 128 - heads, 1) + pltpu.roll(one, 128 - 2 * heads, 1))
        peaks.append(jnp.concatenate(peak, 0))
    top = peaks[0]
    for c in range(1, n):
        top = jnp.maximum(top, peaks[c])
    factors = [jnp.exp(peak - top) for peak in peaks]
    total = jnp.zeros_like(top)
    for c in range(n):
        total = total + factors[c] * jnp.dot(expos[c].astype(bf16), gather, preferred_element_type=f32)
    for c in range(n):
        scale = jnp.where(lane < heads, factors[c] / jnp.where(lane < heads, total, 1.0), 0.0)
        weights[:, c * 256 : (c + 1) * 256] = (expos[c] * two_pass_dot(scale, spread)).astype(bf16)
    first_token = [((p % n) * n + p // n) * t for p in range(parts)]
    for p in range(parts):
        for g in range(groups):
            pair = wide[p, 3 * rows + 8 + 8 * g : 3 * rows + 16 + 8 * g]
            for k in range(per):
                x[pl.ds(first_token[p] + g * per + k, s, stride=tokens), :] = pltpu.roll(pair, 128 - k * ch, 1) if k else pair
    raw = x[...][:, :ch]
    centred = raw - jnp.mean(raw, -1, keepdims=True)
    variance = jnp.mean(centred * centred, -1, keepdims=True)
    normed = (centred * lax.rsqrt(variance + epsilon) * seq_scale[...]).astype(bf16)
    values[...] = jnp.dot(normed, content[...], preferred_element_type=f32).astype(bf16).astype(f32)
    gates = jax.nn.sigmoid(jnp.dot(normed, sigmoid_matrix[...], preferred_element_type=f32))
    width = gates.shape[1]
    head_of = lax.broadcasted_iota(jnp.int32, (cols, width), 1) // (width // heads)
    used = heads * cols
    masked[...] = jnp.zeros_like(masked)
    for q in range(s):
        for c in range(n):
            local = jnp.concatenate([values[q * tokens + a : q * tokens + a + m] for a, m in order[c]], 0)
            spread_out = jnp.concatenate([jnp.where(head_of == h, local, 0.0) for h in range(heads)], 0)
            masked[q, c * 256 : c * 256 + used] = spread_out.astype(bf16)
        averaged = jnp.dot(weights[...], masked[q], preferred_element_type=f32)
        gated[q * tokens : (q + 1) * tokens] = gates[q * tokens : (q + 1) * tokens] * averaged
    delta = two_pass_dot(gated[...], final[...], 1)
    revised[:, :ch] = raw + delta
    for p in range(parts):
        c, r = p // n, p % n
        slab = jnp.zeros((rows, 128), f32)
        for f in range(feats):
            shift = ((f - c) * cols) % 128
            piece = product[f * tokens + r * rows : f * tokens + (r + 1) * rows]
            piece = pltpu.roll(piece, shift, 1) if shift else piece
            slab = jnp.where((small >= f * cols) & (small < (f + 1) * cols), piece, slab)
        start = 3 * rows + 8 + 8 * groups + c * t
        slabs = [slab] + [wide[k * n + r, start : start + t] for k in range(n)]
        for g in range(groups):
            merged = revised[pl.ds(first_token[p] + g * per, s, stride=tokens), :]
            for k in range(1, per):
                piece = revised[pl.ds(first_token[p] + g * per + k, s, stride=tokens), :]
                merged = jnp.where(tiny >= k * ch, pltpu.roll(piece, k * ch, 1), merged)
            slabs.append(merged)
        out[p] = jnp.concatenate(slabs, 0).astype(bf16)


def middle_stage(block, n, rows, cols, heads, feats, order, seq_scale, content, sigmoid_matrix, final):
    parts, tokens = n * n, n * rows
    groups = (block.shape[1] - 3 * rows - 8 - cols) // 8
    width = content.shape[1]
    vmem = pl.BlockSpec(memory_space=pltpu.VMEM)
    return pl.pallas_call(
        functools.partial(middle_kernel, (n, rows, cols, heads, feats, groups, order)),
        out_shape=pltpu.VMEM((parts, rows + cols + 8 * groups, 128), bf16),
        in_specs=[vmem] * 5,
        out_specs=vmem,
        scratch_shapes=[
            pltpu.VMEM(block.shape, f32),
            pltpu.VMEM((feats * tokens, n * 128), bf16),
            pltpu.VMEM((128, n * 128), bf16),
            pltpu.VMEM((feats * tokens, 128), f32),
            pltpu.VMEM((tokens, n * 256), bf16),
            pltpu.VMEM((8 * tokens, 128), f32),
            pltpu.VMEM((8 * tokens, width), f32),
            pltpu.VMEM((8 * tokens, width), f32),
            pltpu.VMEM((8, n * 256, width), bf16),
            pltpu.VMEM((8 * tokens, 128), f32),
        ],
        name="middle_stage",
    )(*map(in_vmem, (block, seq_scale, content, sigmoid_matrix, final)))


def turn_kernel(start, own, revised):
    for a in range((own.shape[1] - start) // 8):
        piece = [own[p, start + 8 * a : start + 8 * a + 8].astype(f32) for p in range(own.shape[0])]
        revised[a * 128 : (a + 1) * 128] = jnp.concatenate(piece, 0).T.astype(bf16)


def last_kernel(sizes, own, other, tri_scale, scale, entry, mixed, pair_output, product, turned, pair):
    n, rows, cols, feats = sizes
    parts = n * n
    part, wide = rows // 2, 2 * n * n
    mine = lax.axis_index("depth")
    theirs = 1 - mine
    for p in range(parts):
        here, there = own[p].astype(f32), other[p].astype(f32)
        product[mine, p * rows : (p + 1) * rows] = here[:rows]
        product[theirs, p * rows : (p + 1) * rows] = there[:rows]
        if p < part:
            pair[pl.ds(pl.multiple_of((mine * part + p) * cols, 8), cols), :] = here[rows : rows + cols]
            pair[pl.ds(pl.multiple_of((theirs * part + p) * cols, 8), cols), :] = there[rows : rows + cols]
    lane = lax.broadcasted_iota(jnp.int32, (cols, 128), 1)
    per = 128 // wide
    for g in range(rows // per):
        stacked = []
        for k in range(per):
            for d in range(2):
                stacked.append(product[d, pl.ds(g * per + k, parts, stride=rows), :])
        flipped = jnp.concatenate(stacked, 0).T
        tiles = [flipped[f * cols : (f + 1) * cols] for f in range(feats)]
        start = g * per * cols
        turned[start : start + per * cols] = jnp.concatenate(swap_groups(tiles, wide, lane), 0)
    value = pair[...]
    normed = (unit_rows(value) * tri_scale[...]).astype(bf16)
    gate = jax.nn.sigmoid(jnp.dot(normed, entry[...], preferred_element_type=f32))
    result = (unit_rows(turned[...]) * scale[...]).astype(bf16)
    pair_output[...] = (value + gate * jnp.dot(result, mixed[...], preferred_element_type=f32)).astype(bf16)


def last_stage(own, other, tri_scale, gate_entry, scale, mixed, n, rows, cols, t, ch):
    parts, width = n * n, mixed.shape[1]
    feats = width // (2 * parts)
    vmem = pl.BlockSpec(memory_space=pltpu.VMEM)
    revised = pl.pallas_call(
        functools.partial(turn_kernel, rows + cols),
        out_shape=jax.ShapeDtypeStruct((t * ch, 8 * parts), bf16),
        in_specs=[vmem],
        out_specs=vmem,
        name="turn_stage",
    )(in_vmem(own))
    pair_output = pl.pallas_call(
        functools.partial(last_kernel, (n, rows, cols, feats)),
        out_shape=jax.ShapeDtypeStruct((rows * cols, width), bf16),
        in_specs=[vmem] * 6,
        out_specs=vmem,
        scratch_shapes=[
            pltpu.VMEM((2, parts * rows, 128), f32),
            pltpu.VMEM((rows * cols, 128), f32),
            pltpu.VMEM((rows * cols, width), f32),
        ],
        name="last_stage",
    )(*map(in_vmem, (own, other, tri_scale, scale, gate_entry, mixed)))
    return revised.reshape(t, ch, 8 * parts).transpose(2, 0, 1), pair_output.reshape(rows, cols, width)


def on_device(
    sequence_stack,
    present_sequence_flags,
    genuine_residue_flags,
    couple_state,
    tensor_scale,
    tensor_entry_matrix,
    tensor_final_matrix,
    tensor_offset,
    mean_sequence_scale,
    mean_couple_scale,
    mean_score_matrix,
    mean_content_matrix,
    mean_sigmoid_matrix,
    mean_final_matrix,
    trimul_scale,
    trimul_entry_matrix,
    trimul_result_scale,
    trimul_final_matrix,
):
    n = lax.axis_size("row")
    parts = n * n
    rows, cols, width = couple_state.shape
    count, t, ch = sequence_stack.shape
    heads = mean_score_matrix.shape[1]
    feats = width // (2 * parts)
    order = tuple(tuple((r * rows + c * t, t) for r in range(n)) for c in range(n))
    flags = present_sequence_flags.reshape(2, count)
    tokens = sequence_stack.transpose(1, 2, 0)
    *sends, right = first_stage(tokens, flags, tensor_scale.reshape(1, ch), tensor_entry_matrix, couple_state, n)

    def move(array, where):
        pairs = [(r * n + c, where(r, c)[0] * n + where(r, c)[1]) for r in range(n) for c in range(n)]
        return lax.ppermute(array, ("row", "col"), pairs)

    rights = [right] + [move(right, lambda r, c, k=k: (r ^ k, c)) for k in range(1, n)]
    lefts = [sends[0]] + [move(sends[k], lambda r, c, k=k: (r, (c + k) % n)) for k in range(1, n)]
    kept = (
        flags,
        tensor_final_matrix,
        tensor_offset.reshape(1, -1),
        mean_couple_scale.reshape(1, -1),
        mean_score_matrix.T,
        trimul_scale.reshape(1, -1),
        mean_sequence_scale.reshape(1, -1),
        mean_content_matrix,
        mean_sigmoid_matrix,
        mean_final_matrix.T,
    )
    ready = ready_stage(
        right, trimul_entry_matrix, tokens, trimul_result_scale, trimul_final_matrix, kept, n, rows, cols
    )
    lefts, ready = lax.optimization_barrier((lefts, ready))
    picked, slab, gate_entry, mixed, scale, *kept = ready
    flags, outer_final, offset, couple_scale, score, tri_scale, seq_scale, content, sigmoid_matrix, mean_final = kept
    share = outer_stage(lefts, rights, flags, outer_final)
    other = lax.ppermute(share, "depth", [(0, 1), (1, 0)])
    block = pair_stage(
        genuine_residue_flags, share, other, offset, couple_scale, score, tri_scale, picked, slab, n, rows, cols
    )
    block = lax.all_to_all(block, ("col", "row"), 0, 0, tiled=True)
    block = middle_stage(
        block, n, rows, cols, heads, feats, order, seq_scale, content, sigmoid_matrix, mean_final
    )
    block = lax.all_to_all(block, ("col", "row"), 0, 0, tiled=True)
    other = lax.ppermute(block[:, : rows + cols], "depth", [(0, 1), (1, 0)])
    return last_stage(block, other, tri_scale, gate_entry, scale, mixed, n, rows, cols, t, ch)


def suits(mesh):
    n = mesh.shape["row"]
    return n == mesh.shape["col"] and n & (n - 1) == 0 and mesh.shape["depth"] == 2


def solution(mesh):
    placed = (P("depth", ("row", "col"), None), P(), P(), P("row", "col", None)) + (P(),) * 14
    return jax.shard_map(
        on_device if suits(mesh) else on_device_generic,
        mesh=mesh,
        in_specs=placed,
        out_specs=(P("depth", ("row", "col"), None), P("row", "col", None)),
        check_vma=False,
    )
```
